512 devices in a mesh: group: 2 (over y), ha: 16 (over x, core), wa: 16 (over z).
Axes of the slice: x: 8, y: 2, z: 16, core: 2. Of those that a mesh axis runs over, the one named last changes fastest.
The devices are a block of a 8x8x16 slice.
Arguments:
- queries: bfloat16 [4, 128, 128, 1536], P('group', 'ha', 'wa'), parts along dimension 0, may hold values from -6 to 6
- keys: bfloat16 [4, 128, 128, 1536], P('group', 'ha', 'wa'), parts along dimension 0, may hold values from -6 to 6
- values: bfloat16 [4, 128, 128, 1536], P('group', 'ha', 'wa'), parts along dimension 0, may hold values from -6 to 6
- out_grad: bfloat16 [4, 128, 128, 1536], P('group', 'ha', 'wa'), parts along dimension 0, may hold values from -96 to 96
- log_norm: float32 [12, 4, 128, 128], P(None, 'group', 'ha', 'wa'), parts along dimension 1, may hold values from 6.5 to 7.5
- delta_rows: float32 [12, 4, 128, 128], P(None, 'group', 'ha', 'wa'), parts along dimension 1, may hold values from -360 to 360
- text_keys: bfloat16 [64, 1536], P('group'), parts along dimension 0, may hold values from -6 to 6
- text_values: bfloat16 [64, 1536], P('group'), parts along dimension 0, may hold values from -6 to 6
- window_table: int32 [16, 16, 9], replicated, may hold values 0 or 1
Outputs:
- query_grad: bfloat16 [4, 128, 128, 1536], P('group', 'ha', 'wa'), parts along dimension 0
- key_grad: bfloat16 [4, 128, 128, 1536], P('group', 'ha', 'wa'), parts along dimension 0
- value_grad: bfloat16 [4, 128, 128, 1536], P('group', 'ha', 'wa'), parts along dimension 0
- text_key_grad: bfloat16 [64, 1536], P('group'), parts along dimension 0
- text_value_grad: bfloat16 [64, 1536], P('group'), parts along dimension 0
The draws below stay inside these ranges and needn't reach their ends.
There are 2 independent parts, one for each index of `group`. The reference program is written for one: setup_inputs(seed, part) draws one part's arguments, and reference() takes and returns one part's arrays. A program takes and returns all parts, laid end to end along the dimension named above; an argument that names none is the same for every part. Nothing has to cross between parts.
All inputs are finite; a program needn't handle non-finite values.
Results may differ from the reference program's by a relative error of at most 0.001.
The reference program's roundings to bfloat16 on the way (of `probs_half` and `score_grad`) count: a program that leaves them out, or rounds other values in their place, can miss the bound.
Values may be sent and summed in bfloat16 or wider, within the bound.
No kernel may reach another device: no remote copies, remote signals or barrier semaphores. Data moves between devices by JAX's collectives and lax.ppermute only.
A program may use at most 64 MiB of HBM per device.

```python
import jax
import jax.numpy as jnp
from jax import lax

HEADS = 12
HDIM = 128
TEXT = 32
FRAMES = 2
TILE = 8
HALO = 2
HD = 1536
NH = 128
NW = 128
N_HA = 16
N_WA = 16


def place_ends(array, own_key, least, high):
    place = [jax.random.randint(jax.random.fold_in(own_key, axis), (), 0, length) for axis, length in enumerate(array.shape)]
    longest = array.shape.index(max(array.shape))
    neighbour = place[:longest] + [(place[longest] + 1) % array.shape[longest]] + place[longest + 1:]
    return array.at[tuple(place)].set(least).at[tuple(neighbour)].set(high)


def shard_levels(stream_key, dims, split, least, largest):
    gain, own = 1.0, jax.random.fold_in(stream_key, 6)
    for axis_at, shards_of in split:
        heights = jnp.exp(jax.random.uniform(jax.random.fold_in(own, axis_at), (shards_of,), jnp.float32, least / len(split), largest / len(split)))
        gain = gain * jnp.repeat(heights, dims[axis_at] // shards_of).reshape([-1 if axis == axis_at else 1 for axis in range(len(dims))])
    return gain


def gaussian(rng, dims, scale, most, shards=(), kind=jnp.bfloat16):
    drawn = jax.random.normal(rng, dims, jnp.float32) * scale
    if len(shards) > 0:
        drawn = shard_levels(rng, dims, shards, -0.22, 0.18) * drawn
    return jnp.clip(drawn, min=-most, max=most).astype(kind)


def setup_inputs(seed: int = 0, part: int = 0) -> dict:
    streams_of = jax.random.split(jax.random.key(seed), 10)
    part_keys = jax.random.split(jax.random.fold_in(streams_of[9], part), 10)
    return {
        "queries": gaussian(part_keys[0], (FRAMES, NH, NW, HD), 1.0, 6.0, ((1, 16), (2, 16))),
        "keys": gaussian(part_keys[1], (FRAMES, NH, NW, HD), 1.0, 6.0, ((1, 16), (2, 16))),
        "values": gaussian(part_keys[2], (FRAMES, NH, NW, HD), 1.0, 6.0, ((1, 16), (2, 16))),
        "out_grad": gaussian(part_keys[3], (FRAMES, NH, NW, HD), 16.0, 96.0, ((1, 16), (2, 16))),
        "log_norm": jnp.clip(6.5 + 1.0 * jax.random.uniform(part_keys[4], (HEADS, FRAMES, NH, NW), jnp.float32) ** shard_levels(part_keys[4], (HEADS, FRAMES, NH, NW), ((2, 16), (3, 16)), -0.2, 0.2), 6.5, 7.5),
        "delta_rows": gaussian(part_keys[5], (HEADS, FRAMES, NH, NW), 60.0, 360.0, ((2, 16), (3, 16)), jnp.float32),
        "text_keys": gaussian(part_keys[6], (TEXT, HD), 1.0, 6.0),
        "text_values": gaussian(part_keys[7], (TEXT, HD), 1.0, 6.0),
        "window_table": place_ends((jax.random.randint(streams_of[8], (N_HA, N_WA, 9), 0, 4) < 3).astype(jnp.int32), jax.random.fold_in(streams_of[8], 1), 0, 1),
    }


def tile_grads(query_rows, cotangent_rows, norm_rows, delta_part, key_rows, value_rows, cell_mask):
    score_scale = 1.0 / (HDIM ** 0.5)
    query_wide = query_rows.astype(jnp.float32)
    cotangent_wide = cotangent_rows.astype(jnp.float32)
    key_wide = key_rows.astype(jnp.float32)
    value_wide = value_rows.astype(jnp.float32)
    scores = jnp.einsum("qhd,khd->hqk", query_wide, key_wide) * score_scale
    probs = jnp.exp(scores - norm_rows[:, :, None])
    if cell_mask is not None:
        probs = probs * cell_mask[None, None, :]
    probs_half = probs.astype(jnp.bfloat16)
    value_part = jnp.einsum("hqk,qhd->khd", probs_half.astype(jnp.float32), cotangent_wide)
    prob_grad = jnp.einsum("qhd,khd->hqk", cotangent_wide, value_wide)
    score_grad = (probs * (prob_grad - delta_part[:, :, None])).astype(jnp.bfloat16).astype(jnp.float32)
    query_part = jnp.einsum("hqk,khd->qhd", score_grad, key_wide) * score_scale
    key_part = jnp.einsum("hqk,qhd->khd", score_grad, query_wide) * score_scale
    return query_part, key_part, value_part


def reference(queries, keys, values, out_grad, log_norm, delta_rows, text_keys, text_values, window_table):
    frames, rows_all, cols_all, width = queries.shape
    tile_side = TILE
    halo_rim = HALO
    window_side = TILE + 2 * HALO
    pad_spec = ((0, 0), (halo_rim, halo_rim), (halo_rim, halo_rim), (0, 0))
    key_pad = jnp.pad(keys, pad_spec, mode="wrap")
    value_pad = jnp.pad(values, pad_spec, mode="wrap")
    position = jnp.arange(window_side, dtype=jnp.int32)
    block_of = (position >= halo_rim).astype(jnp.int32) + (position >= halo_rim + tile_side).astype(jnp.int32)
    text_key_rows = text_keys.reshape(TEXT, HEADS, HDIM)
    text_value_rows = text_values.reshape(TEXT, HEADS, HDIM)

    def per_tile(carry, tile_index):
        grad_pad, text_total = carry
        row_tile = (tile_index // N_WA).astype(jnp.int32)
        col_tile = (tile_index % N_WA).astype(jnp.int32)
        row_start = (row_tile * tile_side).astype(jnp.int32)
        col_start = (col_tile * tile_side).astype(jnp.int32)
        anchor = jnp.zeros((), jnp.int32)
        tile_shape = (frames, tile_side, tile_side, width)
        query_rows = lax.dynamic_slice(queries, (anchor, row_start, col_start, anchor), tile_shape).reshape(-1, HEADS, HDIM)
        cotangent_rows = lax.dynamic_slice(out_grad, (anchor, row_start, col_start, anchor), tile_shape).reshape(-1, HEADS, HDIM)
        stat_shape = (HEADS, frames, tile_side, tile_side)
        norm_rows = lax.dynamic_slice(log_norm, (anchor, anchor, row_start, col_start), stat_shape).reshape(HEADS, -1)
        delta_part = lax.dynamic_slice(delta_rows, (anchor, anchor, row_start, col_start), stat_shape).reshape(HEADS, -1)
        window_shape = (frames, window_side, window_side, width)
        key_rows = lax.dynamic_slice(key_pad, (anchor, row_start, col_start, anchor), window_shape).reshape(-1, HEADS, HDIM)
        value_rows = lax.dynamic_slice(value_pad, (anchor, row_start, col_start, anchor), window_shape).reshape(-1, HEADS, HDIM)
        pattern = lax.dynamic_slice(window_table, (row_tile, col_tile, anchor), (1, 1, 9)).reshape(9).astype(jnp.float32)
        cell_grid = pattern[3 * block_of[:, None] + block_of[None, :]]
        cell_mask = jnp.broadcast_to(cell_grid[None], (frames, window_side, window_side)).reshape(-1)
        video_query, video_key, video_value = tile_grads(query_rows, cotangent_rows, norm_rows, delta_part, key_rows, value_rows, cell_mask)
        text_query, text_key, text_value = tile_grads(query_rows, cotangent_rows, norm_rows, delta_part, text_key_rows, text_value_rows, None)
        query_tile = (video_query + text_query).astype(jnp.bfloat16).reshape(tile_shape)
        window_grad = jnp.stack((video_key, video_value)).reshape((2,) + window_shape)
        start = (anchor, anchor, row_start, col_start, anchor)
        current = lax.dynamic_slice(grad_pad, start, window_grad.shape)
        grad_pad = lax.dynamic_update_slice(grad_pad, current + window_grad, start)
        text_total = text_total + jnp.stack((text_key, text_value))
        return (grad_pad, text_total), query_tile

    grad_start = jnp.zeros((2, frames, rows_all + 2 * halo_rim, cols_all + 2 * halo_rim, width), jnp.float32)
    text_start = jnp.zeros((2, TEXT, HEADS, HDIM), jnp.float32)
    (grad_pad, text_total), query_tiles = lax.scan(per_tile, (grad_start, text_start), jnp.arange(N_HA * N_WA, dtype=jnp.int32))
    folded = grad_pad[:, :, halo_rim:halo_rim + rows_all]
    folded = folded.at[:, :, :halo_rim].add(grad_pad[:, :, halo_rim + rows_all:])
    folded = folded.at[:, :, rows_all - halo_rim:].add(grad_pad[:, :, :halo_rim])
    core = folded[:, :, :, halo_rim:halo_rim + cols_all]
    core = core.at[:, :, :, :halo_rim].add(folded[:, :, :, halo_rim + cols_all:])
    core = core.at[:, :, :, cols_all - halo_rim:].add(folded[:, :, :, :halo_rim])
    query_grad = query_tiles.reshape(N_HA, N_WA, frames, tile_side, tile_side, width)
    query_grad = query_grad.transpose(2, 0, 3, 1, 4, 5).reshape(frames, rows_all, cols_all, width)
    text_key_grad = text_total[0].reshape(TEXT, HEADS * HDIM).astype(jnp.bfloat16)
    text_value_grad = text_total[1].reshape(TEXT, HEADS * HDIM).astype(jnp.bfloat16)
    return query_grad, core[0].astype(jnp.bfloat16), core[1].astype(jnp.bfloat16), text_key_grad, text_value_grad
```

```python
import functools
import math

import jax
import jax.numpy as jnp
import numpy as np
from jax import lax
from jax.experimental import pallas as pl
from jax.experimental.pallas import tpu as pltpu
from jax.sharding import Mesh
from jax.sharding import PartitionSpec as P

HEADS = 12
HDIM = 128
TILE = 8
HALO = 2
HA = ("ha_0", "ha_1")
F32 = jnp.float32
BF16 = jnp.bfloat16
SCALE = 1.0 / math.sqrt(HDIM)

FRAMES = 2
OWN = FRAMES * TILE * TILE
SIDE = FRAMES * TILE * HALO
CORNER = HALO * HALO
BAND = HALO * TILE + 2 * CORNER
ENDS = FRAMES * BAND


def nt(a, b):
    return lax.dot_general(a, b, (((1,), (1,)), ((), ())), preferred_element_type=F32)


def nn(a, b):
    return lax.dot_general(a, b, (((1,), (0,)), ((), ())), preferred_element_type=F32)


def tn(a, b):
    return lax.dot_general(a, b, (((0,), (0,)), ((), ())), preferred_element_type=F32)


def exact(a, b):
    return lax.dot_general(
        a, b, (((1,), (0,)), ((), ())), precision=lax.Precision.HIGHEST, preferred_element_type=F32
    )


def own_row(frame, row, col):
    return frame * TILE * TILE + row * TILE + col


def side_row(frame, row, col):
    return (frame * TILE + row) * HALO + col


def select_sides():
    out = np.zeros((2, SIDE, OWN), np.float32)
    for side, first in enumerate((0, TILE - HALO)):
        for frame in range(FRAMES):
            for row in range(TILE):
                for col in range(HALO):
                    out[side, side_row(frame, row, col), own_row(frame, row, first + col)] = 1
    return out


def select_ends():
    out = np.zeros((2, ENDS, OWN + 2 * SIDE), np.float32)
    for end, first in enumerate((0, TILE - HALO)):
        for frame in range(FRAMES):
            at = frame * BAND
            for row in range(HALO):
                for col in range(TILE):
                    out[end, at, own_row(frame, first + row, col)] = 1
                    at += 1
            for side in range(2):
                for row in range(HALO):
                    for col in range(HALO):
                        out[end, at, OWN + side * SIDE + side_row(frame, first + row, col)] = 1
                        at += 1
    return out


SIDES = select_sides()
BANDS = select_ends()


def sides_kernel(select_ref, keys_ref, values_ref, left_ref, right_ref):
    for part, ref in enumerate((keys_ref, values_ref)):
        rows = ref[...]
        at = pl.ds(part * SIDE, SIDE)
        left_ref[at, :] = nn(select_ref[0], rows).astype(BF16)
        right_ref[at, :] = nn(select_ref[1], rows).astype(BF16)


def ends_kernel(select_ref, keys_ref, values_ref, left_ref, right_ref, top_ref, bottom_ref):
    for part, ref in enumerate((keys_ref, values_ref)):
        at = pl.ds(part * SIDE, SIDE)
        rows = jnp.concatenate([ref[...], left_ref[at, :], right_ref[at, :]], axis=0)
        to = pl.ds(part * ENDS, ENDS)
        top_ref[to, :] = nn(select_ref[0], rows).astype(BF16)
        bottom_ref[to, :] = nn(select_ref[1], rows).astype(BF16)


def text_kernel(
    core_ref, norm_ref, delta_ref, query_ref, out_grad_ref, key_ref, value_ref, grad_ref, stats_ref
):
    lane = lax.broadcasted_iota(jnp.int32, (8, 128), 1)
    row = lax.broadcasted_iota(jnp.int32, (8, 128), 0)
    spread = (lax.rem(lane, 8) == row).astype(F32)
    count = HEADS * 16
    wide_lane = lax.broadcasted_iota(jnp.int32, (count, 128), 1)
    wide_row = lax.broadcasted_iota(jnp.int32, (count, 128), 0)
    here = lax.div(wide_lane, 8) == lax.rem(wide_row, 16)
    head = lax.broadcasted_iota(jnp.int32, (16, count), 0)
    of = lax.div(lax.broadcasted_iota(jnp.int32, (16, count), 1), 16)
    gather = (head == of).astype(F32)
    stats = []
    for which, ref in enumerate((norm_ref, delta_ref)):
        wide = exact(ref[...], spread)
        wide = jnp.where(here, wide, 0.0)
        rows = exact(gather, wide)
        stats_ref[pl.ds(which * 16, 16), :] = rows
        stats.append(rows)
    norm, delta = stats
    core = core_ref[0]
    text = key_ref.shape[0]
    for h in range(HEADS):
        cols = slice(h * HDIM, (h + 1) * HDIM)
        q = query_ref[:, cols]
        g = out_grad_ref[:, cols]
        probs = jnp.exp(nt(key_ref[:, cols], q) * SCALE - norm[h : h + 1])
        prob_grad = nt(value_ref[:, cols], g)
        score_grad = (probs * (prob_grad - delta[h : h + 1])).astype(BF16)
        to = pl.ds(h * text, text)
        grad_ref[core, to, :] = nn(score_grad, q) * SCALE
        grad_ref[1 - core, to, :] = nn(probs.astype(BF16), g)


def video_kernel(
    live_ref,
    stats_ref,
    query_ref,
    out_grad_ref,
    keys_ref,
    values_ref,
    left_ref,
    right_ref,
    top_ref,
    bottom_ref,
    text_key_ref,
    text_value_ref,
    query_grad_ref,
    own_ref,
    left_grad_ref,
    right_grad_ref,
    top_grad_ref,
    bottom_grad_ref,
    mask_ref,
):
    text = text_key_ref.shape[0]
    parts = ((OWN, None), (SIDE, None), (SIDE, None), (ENDS, None), (ENDS, None))

    def live(block):
        return live_ref[block].astype(F32)

    mask_ref[pl.ds(0, OWN), :] = jnp.full((OWN, HDIM), live(4), F32)
    mask_ref[pl.ds(OWN, SIDE), :] = jnp.full((SIDE, HDIM), live(3), F32)
    mask_ref[pl.ds(OWN + SIDE, SIDE), :] = jnp.full((SIDE, HDIM), live(5), F32)
    band = lax.rem(lax.broadcasted_iota(jnp.int32, (ENDS, HDIM), 0), BAND)
    for end, first in ((0, 0), (1, 6)):
        at = OWN + 2 * SIDE + end * ENDS
        mask_ref[pl.ds(at, ENDS), :] = jnp.where(
            band < HALO * TILE,
            live(first + 1),
            jnp.where(band < HALO * TILE + CORNER, live(first), live(first + 2)),
        )
    window = OWN + 2 * SIDE + 2 * ENDS
    mask_ref[pl.ds(window, text), :] = jnp.ones((text, HDIM), F32)

    def rows_of(part, cols):
        side = slice(part * SIDE, (part + 1) * SIDE)
        ends = slice(part * ENDS, (part + 1) * ENDS)
        own, words = ((keys_ref, text_key_ref), (values_ref, text_value_ref))[part]
        return jnp.concatenate(
            [
                own[:, cols],
                left_ref[side, cols],
                right_ref[side, cols],
                top_ref[ends, cols],
                bottom_ref[ends, cols],
                words[:, cols],
            ],
            axis=0,
        )

    for h in range(HEADS):
        cols = slice(h * HDIM, (h + 1) * HDIM)
        q = query_ref[:, cols]
        g = out_grad_ref[:, cols]
        k = rows_of(0, cols)
        v = rows_of(1, cols)
        norm = stats_ref[h : h + 1, :]
        delta = stats_ref[16 + h : 17 + h, :]
        probs = jnp.exp(nt(k, q) * SCALE - norm) * mask_ref[...]
        score_grad = (probs * (nt(v, g) - delta)).astype(BF16)
        query_grad_ref[:, cols] = (tn(score_grad, k) * SCALE).astype(BF16)
        grads = (
            nn(score_grad[:window], q) * SCALE,
            nn(probs[:window].astype(BF16), g),
        )
        for part, grad in enumerate(grads):
            at = 0
            for ref, rows in (
                (own_ref, OWN),
                (left_grad_ref, SIDE),
                (right_grad_ref, SIDE),
                (top_grad_ref, ENDS),
                (bottom_grad_ref, ENDS),
            ):
                ref[part * rows : (part + 1) * rows, cols] = grad[at : at + rows]
                at += rows


def corners_kernel(
    select_ref, left_ref, right_ref, above_ref, below_ref, left_out_ref, right_out_ref
):
    for part in range(2):
        side = pl.ds(part * SIDE, SIDE)
        ends = pl.ds(part * ENDS, ENDS)
        bands = jnp.concatenate([above_ref[ends, :], below_ref[ends, :]], axis=0)
        left_out_ref[side, :] = left_ref[side, :] + exact(select_ref[0], bands)
        right_out_ref[side, :] = right_ref[side, :] + exact(select_ref[1], bands)


def sum_kernel(
    select_ref, own_ref, left_ref, right_ref, above_ref, below_ref, key_ref, value_ref
):
    for part, out in enumerate((key_ref, value_ref)):
        side = pl.ds(part * SIDE, SIDE)
        ends = pl.ds(part * ENDS, ENDS)
        rows = jnp.concatenate(
            [left_ref[side, :], right_ref[side, :], above_ref[ends, :], below_ref[ends, :]], axis=0
        )
        total = own_ref[pl.ds(part * OWN, OWN), :] + exact(select_ref[...], rows)
        out[...] = total.astype(BF16)


def words_kernel(parts_ref, key_ref, value_ref):
    text = key_ref.shape[0]
    rows = parts_ref.shape[1]
    for part, out in enumerate((key_ref, value_ref)):
        for h in range(HEADS):
            for at in range(0, text, 16):
                row = h * text + at
                piece = parts_ref[2 * (row // rows) + part, pl.ds(row % rows, 16), :]
                out[at : at + 16, h * HDIM : (h + 1) * HDIM] = piece


def call(kernel, outs, *args, smem=0, scratch=(), flops=1000000):
    whole = pl.BlockSpec(memory_space=pltpu.VMEM)
    scalars = pl.BlockSpec(memory_space=pltpu.SMEM)
    return pl.pallas_call(
        kernel,
        out_shape=[jax.ShapeDtypeStruct(shape, dtype) for shape, dtype in outs],
        in_specs=[scalars] * smem + [whole] * (len(args) - smem),
        out_specs=[whole] * len(outs),
        scratch_shapes=list(scratch),
        compiler_params=pltpu.CompilerParams(vmem_limit_bytes=12 * 1024 * 1024),
        cost_estimate=pl.CostEstimate(flops=flops, bytes_accessed=1000000, transcendentals=0),
        name=kernel.__name__,
    )(*args)


def shifted(value, axis, steps):
    count = lax.axis_size(axis)
    return lax.ppermute(value, axis, [(i, (i + steps) % count) for i in range(count)])


def to_first(value, axis):
    count = lax.axis_size(axis)
    step = 1
    while step < count:
        pairs = [(i, (i + step) % count) for i in range(step, count, 2 * step)]
        value = value + lax.ppermute(value, axis, pairs)
        step *= 2
    return value


def from_first(value, axis):
    count = lax.axis_size(axis)
    value = jnp.where(lax.axis_index(axis) == 0, value, jnp.zeros_like(value))
    step = count // 2
    while step:
        pairs = [(i, i + step) for i in range(0, count, 2 * step)]
        value = value + lax.ppermute(value, axis, pairs)
        step //= 2
    return value


def local(
    queries, keys, values, out_grad, log_norm, delta_rows, text_keys, text_values, window_table
):
    shape = queries.shape
    width = shape[-1]
    text = text_keys.shape[0]
    q = queries.reshape(OWN, width)
    g = out_grad.reshape(OWN, width)
    k = keys.reshape(OWN, width)
    v = values.reshape(OWN, width)
    anchor = jnp.zeros((), jnp.int32)
    live = lax.dynamic_slice(
        window_table, (lax.axis_index(HA), lax.axis_index("wa"), anchor), (1, 1, 9)
    ).reshape(9)
    core = lax.axis_index("ha_1").reshape(1)

    words, stats = call(
        text_kernel,
        [((2, HEADS * text, HDIM), F32), ((32, HDIM), F32)],
        core,
        log_norm.reshape(-1, TILE),
        delta_rows.reshape(-1, TILE),
        q,
        g,
        text_keys,
        text_values,
        smem=1,
    )

    left, right = call(
        sides_kernel,
        [((2 * SIDE, width), BF16)] * 2,
        jnp.asarray(SIDES, BF16),
        k,
        v,
    )
    from_right = shifted(left, "wa", -1)
    from_left = shifted(right, "wa", 1)

    half = words[0] + shifted(words[1], "ha_1", 1)
    pieces = lax.all_to_all(half, "ha_0", 0, 0, tiled=True)
    piece = pieces.reshape(lax.axis_size("ha_0"), -1, HDIM).sum(axis=0)
    piece = to_first(piece, "wa")

    top, bottom = call(
        ends_kernel,
        [((2 * ENDS, width), BF16)] * 2,
        jnp.asarray(BANDS, BF16),
        k,
        v,
        from_left,
        from_right,
    )
    from_below = shifted(top, HA, -1)
    from_above = shifted(bottom, HA, 1)
    query_grad, own, left_grad, right_grad, top_grad, bottom_grad = call(
        video_kernel,
        [
            ((OWN, width), BF16),
            ((2 * OWN, width), F32),
            ((2 * SIDE, width), F32),
            ((2 * SIDE, width), F32),
            ((2 * ENDS, width), F32),
            ((2 * ENDS, width), F32),
        ],
        live,
        stats,
        q,
        g,
        k,
        v,
        from_left,
        from_right,
        from_above,
        from_below,
        text_keys,
        text_values,
        smem=1,
        scratch=[pltpu.VMEM((OWN + 2 * SIDE + 2 * ENDS + text, HDIM), F32)],
    )
    above = shifted(bottom_grad, HA, 1)
    below = shifted(top_grad, HA, -1)
    back = np.concatenate([BANDS[0].T, BANDS[1].T], axis=1)
    left_grad, right_grad = call(
        corners_kernel,
        [((2 * SIDE, width), F32)] * 2,
        jnp.asarray(np.stack([back[OWN : OWN + SIDE], back[OWN + SIDE :]]), F32),
        left_grad,
        right_grad,
        above,
        below,
    )
    after = shifted(left_grad, "wa", -1)
    before = shifted(right_grad, "wa", 1)
    back = np.concatenate([SIDES[0].T, SIDES[1].T, back[:OWN]], axis=1)
    key_grad, value_grad = call(
        sum_kernel,
        [((OWN, width), BF16)] * 2,
        jnp.asarray(back, F32),
        own,
        before,
        after,
        above,
        below,
    )

    piece = from_first(piece.astype(BF16), "wa")
    count = lax.axis_size(HA)
    pieces = lax.all_to_all(jnp.tile(piece, (count, 1)), HA, 0, 0, tiled=True)
    text_key_grad, text_value_grad = call(
        words_kernel,
        [((text, width), BF16)] * 2,
        pieces.reshape(count, -1, HDIM),
    )
    return (
        query_grad.reshape(shape),
        key_grad.reshape(shape),
        value_grad.reshape(shape),
        text_key_grad,
        text_value_grad,
    )


def solution(mesh):
    split = Mesh(
        mesh.devices.reshape(mesh.shape["group"], 8, 2, mesh.shape["wa"]),
        ("group", "ha_0", "ha_1", "wa"),
    )
    return jax.shard_map(
        local,
        mesh=split,
        in_specs=(
            P("group", HA, "wa", None),
            P("group", HA, "wa", None),
            P("group", HA, "wa", None),
            P("group", HA, "wa", None),
            P(None, "group", HA, "wa"),
            P(None, "group", HA, "wa"),
            P("group", None),
            P("group", None),
            P(),
        ),
        out_specs=(
            P("group", HA, "wa", None),
            P("group", HA, "wa", None),
            P("group", HA, "wa", None),
            P("group", None),
            P("group", None),
        ),
        check_vma=False,
    )
```

```python
import math

import jax
import jax.numpy as jnp
import numpy as np
from jax import lax
from jax.experimental import pallas as pl
from jax.experimental.pallas import tpu as pltpu
from jax.sharding import Mesh
from jax.sharding import PartitionSpec as P


HEADS = 12
HDIM = 128
TILE = 8
HALO = 2
HA = ("ha_0", "ha_1")
F32 = jnp.float32
BF16 = jnp.bfloat16
SCALE = 1.0 / math.sqrt(HDIM)

FRAMES = 2
OWN = FRAMES * TILE * TILE
SIDE = FRAMES * TILE * HALO
CORNER = HALO * HALO
BAND = HALO * TILE + 2 * CORNER
ENDS = FRAMES * BAND


def nt(a, b):
    return lax.dot_general(a, b, (((1,), (1,)), ((), ())), preferred_element_type=F32)


def nn(a, b):
    return lax.dot_general(a, b, (((1,), (0,)), ((), ())), preferred_element_type=F32)


def tn(a, b):
    return lax.dot_general(a, b, (((0,), (0,)), ((), ())), preferred_element_type=F32)


def exact(a, b):
    return lax.dot_general(
        a, b, (((1,), (0,)), ((), ())), precision=lax.Precision.HIGHEST, preferred_element_type=F32
    )


def own_row(frame, row, col):
    return frame * TILE * TILE + row * TILE + col


def side_row(frame, row, col):
    return (frame * TILE + row) * HALO + col


def select_sides():
    out = np.zeros((2, SIDE, OWN), np.float32)
    for side, first in enumerate((0, TILE - HALO)):
        for frame in range(FRAMES):
            for row in range(TILE):
                for col in range(HALO):
                    out[side, side_row(frame, row, col), own_row(frame, row, first + col)] = 1
    return out


def select_ends():
    out = np.zeros((2, ENDS, OWN + 2 * SIDE), np.float32)
    for end, first in enumerate((0, TILE - HALO)):
        for frame in range(FRAMES):
            at = frame * BAND
            for row in range(HALO):
                for col in range(TILE):
                    out[end, at, own_row(frame, first + row, col)] = 1
                    at += 1
            for side in range(2):
                for row in range(HALO):
                    for col in range(HALO):
                        out[end, at, OWN + side * SIDE + side_row(frame, first + row, col)] = 1
                        at += 1
    return out


SIDES = select_sides()
BANDS = select_ends()


GROUP = 4


def sides_kernel(ready, done, select_ref, keys_ref, values_ref, left_ref, right_ref):
    for h in range(0, HEADS, GROUP):
        ready(h)
        cols = slice(h * HDIM, (h + GROUP) * HDIM)
        for part, ref in enumerate((keys_ref, values_ref)):
            rows = ref[:, cols]
            at = slice(part * SIDE, (part + 1) * SIDE)
            left_ref[at, cols] = nn(select_ref[0], rows).astype(BF16)
            right_ref[at, cols] = nn(select_ref[1], rows).astype(BF16)
        done(h)


def ends_kernel(
    ready, done, select_ref, keys_ref, values_ref, left_ref, right_ref, top_ref, bottom_ref
):
    for h in range(0, HEADS, GROUP):
        ready(h)
        cols = slice(h * HDIM, (h + GROUP) * HDIM)
        for part, ref in enumerate((keys_ref, values_ref)):
            at = slice(part * SIDE, (part + 1) * SIDE)
            rows = jnp.concatenate([ref[:, cols], left_ref[at, cols], right_ref[at, cols]], axis=0)
            to = slice(part * ENDS, (part + 1) * ENDS)
            top_ref[to, cols] = nn(select_ref[0], rows).astype(BF16)
            bottom_ref[to, cols] = nn(select_ref[1], rows).astype(BF16)
        done(h)


def text_kernel(
    ready, done, norm_ref, delta_ref, query_ref, out_grad_ref, key_ref, value_ref, grad_ref, stats_ref
):
    heads = lax.broadcasted_iota(jnp.int32, (16, HEADS), 1)
    identity = (heads == lax.broadcasted_iota(jnp.int32, (16, HEADS), 0)).astype(F32)
    stats = []
    for which, ref in enumerate((norm_ref, delta_ref)):
        rows = lax.dot_general(
            identity,
            ref[...],
            (((1,), (1,)), ((), ())),
            precision=lax.Precision.HIGHEST,
            preferred_element_type=F32,
        )
        stats_ref[which * 16 : (which + 1) * 16, :] = rows
        stats.append(rows)
    norm, delta = stats
    text = key_ref.shape[0]
    piece = grad_ref.shape[0] // 16
    for h in range(HEADS):
        ready(h)
        cols = slice(h * HDIM, (h + 1) * HDIM)
        q = query_ref[:, cols]
        g = out_grad_ref[:, cols]
        probs = jnp.exp(nt(key_ref[:, cols], q) * SCALE - norm[h : h + 1])
        prob_grad = nt(value_ref[:, cols], g)
        score_grad = (probs * (prob_grad - delta[h : h + 1])).astype(BF16)
        for part, grad in enumerate((nn(score_grad, q) * SCALE, nn(probs.astype(BF16), g))):
            for at in range(0, text, 16):
                chip, within = divmod(h * text + at, piece)
                to = (2 * chip + part) * piece + within
                grad_ref[to : to + 16, :] = grad[at : at + 16]


def backward(q, g, k, v, norm, delta, live):
    probs = jnp.exp(nt(k, q) * SCALE - norm)
    if live is not None:
        probs = probs * live
    score_grad = (probs * (nt(v, g) - delta)).astype(BF16)
    return probs.astype(BF16), score_grad


def own_kernel(
    ready,
    done,
    live_ref,
    stats_ref,
    query_ref,
    out_grad_ref,
    keys_ref,
    values_ref,
    text_key_ref,
    text_value_ref,
    query_grad_ref,
    own_ref,
):
    text = text_key_ref.shape[0]
    rows = lax.broadcasted_iota(jnp.int32, (OWN + text, HDIM), 0)
    live = jnp.where(rows < OWN, live_ref[4].astype(F32), 1.0)
    for h in range(HEADS):
        ready(h)
        cols = slice(h * HDIM, (h + 1) * HDIM)
        q = query_ref[:, cols]
        g = out_grad_ref[:, cols]
        k = jnp.concatenate([keys_ref[:, cols], text_key_ref[:, cols]], axis=0)
        v = jnp.concatenate([values_ref[:, cols], text_value_ref[:, cols]], axis=0)
        norm = stats_ref[h : h + 1, :]
        delta = stats_ref[16 + h : 17 + h, :]
        probs, score_grad = backward(q, g, k, v, norm, delta, live)
        query_grad_ref[:, cols] = tn(score_grad, k)
        own_ref[:OWN, cols] = nn(score_grad[:OWN], q) * SCALE
        own_ref[OWN:, cols] = nn(probs[:OWN], g)
        done(h)


def halo_kernel(
    ready,
    done,
    live_ref,
    stats_ref,
    query_ref,
    out_grad_ref,
    left_ref,
    right_ref,
    top_ref,
    bottom_ref,
    part_ref,
    top_grad_ref,
    bottom_grad_ref,
    left_grad_ref,
    right_grad_ref,
    query_grad_ref,
    mask_ref,
):
    def live(block):
        return live_ref[block].astype(F32)

    band = lax.rem(lax.broadcasted_iota(jnp.int32, (ENDS, HDIM), 0), BAND)
    for end, first in ((0, 0), (1, 6)):
        mask_ref[end * ENDS : (end + 1) * ENDS, :] = jnp.where(
            band < HALO * TILE,
            live(first + 1),
            jnp.where(band < HALO * TILE + CORNER, live(first), live(first + 2)),
        )
    at = 2 * ENDS
    mask_ref[at : at + SIDE, :] = jnp.full((SIDE, HDIM), live(3), F32)
    mask_ref[at + SIDE : at + 2 * SIDE, :] = jnp.full((SIDE, HDIM), live(5), F32)
    for h in range(HEADS):
        ready(h)
        cols = slice(h * HDIM, (h + 1) * HDIM)
        q = query_ref[:, cols]
        g = out_grad_ref[:, cols]
        k, v = (
            jnp.concatenate(
                [
                    top_ref[part * ENDS : (part + 1) * ENDS, cols],
                    bottom_ref[part * ENDS : (part + 1) * ENDS, cols],
                    left_ref[part * SIDE : (part + 1) * SIDE, cols],
                    right_ref[part * SIDE : (part + 1) * SIDE, cols],
                ],
                axis=0,
            )
            for part in range(2)
        )
        norm = stats_ref[h : h + 1, :]
        delta = stats_ref[16 + h : 17 + h, :]
        probs, score_grad = backward(q, g, k, v, norm, delta, mask_ref[...])
        query_grad = (part_ref[:, cols] + tn(score_grad, k)) * SCALE
        query_grad_ref[:, cols] = query_grad.astype(BF16)
        for part, grad in enumerate((nn(score_grad, q) * SCALE, nn(probs, g))):
            at = 0
            for ref, rows in (
                (top_grad_ref, ENDS),
                (bottom_grad_ref, ENDS),
                (left_grad_ref, SIDE),
                (right_grad_ref, SIDE),
            ):
                ref[part * rows : (part + 1) * rows, cols] = grad[at : at + rows]
                at += rows
        done(h)


def corners_kernel(
    ready, done, select_ref, left_ref, right_ref, above_ref, below_ref, left_out_ref, right_out_ref
):
    for h in range(0, HEADS, GROUP):
        ready(h)
        cols = slice(h * HDIM, (h + GROUP) * HDIM)
        for part in range(2):
            side = slice(part * SIDE, (part + 1) * SIDE)
            ends = slice(part * ENDS, (part + 1) * ENDS)
            bands = jnp.concatenate([above_ref[ends, cols], below_ref[ends, cols]], axis=0)
            more = exact(select_ref[...], bands)
            left_out_ref[side, cols] = left_ref[side, cols] + more[:SIDE]
            right_out_ref[side, cols] = right_ref[side, cols] + more[SIDE:]
        done(h)


def bands_kernel(ready, done, own_ref, above_ref, below_ref, out_ref):
    for h in range(0, HEADS, GROUP):
        ready(h)
        cols = slice(h * HDIM, (h + GROUP) * HDIM)
        out_ref[:, cols] = own_ref[:, cols]
        for part in range(2):
            for frame in range(FRAMES):
                to = part * OWN + frame * TILE * TILE
                at = part * ENDS + frame * BAND
                rows = HALO * TILE
                out_ref[to : to + rows, cols] += above_ref[at : at + rows, cols]
                end = to + (TILE - HALO) * TILE
                out_ref[end : end + rows, cols] += below_ref[at : at + rows, cols]
        done(h)


def sum_kernel(ready, done, select_ref, own_ref, left_ref, right_ref, key_ref, value_ref):
    for h in range(0, HEADS, GROUP):
        ready(h)
        cols = slice(h * HDIM, (h + GROUP) * HDIM)
        for part, out in enumerate((key_ref, value_ref)):
            side = slice(part * SIDE, (part + 1) * SIDE)
            rows = jnp.concatenate([left_ref[side, cols], right_ref[side, cols]], axis=0)
            total = own_ref[part * OWN : (part + 1) * OWN, cols] + exact(select_ref[...], rows)
            out[:, cols] = total.astype(BF16)
        done(h)


def words_kernel(ready, done, parts_ref, key_ref, value_ref):
    text = key_ref.shape[0]
    rows = parts_ref.shape[1]
    for part, out in enumerate((key_ref, value_ref)):
        for h in range(HEADS):
            for at in range(0, text, 16):
                chip, within = divmod(h * text + at, rows)
                piece = parts_ref[2 * chip + part, within : within + 16, :]
                out[at : at + 16, h * HDIM : (h + 1) * HDIM] = piece


def call(kernel, outs, ins, scratch=(), us=1.0, room=0.0):
    spaces = {"s": pltpu.SMEM, "v": pltpu.VMEM, "h": pltpu.HBM}
    n_in, n_out = len(ins), len(outs)
    shapes = [(a.shape, a.dtype) for a, _ in ins] + [(shape, dtype) for shape, dtype, _ in outs]
    places = [place for _, place in ins] + [place for _, _, place in outs]
    held = [i for i, place in enumerate(places) if place == "h"]
    groups = HEADS // GROUP

    def pieces(i):
        shape, _ = shapes[i]
        if len(shape) == 2 and shape[1] == HEADS * HDIM:
            step = GROUP * HDIM
            return [(slice(None), slice(n * step, (n + 1) * step)) for n in range(groups)]
        return [(Ellipsis,)]

    def body(*refs):
        here = list(refs[: n_in + n_out])
        buffers = refs[n_in + n_out : n_in + n_out + len(held)]
        semaphores = refs[n_in + n_out + len(held)]
        rest = refs[n_in + n_out + len(held) + 1 :]
        arriving, leaving, started = [], [], []
        for n, i in enumerate(held):
            far, near = here[i], buffers[n]
            for m, at in enumerate(pieces(i)):
                source, target = (far, near) if i < n_in else (near, far)
                copy = pltpu.make_async_copy(source.at[at], target.at[at], semaphores.at[n, m])
                (arriving if i < n_in else leaving).append((m, len(pieces(i)), copy))
            here[i] = near
        for group in range(groups):
            for m, _, copy in arriving:
                if m == group:
                    copy.start()
        for _, count, copy in arriving:
            if count == 1:
                copy.wait()

        def ready(h):
            if h % GROUP == 0:
                for m, count, copy in arriving:
                    if count > 1 and m == h // GROUP:
                        copy.wait()

        def done(h):
            if h % GROUP == GROUP - 1 or h % GROUP == 0 and kernel in whole_groups:
                for m, count, copy in leaving:
                    if count > 1 and m == h // GROUP:
                        copy.start()
                        started.append(copy)

        kernel(ready, done, *here, *rest)
        for _, _, copy in leaving:
            if all(copy is not other for other in started):
                copy.start()
        for _, _, copy in leaving:
            copy.wait()

    return pl.pallas_call(
        body,
        out_shape=[jax.ShapeDtypeStruct(shape, dtype) for shape, dtype, _ in outs],
        in_specs=[pl.BlockSpec(memory_space=spaces[place]) for _, place in ins],
        out_specs=[pl.BlockSpec(memory_space=spaces[place]) for _, _, place in outs],
        scratch_shapes=[
            *(pltpu.VMEM(*shapes[i]) for i in held),
            pltpu.SemaphoreType.DMA((max(len(held), 1), groups)),
            *scratch,
        ],
        compiler_params=pltpu.CompilerParams(vmem_limit_bytes=int((60.5 - room) * 2**20)),
        cost_estimate=pl.CostEstimate(
            flops=int(us * FLOPS_PER_US), bytes_accessed=1000000, transcendentals=0
        ),
    )(*(a for a, _ in ins))


FLOPS_PER_US = 50000000
whole_groups = (sides_kernel, ends_kernel, corners_kernel, bands_kernel, sum_kernel)


def shifted(value, axis, steps):
    count = lax.axis_size(axis)
    return lax.ppermute(value, axis, [(i, (i + steps) % count) for i in range(count)])


def by_query(rows):
    return rows.transpose(1, 2, 3, 0).reshape(OWN, HEADS)


def to_all(value, axis):
    count = lax.axis_size(axis)
    everyone = jnp.broadcast_to(value[None], (count, *value.shape))
    return lax.all_to_all(everyone, axis, 0, 0, tiled=True)


def local(
    queries, keys, values, out_grad, log_norm, delta_rows, text_keys, text_values, window_table
):
    shape = queries.shape
    width = shape[-1]
    text = text_keys.shape[0]
    q = queries.reshape(OWN, width)
    g = out_grad.reshape(OWN, width)
    k = keys.reshape(OWN, width)
    v = values.reshape(OWN, width)
    anchor = jnp.zeros((), jnp.int32)
    live = lax.dynamic_slice(
        window_table, (lax.axis_index(HA), lax.axis_index("wa"), anchor), (1, 1, 9)
    ).reshape(9)

    words, stats = call(
        text_kernel,
        [((2 * HEADS * text, HDIM), F32, "h"), ((32, HDIM), F32, "h")],
        [
            (by_query(log_norm), "h"),
            (by_query(delta_rows), "h"),
            (q, "h"),
            (g, "h"),
            (text_keys, "h"),
            (text_values, "h"),
        ],
        us=3,
    )
    count = lax.axis_size(HA)
    words = lax.all_to_all(words.reshape(count, -1, HDIM), HA, 0, 0, tiled=True)
    piece = words.sum(axis=0)
    pieces = to_all(piece, "wa")
    piece = pieces.sum(axis=0).astype(BF16)
    pieces = to_all(piece, HA)
    text_key_grad, text_value_grad = call(
        words_kernel, [((text, width), BF16, "h")] * 2, [(pieces, "h")]
    )

    left, right = call(
        sides_kernel,
        [((2 * SIDE, width), BF16, "h")] * 2,
        [(jnp.asarray(SIDES, BF16), "h"), (k, "h"), (v, "h")],
    )
    from_right = shifted(left, "wa", -1)
    from_left = shifted(right, "wa", 1)
    part, own = call(
        own_kernel,
        [((OWN, width), F32, "h"), ((2 * OWN, width), F32, "h")],
        [
            (live, "s"),
            (stats, "h"),
            (q, "h"),
            (g, "h"),
            (k, "h"),
            (v, "h"),
            (text_keys, "h"),
            (text_values, "h"),
        ],
        us=3,
    )
    top, bottom = call(
        ends_kernel,
        [((2 * ENDS, width), BF16, "h")] * 2,
        [(jnp.asarray(BANDS, BF16), "h"), (k, "h"), (v, "h"), (from_left, "v"), (from_right, "v")],
        room=2.0,
    )
    from_below = shifted(top, HA, -1)
    from_above = shifted(bottom, HA, 1)
    top_grad, bottom_grad, left_grad, right_grad, query_grad = call(
        halo_kernel,
        [((2 * ENDS, width), F32, "v")] * 2
        + [((2 * SIDE, width), F32, "v")] * 2
        + [((OWN, width), BF16, "h")],
        [
            (live, "s"),
            (stats, "h"),
            (q, "h"),
            (g, "h"),
            (from_left, "h"),
            (from_right, "h"),
            (from_above, "h"),
            (from_below, "h"),
            (part, "h"),
        ],
        scratch=[pltpu.VMEM((2 * ENDS + 2 * SIDE, HDIM), F32)],
        us=3,
        room=6.0,
    )
    above = shifted(bottom_grad, HA, 1)
    below = shifted(top_grad, HA, -1)
    back = np.concatenate([BANDS[0].T, BANDS[1].T], axis=1)
    left_grad, right_grad = call(
        corners_kernel,
        [((2 * SIDE, width), F32, "h")] * 2,
        [
            (jnp.asarray(back[OWN:], F32), "h"),
            (left_grad, "v"),
            (right_grad, "v"),
            (above, "v"),
            (below, "v"),
        ],
        room=6.0,
    )
    after = shifted(left_grad, "wa", -1)
    before = shifted(right_grad, "wa", 1)
    (own,) = call(
        bands_kernel,
        [((2 * OWN, width), F32, "h")],
        [(own, "h"), (above, "v"), (below, "v")],
        room=6.0,
    )
    back = np.concatenate([SIDES[0].T, SIDES[1].T], axis=1)
    key_grad, value_grad = call(
        sum_kernel,
        [((OWN, width), BF16, "h")] * 2,
        [(jnp.asarray(back, F32), "h"), (own, "h"), (before, "h"), (after, "h")],
    )
    return (
        query_grad.reshape(shape),
        key_grad.reshape(shape),
        value_grad.reshape(shape),
        text_key_grad,
        text_value_grad,
    )


def solution(mesh):
    split = Mesh(
        mesh.devices.reshape(mesh.shape["group"], 8, 2, mesh.shape["wa"]),
        ("group", "ha_0", "ha_1", "wa"),
    )
    return jax.shard_map(
        local,
        mesh=split,
        in_specs=(
            P("group", HA, "wa", None),
            P("group", HA, "wa", None),
            P("group", HA, "wa", None),
            P("group", HA, "wa", None),
            P(None, "group", HA, "wa"),
            P(None, "group", HA, "wa"),
            P("group", None),
            P("group", None),
            P(),
        ),
        out_specs=(
            P("group", HA, "wa", None),
            P("group", HA, "wa", None),
            P("group", HA, "wa", None),
            P("group", None),
            P("group", None),
        ),
        check_vma=False,
    )
```

```python
import math

import jax
import jax.numpy as jnp
import numpy as np
from jax import lax
from jax.experimental import pallas as pl
from jax.experimental.pallas import tpu as pltpu
from jax.sharding import Mesh
from jax.sharding import PartitionSpec as P


HEADS = 12
HDIM = 128
TILE = 8
HALO = 2
HA = ("ha_0", "ha_1")
F32 = jnp.float32
BF16 = jnp.bfloat16
SCALE = 1.0 / math.sqrt(HDIM)

FRAMES = 2
OWN = FRAMES * TILE * TILE
SIDE = FRAMES * TILE * HALO
CORNER = HALO * HALO
BAND = HALO * TILE + 2 * CORNER
ENDS = FRAMES * BAND


def nt(a, b):
    return lax.dot_general(a, b, (((1,), (1,)), ((), ())), preferred_element_type=F32)


def nn(a, b):
    return lax.dot_general(a, b, (((1,), (0,)), ((), ())), preferred_element_type=F32)


def tn(a, b):
    return lax.dot_general(a, b, (((0,), (0,)), ((), ())), preferred_element_type=F32)


def exact(a, b):
    return lax.dot_general(
        a, b, (((1,), (0,)), ((), ())), precision=lax.Precision.HIGHEST, preferred_element_type=F32
    )


def own_row(frame, row, col):
    return frame * TILE * TILE + row * TILE + col


def side_row(frame, row, col):
    return (frame * TILE + row) * HALO + col


def select_sides():
    out = np.zeros((2, SIDE, OWN), np.float32)
    for side, first in enumerate((0, TILE - HALO)):
        for frame in range(FRAMES):
            for row in range(TILE):
                for col in range(HALO):
                    out[side, side_row(frame, row, col), own_row(frame, row, first + col)] = 1
    return out


def select_ends():
    out = np.zeros((2, ENDS, OWN + 2 * SIDE), np.float32)
    for end, first in enumerate((0, TILE - HALO)):
        for frame in range(FRAMES):
            at = frame * BAND
            for row in range(HALO):
                for col in range(TILE):
                    out[end, at, own_row(frame, first + row, col)] = 1
                    at += 1
            for side in range(2):
                for row in range(HALO):
                    for col in range(HALO):
                        out[end, at, OWN + side * SIDE + side_row(frame, first + row, col)] = 1
                        at += 1
    return out


SIDES = select_sides()
BANDS = select_ends()


GROUP = 4


def ends_kernel(select_ref, keys_ref, values_ref, left_ref, right_ref, top_ref, bottom_ref):
    for part, ref in enumerate((keys_ref, values_ref)):
        at = slice(part * SIDE, (part + 1) * SIDE)
        rows = jnp.concatenate([ref[...], left_ref[at, :], right_ref[at, :]], axis=0)
        to = slice(part * ENDS, (part + 1) * ENDS)
        top_ref[to, :] = nn(select_ref[0], rows).astype(BF16)
        bottom_ref[to, :] = nn(select_ref[1], rows).astype(BF16)


def first_kernel(
    ready,
    select_ref,
    keys_ref,
    values_ref,
    norm_ref,
    delta_ref,
    query_ref,
    out_grad_ref,
    key_ref,
    value_ref,
    left_ref,
    right_ref,
    grad_ref,
    stats_ref,
):
    for h in range(0, HEADS, GROUP):
        ready(h, 0)
        cols = slice(h * HDIM, (h + GROUP) * HDIM)
        for part, ref in enumerate((keys_ref, values_ref)):
            rows = ref[:, cols]
            at = slice(part * SIDE, (part + 1) * SIDE)
            left_ref[at, cols] = nn(select_ref[0], rows).astype(BF16)
            right_ref[at, cols] = nn(select_ref[1], rows).astype(BF16)
    heads = lax.broadcasted_iota(jnp.int32, (16, HEADS), 1)
    identity = (heads == lax.broadcasted_iota(jnp.int32, (16, HEADS), 0)).astype(F32)
    stats = []
    for which, ref in enumerate((norm_ref, delta_ref)):
        rows = lax.dot_general(
            identity,
            ref[...],
            (((1,), (1,)), ((), ())),
            precision=lax.Precision.HIGHEST,
            preferred_element_type=F32,
        )
        stats_ref[which * 16 : (which + 1) * 16, :] = rows
        stats.append(rows)
    norm, delta = stats
    text = key_ref.shape[0]
    piece = grad_ref.shape[0] // 16
    for h in range(HEADS):
        ready(h, 1)
        cols = slice(h * HDIM, (h + 1) * HDIM)
        q = query_ref[:, cols]
        g = out_grad_ref[:, cols]
        probs = jnp.exp(nt(key_ref[:, cols], q) * SCALE - norm[h : h + 1])
        prob_grad = nt(value_ref[:, cols], g)
        score_grad = (probs * (prob_grad - delta[h : h + 1])).astype(BF16)
        for part, grad in enumerate((nn(score_grad, q) * SCALE, nn(probs.astype(BF16), g))):
            for at in range(0, text, 16):
                chip, within = divmod(h * text + at, piece)
                to = (2 * chip + part) * piece + within
                grad_ref[to : to + 16, :] = grad[at : at + 16]


def backward(q, g, k, v, norm, delta, live):
    probs = jnp.exp(nt(k, q) * SCALE - norm)
    if live is not None:
        probs = probs * live
    score_grad = (probs * (nt(v, g) - delta)).astype(BF16)
    return probs.astype(BF16), score_grad


def own_kernel(
    live_ref,
    stats_ref,
    query_ref,
    out_grad_ref,
    keys_ref,
    values_ref,
    text_key_ref,
    text_value_ref,
    query_grad_ref,
    own_ref,
):
    text = text_key_ref.shape[0]
    rows = lax.broadcasted_iota(jnp.int32, (OWN + text, HDIM), 0)
    live = jnp.where(rows < OWN, live_ref[4].astype(F32), 1.0)
    for h in range(HEADS):
        cols = slice(h * HDIM, (h + 1) * HDIM)
        q = query_ref[:, cols]
        g = out_grad_ref[:, cols]
        k = jnp.concatenate([keys_ref[:, cols], text_key_ref[:, cols]], axis=0)
        v = jnp.concatenate([values_ref[:, cols], text_value_ref[:, cols]], axis=0)
        norm = stats_ref[h : h + 1, :]
        delta = stats_ref[16 + h : 17 + h, :]
        probs, score_grad = backward(q, g, k, v, norm, delta, live)
        query_grad_ref[:, cols] = tn(score_grad, k)
        own_ref[:OWN, cols] = nn(score_grad[:OWN], q) * SCALE
        own_ref[OWN:, cols] = nn(probs[:OWN], g)


def band_kernel(
    live_ref,
    stats_ref,
    query_ref,
    out_grad_ref,
    top_ref,
    bottom_ref,
    part_ref,
    top_grad_ref,
    bottom_grad_ref,
    query_grad_ref,
):
    def live(block):
        return live_ref[block].astype(F32)

    band = lax.rem(lax.broadcasted_iota(jnp.int32, (ENDS, HDIM), 0), BAND)
    lives = [
        jnp.where(
            band < HALO * TILE,
            live(first + 1),
            jnp.where(band < HALO * TILE + CORNER, live(first), live(first + 2)),
        )
        for first in (0, 6)
    ]
    two_halves(
        (stats_ref, query_ref, out_grad_ref, top_ref, bottom_ref, part_ref),
        (top_grad_ref, bottom_grad_ref, query_grad_ref),
        jnp.concatenate(lives, axis=0),
        1.0,
    )


def side_kernel(
    live_ref,
    stats_ref,
    query_ref,
    out_grad_ref,
    left_ref,
    right_ref,
    part_ref,
    left_grad_ref,
    right_grad_ref,
    query_grad_ref,
):
    rows = lax.broadcasted_iota(jnp.int32, (2 * SIDE, HDIM), 0)
    lives = jnp.where(rows < SIDE, live_ref[3].astype(F32), live_ref[5].astype(F32))
    two_halves(
        (stats_ref, query_ref, out_grad_ref, left_ref, right_ref, part_ref),
        (left_grad_ref, right_grad_ref, query_grad_ref),
        lives,
        SCALE,
    )


def two_halves(given, made, live, scale):
    stats_ref, query_ref, out_grad_ref, first_ref, second_ref, part_ref = given
    first_grad_ref, second_grad_ref, query_grad_ref = made
    rows = first_ref.shape[0] // 2
    for h in range(HEADS):
        cols = slice(h * HDIM, (h + 1) * HDIM)
        q = query_ref[:, cols]
        g = out_grad_ref[:, cols]
        k, v = (
            jnp.concatenate([first_ref[at, cols], second_ref[at, cols]], axis=0)
            for at in (slice(0, rows), slice(rows, 2 * rows))
        )
        norm = stats_ref[h : h + 1, :]
        delta = stats_ref[16 + h : 17 + h, :]
        probs, score_grad = backward(q, g, k, v, norm, delta, live)
        query_grad = part_ref[:, cols] + tn(score_grad, k)
        query_grad_ref[:, cols] = (query_grad * scale).astype(query_grad_ref.dtype)
        for at, grad in ((slice(0, rows), nn(score_grad, q) * SCALE), (slice(rows, 2 * rows), nn(probs, g))):
            first_grad_ref[at, cols] = grad[:rows]
            second_grad_ref[at, cols] = grad[rows:]


def corners_kernel(
    select_ref, left_ref, right_ref, above_ref, below_ref, left_out_ref, right_out_ref
):
    for part in range(2):
        side = slice(part * SIDE, (part + 1) * SIDE)
        ends = slice(part * ENDS, (part + 1) * ENDS)
        bands = jnp.concatenate([above_ref[ends, :], below_ref[ends, :]], axis=0)
        more = exact(select_ref[...], bands)
        left_out_ref[side, :] = left_ref[side, :] + more[:SIDE]
        right_out_ref[side, :] = right_ref[side, :] + more[SIDE:]


def sum_kernel(
    select_ref, own_ref, left_ref, right_ref, above_ref, below_ref, key_ref, value_ref
):
    edge = HALO * TILE
    for part, out in enumerate((key_ref, value_ref)):
        side = slice(part * SIDE, (part + 1) * SIDE)
        rows = jnp.concatenate([left_ref[side, :], right_ref[side, :]], axis=0)
        total = own_ref[part * OWN : (part + 1) * OWN, :] + exact(select_ref[...], rows)
        for frame in range(FRAMES):
            at = part * ENDS + frame * BAND
            top = frame * TILE * TILE
            bottom = top + TILE * TILE - edge
            end = top + TILE * TILE
            out[top : top + edge, :] = (
                total[top : top + edge] + above_ref[at : at + edge, :]
            ).astype(BF16)
            out[top + edge : bottom, :] = total[top + edge : bottom].astype(BF16)
            out[bottom:end, :] = (total[bottom:end] + below_ref[at : at + edge, :]).astype(BF16)


def words_kernel(parts_ref, key_ref, value_ref):
    text = key_ref.shape[0]
    rows = parts_ref.shape[1]
    for part, out in enumerate((key_ref, value_ref)):
        for h in range(HEADS):
            for at in range(0, text, 16):
                chip, within = divmod(h * text + at, rows)
                piece = parts_ref[2 * chip + part, within : within + 16, :]
                out[at : at + 16, h * HDIM : (h + 1) * HDIM] = piece


def call(kernel, outs, ins, us=1.0, smem=0, early=None):
    groups = HEADS // GROUP
    step = GROUP * HDIM

    def body(*refs):
        n = len(ins)
        outputs = refs[n : n + len(outs)]
        buffers = refs[n + len(outs) : -1]
        semaphores = refs[-1]
        small, wide = [], {}
        for i, (far, near) in enumerate(zip(refs[:n], buffers)):
            if ins[i].ndim == 2 and ins[i].shape[1] == groups * step:
                for m in range(groups):
                    at = (slice(None), slice(m * step, (m + 1) * step))
                    copy = pltpu.make_async_copy(far.at[at], near.at[at], semaphores.at[i, m])
                    wide.setdefault((int(i >= early), m), []).append(copy)
            else:
                small.append(pltpu.make_async_copy(far, near, semaphores.at[i, 0]))
        for copies in (small, *(wide[key] for key in sorted(wide))):
            for copy in copies:
                copy.start()
        for copy in small:
            copy.wait()

        def ready(h, part):
            if h % GROUP == 0:
                for copy in wide[part, h // GROUP]:
                    copy.wait()

        kernel(ready, *buffers, *outputs)

    here = pl.BlockSpec(memory_space=pltpu.VMEM)
    scalars = pl.BlockSpec(memory_space=pltpu.SMEM)
    if early is None:
        function, specs, scratch, limit = kernel, [scalars] * smem + [here] * (len(ins) - smem), [], 16
    else:
        function, specs, limit = body, [pl.BlockSpec(memory_space=pltpu.HBM)] * len(ins), 56
        scratch = [pltpu.VMEM(a.shape, a.dtype) for a in ins]
        scratch.append(pltpu.SemaphoreType.DMA((len(ins), groups)))
    return pl.pallas_call(
        function,
        out_shape=[jax.ShapeDtypeStruct(shape, dtype) for shape, dtype in outs],
        in_specs=specs,
        out_specs=[here] * len(outs),
        scratch_shapes=scratch,
        compiler_params=pltpu.CompilerParams(vmem_limit_bytes=limit * 2**20),
        cost_estimate=pl.CostEstimate(
            flops=int(us * 50000000), bytes_accessed=1000000, transcendentals=0
        ),
    )(*ins)


def shifted(value, axis, steps):
    count = lax.axis_size(axis)
    return lax.ppermute(value, axis, [(i, (i + steps) % count) for i in range(count)])


def by_query(rows):
    return rows.transpose(1, 2, 3, 0).reshape(OWN, HEADS)


def to_all(value, axis):
    count = lax.axis_size(axis)
    everyone = jnp.broadcast_to(value[None], (count, *value.shape))
    return lax.all_to_all(everyone, axis, 0, 0, tiled=True)


def local(
    queries, keys, values, out_grad, log_norm, delta_rows, text_keys, text_values, window_table
):
    shape = queries.shape
    width = shape[-1]
    text = text_keys.shape[0]
    q = queries.reshape(OWN, width)
    g = out_grad.reshape(OWN, width)
    k = keys.reshape(OWN, width)
    v = values.reshape(OWN, width)
    anchor = jnp.zeros((), jnp.int32)
    live = lax.dynamic_slice(
        window_table, (lax.axis_index(HA), lax.axis_index("wa"), anchor), (1, 1, 9)
    ).reshape(9)

    left, right, words, stats = call(
        first_kernel,
        [
            ((2 * SIDE, width), BF16),
            ((2 * SIDE, width), BF16),
            ((2 * HEADS * text, HDIM), F32),
            ((32, HDIM), F32),
        ],
        [
            jnp.asarray(SIDES, BF16),
            k,
            v,
            by_query(log_norm),
            by_query(delta_rows),
            q,
            g,
            text_keys,
            text_values,
        ],
        us=3,
        early=3,
    )
    count = lax.axis_size(HA)
    words = lax.all_to_all(words.reshape(count, -1, HDIM), HA, 0, 0, tiled=True)
    piece = words.sum(axis=0)
    pieces = to_all(piece, "wa")
    piece = pieces.sum(axis=0).astype(BF16)
    pieces = to_all(piece, HA)
    text_key_grad, text_value_grad = call(
        words_kernel, [((text, width), BF16)] * 2, [pieces]
    )

    from_right = shifted(left, "wa", -1)
    from_left = shifted(right, "wa", 1)
    part, own = call(
        own_kernel,
        [((OWN, width), F32), ((2 * OWN, width), F32)],
        [live, stats, q, g, k, v, text_keys, text_values],
        us=3,
        smem=1,
    )
    top, bottom = call(
        ends_kernel,
        [((2 * ENDS, width), BF16)] * 2,
        [jnp.asarray(BANDS, BF16), k, v, from_left, from_right],
    )
    from_below = shifted(top, HA, -1)
    from_above = shifted(bottom, HA, 1)
    top_grad, bottom_grad, part = call(
        band_kernel,
        [((2 * ENDS, width), F32)] * 2 + [((OWN, width), F32)],
        [live, stats, q, g, from_above, from_below, part],
        us=2,
        smem=1,
    )
    above = shifted(bottom_grad, HA, 1)
    below = shifted(top_grad, HA, -1)
    left_grad, right_grad, query_grad = call(
        side_kernel,
        [((2 * SIDE, width), F32)] * 2 + [((OWN, width), BF16)],
        [live, stats, q, g, from_left, from_right, part],
        us=2,
        smem=1,
    )
    back = np.concatenate([BANDS[0].T, BANDS[1].T], axis=1)
    left_grad, right_grad = call(
        corners_kernel,
        [((2 * SIDE, width), F32)] * 2,
        [jnp.asarray(back[OWN:], F32), left_grad, right_grad, above, below],
    )
    after = shifted(left_grad, "wa", -1)
    before = shifted(right_grad, "wa", 1)
    back = np.concatenate([SIDES[0].T, SIDES[1].T], axis=1)
    key_grad, value_grad = call(
        sum_kernel,
        [((OWN, width), BF16)] * 2,
        [jnp.asarray(back, F32), own, before, after, above, below],
    )
    return (
        query_grad.reshape(shape),
        key_grad.reshape(shape),
        value_grad.reshape(shape),
        text_key_grad,
        text_value_grad,
    )


def solution(mesh):
    split = Mesh(
        mesh.devices.reshape(mesh.shape["group"], 8, 2, mesh.shape["wa"]),
        ("group", "ha_0", "ha_1", "wa"),
    )
    return jax.shard_map(
        local,
        mesh=split,
        in_specs=(
            P("group", HA, "wa", None),
            P("group", HA, "wa", None),
            P("group", HA, "wa", None),
            P("group", HA, "wa", None),
            P(None, "group", HA, "wa"),
            P(None, "group", HA, "wa"),
            P("group", None),
            P("group", None),
            P(),
        ),
        out_specs=(
            P("group", HA, "wa", None),
            P("group", HA, "wa", None),
            P("group", HA, "wa", None),
            P("group", None),
            P("group", None),
        ),
        check_vma=False,
    )
```

```python
import math

import jax
import jax.numpy as jnp
import numpy as np
from jax import lax
from jax.experimental import pallas as pl
from jax.experimental.pallas import tpu as pltpu
from jax.sharding import Mesh
from jax.sharding import PartitionSpec as P


HEADS = 12
HDIM = 128
TILE = 8
HALO = 2
HA = ("ha_0", "ha_1")
F32 = jnp.float32
BF16 = jnp.bfloat16
SCALE = 1.0 / math.sqrt(HDIM)

FRAMES = 2
OWN = FRAMES * TILE * TILE
SIDE = FRAMES * TILE * HALO
CORNER = HALO * HALO
BAND = HALO * TILE + 2 * CORNER
ENDS = FRAMES * BAND


def nt(a, b):
    return lax.dot_general(a, b, (((1,), (1,)), ((), ())), preferred_element_type=F32)


def nn(a, b):
    return lax.dot_general(a, b, (((1,), (0,)), ((), ())), preferred_element_type=F32)


def tn(a, b):
    return lax.dot_general(a, b, (((0,), (0,)), ((), ())), preferred_element_type=F32)


def exact(a, b):
    return lax.dot_general(
        a, b, (((1,), (0,)), ((), ())), precision=lax.Precision.HIGHEST, preferred_element_type=F32
    )


def own_row(frame, row, col):
    return frame * TILE * TILE + row * TILE + col


def side_row(frame, row, col):
    return (frame * TILE + row) * HALO + col


def select_sides():
    out = np.zeros((2, SIDE, OWN), np.float32)
    for side, first in enumerate((0, TILE - HALO)):
        for frame in range(FRAMES):
            for row in range(TILE):
                for col in range(HALO):
                    out[side, side_row(frame, row, col), own_row(frame, row, first + col)] = 1
    return out


def select_ends():
    out = np.zeros((2, ENDS, OWN + 2 * SIDE), np.float32)
    for end, first in enumerate((0, TILE - HALO)):
        for frame in range(FRAMES):
            at = frame * BAND
            for row in range(HALO):
                for col in range(TILE):
                    out[end, at, own_row(frame, first + row, col)] = 1
                    at += 1
            for side in range(2):
                for row in range(HALO):
                    for col in range(HALO):
                        out[end, at, OWN + side * SIDE + side_row(frame, first + row, col)] = 1
                        at += 1
    return out


SIDES = select_sides()
BANDS = select_ends()


GROUP = 2


def ends_kernel(select_ref, keys_ref, values_ref, left_ref, right_ref, top_ref, bottom_ref):
    for part, ref in enumerate((keys_ref, values_ref)):
        at = slice(part * SIDE, (part + 1) * SIDE)
        rows = jnp.concatenate([ref[...], left_ref[at, :], right_ref[at, :]], axis=0)
        to = slice(part * ENDS, (part + 1) * ENDS)
        top_ref[to, :] = nn(select_ref[0], rows).astype(BF16)
        bottom_ref[to, :] = nn(select_ref[1], rows).astype(BF16)


def sides_kernel(select_ref, keys_ref, values_ref, left_ref, right_ref):
    for part, ref in enumerate((keys_ref, values_ref)):
        rows = ref[...]
        at = slice(part * SIDE, (part + 1) * SIDE)
        left_ref[at, :] = nn(select_ref[0], rows).astype(BF16)
        right_ref[at, :] = nn(select_ref[1], rows).astype(BF16)


def text_kernel(
    ready, norm_ref, delta_ref, query_ref, out_grad_ref, key_ref, value_ref, grad_ref, stats_ref
):
    heads = lax.broadcasted_iota(jnp.int32, (16, HEADS), 1)
    identity = (heads == lax.broadcasted_iota(jnp.int32, (16, HEADS), 0)).astype(F32)
    stats = []
    for which, ref in enumerate((norm_ref, delta_ref)):
        rows = lax.dot_general(
            identity,
            ref[...],
            (((1,), (1,)), ((), ())),
            precision=lax.Precision.HIGHEST,
            preferred_element_type=F32,
        )
        stats_ref[which * 16 : (which + 1) * 16, :] = rows
        stats.append(rows)
    norm, delta = stats
    text = key_ref.shape[0]
    piece = grad_ref.shape[0] // 16
    for h in range(HEADS):
        ready(h)
        cols = slice(h * HDIM, (h + 1) * HDIM)
        q = query_ref[:, cols]
        g = out_grad_ref[:, cols]
        probs = jnp.exp(nt(key_ref[:, cols], q) * SCALE - norm[h : h + 1])
        prob_grad = nt(value_ref[:, cols], g)
        score_grad = (probs * (prob_grad - delta[h : h + 1])).astype(BF16)
        for part, grad in enumerate((nn(score_grad, q) * SCALE, nn(probs.astype(BF16), g))):
            for at in range(0, text, 16):
                chip, within = divmod(h * text + at, piece)
                to = (2 * chip + part) * piece + within
                grad_ref[to : to + 16, :] = grad[at : at + 16]


def backward(q, g, k, v, norm, delta, live):
    probs = jnp.exp(nt(k, q) * SCALE - norm)
    if live is not None:
        probs = probs * live
    score_grad = (probs * (nt(v, g) - delta)).astype(BF16)
    return probs.astype(BF16), score_grad


def own_kernel(
    live_ref,
    stats_ref,
    query_ref,
    out_grad_ref,
    keys_ref,
    values_ref,
    text_key_ref,
    text_value_ref,
    query_grad_ref,
    own_ref,
):
    text = text_key_ref.shape[0]
    rows = lax.broadcasted_iota(jnp.int32, (OWN + text, HDIM), 0)
    live = jnp.where(rows < OWN, live_ref[4].astype(F32), 1.0)
    for h in range(HEADS):
        cols = slice(h * HDIM, (h + 1) * HDIM)
        q = query_ref[:, cols]
        g = out_grad_ref[:, cols]
        k = jnp.concatenate([keys_ref[:, cols], text_key_ref[:, cols]], axis=0)
        v = jnp.concatenate([values_ref[:, cols], text_value_ref[:, cols]], axis=0)
        norm = stats_ref[h : h + 1, :]
        delta = stats_ref[16 + h : 17 + h, :]
        probs, score_grad = backward(q, g, k, v, norm, delta, live)
        query_grad_ref[:, cols] = tn(score_grad, k)
        own_ref[:OWN, cols] = nn(score_grad[:OWN], q) * SCALE
        own_ref[OWN:, cols] = nn(probs[:OWN], g)


def band_kernel(
    live_ref,
    stats_ref,
    query_ref,
    out_grad_ref,
    top_ref,
    bottom_ref,
    part_ref,
    top_grad_ref,
    bottom_grad_ref,
    query_grad_ref,
):
    def live(block):
        return live_ref[block].astype(F32)

    band = lax.rem(lax.broadcasted_iota(jnp.int32, (ENDS, HDIM), 0), BAND)
    lives = [
        jnp.where(
            band < HALO * TILE,
            live(first + 1),
            jnp.where(band < HALO * TILE + CORNER, live(first), live(first + 2)),
        )
        for first in (0, 6)
    ]
    two_halves(
        (stats_ref, query_ref, out_grad_ref, top_ref, bottom_ref, part_ref),
        (top_grad_ref, bottom_grad_ref, query_grad_ref),
        jnp.concatenate(lives, axis=0),
        1.0,
    )


def side_kernel(
    live_ref,
    stats_ref,
    query_ref,
    out_grad_ref,
    left_ref,
    right_ref,
    part_ref,
    left_grad_ref,
    right_grad_ref,
    query_grad_ref,
):
    rows = lax.broadcasted_iota(jnp.int32, (2 * SIDE, HDIM), 0)
    lives = jnp.where(rows < SIDE, live_ref[3].astype(F32), live_ref[5].astype(F32))
    two_halves(
        (stats_ref, query_ref, out_grad_ref, left_ref, right_ref, part_ref),
        (left_grad_ref, right_grad_ref, query_grad_ref),
        lives,
        SCALE,
    )


def two_halves(given, made, live, scale):
    stats_ref, query_ref, out_grad_ref, first_ref, second_ref, part_ref = given
    first_grad_ref, second_grad_ref, query_grad_ref = made
    rows = first_ref.shape[0] // 2
    for h in range(HEADS):
        cols = slice(h * HDIM, (h + 1) * HDIM)
        q = query_ref[:, cols]
        g = out_grad_ref[:, cols]
        k, v = (
            jnp.concatenate([first_ref[at, cols], second_ref[at, cols]], axis=0)
            for at in (slice(0, rows), slice(rows, 2 * rows))
        )
        norm = stats_ref[h : h + 1, :]
        delta = stats_ref[16 + h : 17 + h, :]
        probs, score_grad = backward(q, g, k, v, norm, delta, live)
        query_grad = part_ref[:, cols] + tn(score_grad, k)
        query_grad_ref[:, cols] = (query_grad * scale).astype(query_grad_ref.dtype)
        for at, grad in ((slice(0, rows), nn(score_grad, q) * SCALE), (slice(rows, 2 * rows), nn(probs, g))):
            first_grad_ref[at, cols] = grad[:rows]
            second_grad_ref[at, cols] = grad[rows:]


def corners_kernel(
    select_ref, left_ref, right_ref, above_ref, below_ref, left_out_ref, right_out_ref
):
    for part in range(2):
        side = slice(part * SIDE, (part + 1) * SIDE)
        ends = slice(part * ENDS, (part + 1) * ENDS)
        bands = jnp.concatenate([above_ref[ends, :], below_ref[ends, :]], axis=0)
        more = exact(select_ref[...], bands)
        left_out_ref[side, :] = left_ref[side, :] + more[:SIDE]
        right_out_ref[side, :] = right_ref[side, :] + more[SIDE:]


def sum_kernel(
    select_ref, own_ref, left_ref, right_ref, above_ref, below_ref, key_ref, value_ref
):
    edge = HALO * TILE
    for part, out in enumerate((key_ref, value_ref)):
        side = slice(part * SIDE, (part + 1) * SIDE)
        rows = jnp.concatenate([left_ref[side, :], right_ref[side, :]], axis=0)
        total = own_ref[part * OWN : (part + 1) * OWN, :] + exact(select_ref[...], rows)
        for frame in range(FRAMES):
            at = part * ENDS + frame * BAND
            top = frame * TILE * TILE
            bottom = top + TILE * TILE - edge
            end = top + TILE * TILE
            out[top : top + edge, :] = (
                total[top : top + edge] + above_ref[at : at + edge, :]
            ).astype(BF16)
            out[top + edge : bottom, :] = total[top + edge : bottom].astype(BF16)
            out[bottom:end, :] = (total[bottom:end] + below_ref[at : at + edge, :]).astype(BF16)


def words_kernel(parts_ref, key_ref, value_ref):
    text = key_ref.shape[0]
    rows = parts_ref.shape[1]
    for part, out in enumerate((key_ref, value_ref)):
        for h in range(HEADS):
            for at in range(0, text, 16):
                chip, within = divmod(h * text + at, rows)
                piece = parts_ref[2 * chip + part, within : within + 16, :]
                out[at : at + 16, h * HDIM : (h + 1) * HDIM] = piece


def call(kernel, outs, ins, us=1.0, smem=0, fetch=False):
    groups = HEADS // GROUP
    step = GROUP * HDIM

    def body(*refs):
        n = len(ins)
        outputs = refs[n : n + len(outs)]
        buffers = refs[n + len(outs) : -1]
        semaphores = refs[-1]
        small, wide = [], [[] for _ in range(groups)]
        for i, (far, near) in enumerate(zip(refs[:n], buffers)):
            if ins[i].ndim == 2 and ins[i].shape[1] == groups * step:
                for m in range(groups):
                    at = (slice(None), slice(m * step, (m + 1) * step))
                    copy = pltpu.make_async_copy(far.at[at], near.at[at], semaphores.at[i, m])
                    wide[m].append(copy)
            else:
                small.append(pltpu.make_async_copy(far, near, semaphores.at[i, 0]))
        for copies in (small, *wide):
            for copy in copies:
                copy.start()
        for copy in small:
            copy.wait()

        def ready(h):
            if h % GROUP == 0:
                for copy in wide[h // GROUP]:
                    copy.wait()

        kernel(ready, *buffers, *outputs)

    here = pl.BlockSpec(memory_space=pltpu.VMEM)
    scalars = pl.BlockSpec(memory_space=pltpu.SMEM)
    if not fetch:
        function, specs, scratch, limit = kernel, [scalars] * smem + [here] * (len(ins) - smem), [], 16
    else:
        function, specs, limit = body, [pl.BlockSpec(memory_space=pltpu.HBM)] * len(ins), 56
        scratch = [pltpu.VMEM(a.shape, a.dtype) for a in ins]
        scratch.append(pltpu.SemaphoreType.DMA((len(ins), groups)))
    return pl.pallas_call(
        function,
        out_shape=[jax.ShapeDtypeStruct(shape, dtype) for shape, dtype in outs],
        in_specs=specs,
        out_specs=[here] * len(outs),
        scratch_shapes=scratch,
        compiler_params=pltpu.CompilerParams(vmem_limit_bytes=limit * 2**20),
        cost_estimate=pl.CostEstimate(
            flops=int(us * 50000000), bytes_accessed=1000000, transcendentals=0
        ),
    )(*ins)


def shifted(value, axis, steps):
    count = lax.axis_size(axis)
    return lax.ppermute(value, axis, [(i, (i + steps) % count) for i in range(count)])


def by_query(rows):
    return rows.transpose(1, 2, 3, 0).reshape(OWN, HEADS)


def to_all(value, axis):
    count = lax.axis_size(axis)
    everyone = jnp.broadcast_to(value[None], (count, *value.shape))
    return lax.all_to_all(everyone, axis, 0, 0, tiled=True)


def local(
    queries, keys, values, out_grad, log_norm, delta_rows, text_keys, text_values, window_table
):
    shape = queries.shape
    width = shape[-1]
    text = text_keys.shape[0]
    q = queries.reshape(OWN, width)
    g = out_grad.reshape(OWN, width)
    k = keys.reshape(OWN, width)
    v = values.reshape(OWN, width)
    anchor = jnp.zeros((), jnp.int32)
    live = lax.dynamic_slice(
        window_table, (lax.axis_index(HA), lax.axis_index("wa"), anchor), (1, 1, 9)
    ).reshape(9)

    words, stats = call(
        text_kernel,
        [((2 * HEADS * text, HDIM), F32), ((32, HDIM), F32)],
        [by_query(log_norm), by_query(delta_rows), q, g, text_keys, text_values],
        us=3,
        fetch=True,
    )
    count = lax.axis_size(HA)
    words = lax.all_to_all(words.reshape(count, -1, HDIM), HA, 0, 0, tiled=True)
    piece = words.sum(axis=0)
    pieces = to_all(piece, "wa")
    piece = pieces.sum(axis=0).astype(BF16)
    pieces = to_all(piece, HA)
    text_key_grad, text_value_grad = call(
        words_kernel, [((text, width), BF16)] * 2, [pieces]
    )

    left, right = call(
        sides_kernel, [((2 * SIDE, width), BF16)] * 2, [jnp.asarray(SIDES, BF16), k, v]
    )
    from_right = shifted(left, "wa", -1)
    from_left = shifted(right, "wa", 1)
    part, own = call(
        own_kernel,
        [((OWN, width), F32), ((2 * OWN, width), F32)],
        [live, stats, q, g, k, v, text_keys, text_values],
        us=3,
        smem=1,
    )
    top, bottom = call(
        ends_kernel,
        [((2 * ENDS, width), BF16)] * 2,
        [jnp.asarray(BANDS, BF16), k, v, from_left, from_right],
    )
    from_below = shifted(top, HA, -1)
    from_above = shifted(bottom, HA, 1)
    top_grad, bottom_grad, part = call(
        band_kernel,
        [((2 * ENDS, width), F32)] * 2 + [((OWN, width), F32)],
        [live, stats, q, g, from_above, from_below, part],
        us=2,
        smem=1,
    )
    above = shifted(bottom_grad, HA, 1)
    below = shifted(top_grad, HA, -1)
    left_grad, right_grad, query_grad = call(
        side_kernel,
        [((2 * SIDE, width), F32)] * 2 + [((OWN, width), BF16)],
        [live, stats, q, g, from_left, from_right, part],
        us=2,
        smem=1,
    )
    back = np.concatenate([BANDS[0].T, BANDS[1].T], axis=1)
    left_grad, right_grad = call(
        corners_kernel,
        [((2 * SIDE, width), F32)] * 2,
        [jnp.asarray(back[OWN:], F32), left_grad, right_grad, above, below],
    )
    after = shifted(left_grad, "wa", -1)
    before = shifted(right_grad, "wa", 1)
    back = np.concatenate([SIDES[0].T, SIDES[1].T], axis=1)
    key_grad, value_grad = call(
        sum_kernel,
        [((OWN, width), BF16)] * 2,
        [jnp.asarray(back, F32), own, before, after, above, below],
    )
    return (
        query_grad.reshape(shape),
        key_grad.reshape(shape),
        value_grad.reshape(shape),
        text_key_grad,
        text_value_grad,
    )


def solution(mesh):
    split = Mesh(
        mesh.devices.reshape(mesh.shape["group"], 8, 2, mesh.shape["wa"]),
        ("group", "ha_0", "ha_1", "wa"),
    )
    return jax.shard_map(
        local,
        mesh=split,
        in_specs=(
            P("group", HA, "wa", None),
            P("group", HA, "wa", None),
            P("group", HA, "wa", None),
            P("group", HA, "wa", None),
            P(None, "group", HA, "wa"),
            P(None, "group", HA, "wa"),
            P("group", None),
            P("group", None),
            P(),
        ),
        out_specs=(
            P("group", HA, "wa", None),
            P("group", HA, "wa", None),
            P("group", HA, "wa", None),
            P("group", None),
            P("group", None),
        ),
        check_vma=False,
    )
```

```python
import math

import jax
import jax.numpy as jnp
import numpy as np
from jax import lax
from jax.experimental import pallas as pl
from jax.experimental.pallas import tpu as pltpu
from jax.sharding import Mesh
from jax.sharding import PartitionSpec as P


HEADS = 12
HDIM = 128
TILE = 8
HALO = 2
HA = ("ha_0", "ha_1")
F32 = jnp.float32
BF16 = jnp.bfloat16
SCALE = 1.0 / math.sqrt(HDIM)

FRAMES = 2
OWN = FRAMES * TILE * TILE
SIDE = FRAMES * TILE * HALO
CORNER = HALO * HALO
BAND = HALO * TILE + 2 * CORNER
ENDS = FRAMES * BAND


def nt(a, b):
    return lax.dot_general(a, b, (((1,), (1,)), ((), ())), preferred_element_type=F32)


def nn(a, b):
    return lax.dot_general(a, b, (((1,), (0,)), ((), ())), preferred_element_type=F32)


def tn(a, b):
    return lax.dot_general(a, b, (((0,), (0,)), ((), ())), preferred_element_type=F32)


def exact(a, b):
    return lax.dot_general(
        a, b, (((1,), (0,)), ((), ())), precision=lax.Precision.HIGHEST, preferred_element_type=F32
    )


STEPS = 128.0
MOST = 32000.0
I16 = jnp.int16


def scaled(x, level):
    half = jnp.exp2(level * (0.5 / STEPS))
    return (x * half) * half


def coded(x):
    most = jnp.maximum(jnp.max(jnp.abs(x), axis=0, keepdims=True), 2.0**-120)
    level = jnp.ceil(jnp.log2(most) * STEPS)
    code = jnp.floor(scaled(x, -level) * MOST + 0.5)
    return code.astype(jnp.int32).astype(I16), level


def levels_of(rows):
    blank = jnp.zeros((8 - len(rows), rows[0].shape[1]), F32)
    return jnp.concatenate([*rows, blank], axis=0).astype(jnp.int32).astype(I16)


def wide(code):
    return code.astype(jnp.int32).astype(F32)


def decoded(code, level):
    return scaled(wide(code) * (1.0 / MOST), level)


def own_row(frame, row, col):
    return frame * TILE * TILE + row * TILE + col


def side_row(frame, row, col):
    return (frame * TILE + row) * HALO + col


def select_sides():
    out = np.zeros((2, SIDE, OWN), np.float32)
    for side, first in enumerate((0, TILE - HALO)):
        for frame in range(FRAMES):
            for row in range(TILE):
                for col in range(HALO):
                    out[side, side_row(frame, row, col), own_row(frame, row, first + col)] = 1
    return out


def select_ends():
    out = np.zeros((2, ENDS, OWN + 2 * SIDE), np.float32)
    for end, first in enumerate((0, TILE - HALO)):
        for frame in range(FRAMES):
            at = frame * BAND
            for row in range(HALO):
                for col in range(TILE):
                    out[end, at, own_row(frame, first + row, col)] = 1
                    at += 1
            for side in range(2):
                for row in range(HALO):
                    for col in range(HALO):
                        out[end, at, OWN + side * SIDE + side_row(frame, first + row, col)] = 1
                        at += 1
    return out


SIDES = select_sides()
BANDS = select_ends()


GROUP = 2


def ends_kernel(select_ref, keys_ref, values_ref, left_ref, right_ref, top_ref, bottom_ref):
    for part, ref in enumerate((keys_ref, values_ref)):
        at = slice(part * SIDE, (part + 1) * SIDE)
        rows = jnp.concatenate([ref[...], left_ref[at, :], right_ref[at, :]], axis=0)
        to = slice(part * ENDS, (part + 1) * ENDS)
        top_ref[to, :] = nn(select_ref[0], rows).astype(BF16)
        bottom_ref[to, :] = nn(select_ref[1], rows).astype(BF16)


def sides_kernel(select_ref, keys_ref, values_ref, left_ref, right_ref):
    for part, ref in enumerate((keys_ref, values_ref)):
        rows = ref[...]
        at = slice(part * SIDE, (part + 1) * SIDE)
        left_ref[at, :] = nn(select_ref[0], rows).astype(BF16)
        right_ref[at, :] = nn(select_ref[1], rows).astype(BF16)


def text_kernel(
    ready,
    norm_ref,
    delta_ref,
    query_ref,
    out_grad_ref,
    key_ref,
    value_ref,
    grad_ref,
    stats_ref,
    levels_ref,
):
    levels_ref[...] = jnp.zeros(levels_ref.shape, F32)
    heads = lax.broadcasted_iota(jnp.int32, (16, HEADS), 1)
    identity = (heads == lax.broadcasted_iota(jnp.int32, (16, HEADS), 0)).astype(F32)
    stats = []
    for which, ref in enumerate((norm_ref, delta_ref)):
        rows = lax.dot_general(
            identity,
            ref[...],
            (((1,), (1,)), ((), ())),
            precision=lax.Precision.HIGHEST,
            preferred_element_type=F32,
        )
        stats_ref[which * 16 : (which + 1) * 16, :] = rows
        stats.append(rows)
    norm, delta = stats
    text = key_ref.shape[0]
    pieces = levels_ref.shape[0] // 8
    sent = grad_ref.shape[0] // pieces
    piece = sent - 8
    for h in range(HEADS):
        ready(h)
        cols = slice(h * HDIM, (h + 1) * HDIM)
        q = query_ref[:, cols]
        g = out_grad_ref[:, cols]
        probs = jnp.exp(nt(key_ref[:, cols], q) * SCALE - norm[h : h + 1])
        prob_grad = nt(value_ref[:, cols], g)
        score_grad = (probs * (prob_grad - delta[h : h + 1])).astype(BF16)
        for part, grad in enumerate((nn(score_grad, q) * SCALE, nn(probs.astype(BF16), g))):
            for at in range(0, text, 16):
                chip, within = divmod(h * text + at, piece)
                to = 2 * chip + part
                code, level = coded(grad[at : at + 16])
                grad_ref[to * sent + within : to * sent + within + 16, :] = code
                levels_ref[to * 8 + within // 16 : to * 8 + within // 16 + 1, :] = level
    for to in range(pieces):
        levels = levels_ref[to * 8 : (to + 1) * 8, :].astype(jnp.int32).astype(I16)
        grad_ref[(to + 1) * sent - 8 : (to + 1) * sent, :] = levels


def over_chips_kernel(parts_ref, out_ref):
    count, sent, _ = parts_ref.shape
    total = 0.0
    for n in range(count):
        levels = wide(parts_ref[n, sent - 8 :, :])
        blocks = [
            decoded(parts_ref[n, 16 * b : 16 * b + 16, :], levels[b : b + 1])
            for b in range((sent - 8) // 16)
        ]
        total = total + jnp.concatenate(blocks, axis=0)
    code, level = coded(total)
    levels = levels_of([level])
    for n in range(out_ref.shape[0]):
        out_ref[n, : sent - 8, :] = code
        out_ref[n, sent - 8 :, :] = levels


def over_tiles_kernel(parts_ref, out_ref):
    count, sent, _ = parts_ref.shape
    total = 0.0
    for n in range(count):
        level = wide(parts_ref[n, sent - 8 :, :])[:1]
        total = total + decoded(parts_ref[n, : sent - 8, :], level)
    total = total.astype(BF16)
    for n in range(out_ref.shape[0]):
        out_ref[n] = total


def backward(q, g, k, v, norm, delta, live):
    probs = jnp.exp(nt(k, q) * SCALE - norm)
    if live is not None:
        probs = probs * live
    score_grad = (probs * (nt(v, g) - delta)).astype(BF16)
    return probs.astype(BF16), score_grad


def own_kernel(
    live_ref,
    stats_ref,
    query_ref,
    out_grad_ref,
    keys_ref,
    values_ref,
    text_key_ref,
    text_value_ref,
    query_grad_ref,
    own_ref,
):
    text = text_key_ref.shape[0]
    rows = lax.broadcasted_iota(jnp.int32, (OWN + text, HDIM), 0)
    live = jnp.where(rows < OWN, live_ref[4].astype(F32), 1.0)
    for h in range(HEADS):
        cols = slice(h * HDIM, (h + 1) * HDIM)
        q = query_ref[:, cols]
        g = out_grad_ref[:, cols]
        k = jnp.concatenate([keys_ref[:, cols], text_key_ref[:, cols]], axis=0)
        v = jnp.concatenate([values_ref[:, cols], text_value_ref[:, cols]], axis=0)
        norm = stats_ref[h : h + 1, :]
        delta = stats_ref[16 + h : 17 + h, :]
        probs, score_grad = backward(q, g, k, v, norm, delta, live)
        query_grad_ref[:, cols] = tn(score_grad, k)
        own_ref[:OWN, cols] = nn(score_grad[:OWN], q) * SCALE
        own_ref[OWN:, cols] = nn(probs[:OWN], g)


def band_kernel(
    live_ref,
    stats_ref,
    query_ref,
    out_grad_ref,
    top_ref,
    bottom_ref,
    part_ref,
    top_grad_ref,
    bottom_grad_ref,
    query_grad_ref,
):
    def live(block):
        return live_ref[block].astype(F32)

    band = lax.rem(lax.broadcasted_iota(jnp.int32, (ENDS, HDIM), 0), BAND)
    lives = [
        jnp.where(
            band < HALO * TILE,
            live(first + 1),
            jnp.where(band < HALO * TILE + CORNER, live(first), live(first + 2)),
        )
        for first in (0, 6)
    ]
    two_halves(
        (stats_ref, query_ref, out_grad_ref, top_ref, bottom_ref, part_ref),
        (top_grad_ref, bottom_grad_ref, query_grad_ref),
        jnp.concatenate(lives, axis=0),
        1.0,
        True,
    )


def side_kernel(
    live_ref,
    stats_ref,
    query_ref,
    out_grad_ref,
    left_ref,
    right_ref,
    part_ref,
    left_grad_ref,
    right_grad_ref,
    query_grad_ref,
):
    rows = lax.broadcasted_iota(jnp.int32, (2 * SIDE, HDIM), 0)
    lives = jnp.where(rows < SIDE, live_ref[3].astype(F32), live_ref[5].astype(F32))
    two_halves(
        (stats_ref, query_ref, out_grad_ref, left_ref, right_ref, part_ref),
        (left_grad_ref, right_grad_ref, query_grad_ref),
        lives,
        SCALE,
        False,
    )


def two_halves(given, made, live, scale, code):
    stats_ref, query_ref, out_grad_ref, first_ref, second_ref, part_ref = given
    first_grad_ref, second_grad_ref, query_grad_ref = made
    rows = first_ref.shape[0] // 2
    for h in range(HEADS):
        cols = slice(h * HDIM, (h + 1) * HDIM)
        q = query_ref[:, cols]
        g = out_grad_ref[:, cols]
        k, v = (
            jnp.concatenate([first_ref[at, cols], second_ref[at, cols]], axis=0)
            for at in (slice(0, rows), slice(rows, 2 * rows))
        )
        norm = stats_ref[h : h + 1, :]
        delta = stats_ref[16 + h : 17 + h, :]
        probs, score_grad = backward(q, g, k, v, norm, delta, live)
        query_grad = part_ref[:, cols] + tn(score_grad, k)
        query_grad_ref[:, cols] = (query_grad * scale).astype(query_grad_ref.dtype)
        grads = (nn(score_grad, q) * SCALE, nn(probs, g))
        for n, ref in enumerate((first_grad_ref, second_grad_ref)):
            levels = []
            for at, grad in ((slice(0, rows), grads[0]), (slice(rows, 2 * rows), grads[1])):
                block = grad[n * rows : (n + 1) * rows]
                if code:
                    block, level = coded(block)
                    levels.append(level)
                ref[at, cols] = block
            if code:
                ref[2 * rows :, cols] = levels_of(levels)


def received(ref, part, rows):
    level = wide(ref[2 * rows :, :])[part : part + 1]
    return decoded(ref[part * rows : (part + 1) * rows, :], level)


def corners_kernel(
    select_ref, left_ref, right_ref, above_ref, below_ref, left_out_ref, right_out_ref
):
    levels = ([], [])
    for part in range(2):
        side = slice(part * SIDE, (part + 1) * SIDE)
        bands = [received(ref, part, ENDS) for ref in (above_ref, below_ref)]
        more = exact(select_ref[...], jnp.concatenate(bands, axis=0))
        for n, (ref, out) in enumerate(((left_ref, left_out_ref), (right_ref, right_out_ref))):
            code, level = coded(ref[side, :] + more[n * SIDE : (n + 1) * SIDE])
            out[side, :] = code
            levels[n].append(level)
    left_out_ref[2 * SIDE :, :] = levels_of(levels[0])
    right_out_ref[2 * SIDE :, :] = levels_of(levels[1])


def sum_kernel(
    select_ref, own_ref, left_ref, right_ref, above_ref, below_ref, key_ref, value_ref
):
    edge = HALO * TILE
    for part, out in enumerate((key_ref, value_ref)):
        above, below = received(above_ref, part, ENDS), received(below_ref, part, ENDS)
        sides = [received(ref, part, SIDE) for ref in (left_ref, right_ref)]
        rows = jnp.concatenate(sides, axis=0)
        total = own_ref[part * OWN : (part + 1) * OWN, :] + exact(select_ref[...], rows)
        for frame in range(FRAMES):
            at = frame * BAND
            top = frame * TILE * TILE
            bottom = top + TILE * TILE - edge
            end = top + TILE * TILE
            out[top : top + edge, :] = (
                total[top : top + edge] + above[at : at + edge]
            ).astype(BF16)
            out[top + edge : bottom, :] = total[top + edge : bottom].astype(BF16)
            out[bottom:end, :] = (total[bottom:end] + below[at : at + edge]).astype(BF16)


def words_kernel(parts_ref, key_ref, value_ref):
    text = key_ref.shape[0]
    rows = parts_ref.shape[1]
    for part, out in enumerate((key_ref, value_ref)):
        for h in range(HEADS):
            for at in range(0, text, 16):
                chip, within = divmod(h * text + at, rows)
                piece = parts_ref[2 * chip + part, within : within + 16, :]
                out[at : at + 16, h * HDIM : (h + 1) * HDIM] = piece


def call(kernel, outs, ins, us=1.0, smem=0, fetch=False, scratch=()):
    groups = HEADS // GROUP
    step = GROUP * HDIM

    def body(*refs):
        n = len(ins)
        outputs = refs[n : n + len(outs)]
        buffers = refs[n + len(outs) : 2 * n + len(outs)]
        semaphores, *rest = refs[2 * n + len(outs) :]
        small, wide = [], [[] for _ in range(groups)]
        for i, (far, near) in enumerate(zip(refs[:n], buffers)):
            if ins[i].ndim == 2 and ins[i].shape[1] == groups * step:
                for m in range(groups):
                    at = (slice(None), slice(m * step, (m + 1) * step))
                    copy = pltpu.make_async_copy(far.at[at], near.at[at], semaphores.at[i, m])
                    wide[m].append(copy)
            else:
                small.append(pltpu.make_async_copy(far, near, semaphores.at[i, 0]))
        for copies in (small, *wide):
            for copy in copies:
                copy.start()
        for copy in small:
            copy.wait()

        def ready(h):
            if h % GROUP == 0:
                for copy in wide[h // GROUP]:
                    copy.wait()

        kernel(ready, *buffers, *outputs, *rest)

    here = pl.BlockSpec(memory_space=pltpu.VMEM)
    scalars = pl.BlockSpec(memory_space=pltpu.SMEM)
    if not fetch:
        function, specs, scratch, limit = kernel, [scalars] * smem + [here] * (len(ins) - smem), [*scratch], 16
    else:
        function, specs, limit = body, [pl.BlockSpec(memory_space=pltpu.HBM)] * len(ins), 56
        buffers = [pltpu.VMEM(a.shape, a.dtype) for a in ins]
        scratch = [*buffers, pltpu.SemaphoreType.DMA((len(ins), groups)), *scratch]
    return pl.pallas_call(
        function,
        out_shape=[jax.ShapeDtypeStruct(shape, dtype) for shape, dtype in outs],
        in_specs=specs,
        out_specs=[here] * len(outs),
        scratch_shapes=scratch,
        compiler_params=pltpu.CompilerParams(vmem_limit_bytes=limit * 2**20),
        cost_estimate=pl.CostEstimate(
            flops=int(us * 50000000), bytes_accessed=1000000, transcendentals=0
        ),
    )(*ins)


def shifted(value, axis, steps):
    count = lax.axis_size(axis)
    return lax.ppermute(value, axis, [(i, (i + steps) % count) for i in range(count)])


def by_query(rows):
    return rows.transpose(1, 2, 3, 0).reshape(OWN, HEADS)


def exchanged(pieces, axis):
    return lax.all_to_all(pieces, axis, 0, 0, tiled=True)


def local(
    queries, keys, values, out_grad, log_norm, delta_rows, text_keys, text_values, window_table
):
    shape = queries.shape
    width = shape[-1]
    text = text_keys.shape[0]
    q = queries.reshape(OWN, width)
    g = out_grad.reshape(OWN, width)
    k = keys.reshape(OWN, width)
    v = values.reshape(OWN, width)
    anchor = jnp.zeros((), jnp.int32)
    live = lax.dynamic_slice(
        window_table, (lax.axis_index(HA), lax.axis_index("wa"), anchor), (1, 1, 9)
    ).reshape(9)

    count = lax.axis_size(HA)
    piece = 2 * HEADS * text // count
    sent = piece + 8
    words, stats = call(
        text_kernel,
        [((count * sent, HDIM), I16), ((32, HDIM), F32)],
        [by_query(log_norm), by_query(delta_rows), q, g, text_keys, text_values],
        us=3,
        fetch=True,
        scratch=[pltpu.VMEM((count * 8, HDIM), F32)],
    )
    words = exchanged(words.reshape(count, sent, HDIM), HA)
    tiles = lax.axis_size("wa")
    (words,) = call(over_chips_kernel, [((tiles, sent, HDIM), I16)], [words])
    words = exchanged(words, "wa")
    (words,) = call(over_tiles_kernel, [((count, piece, HDIM), BF16)], [words])
    words = exchanged(words, HA)
    text_key_grad, text_value_grad = call(
        words_kernel, [((text, width), BF16)] * 2, [words]
    )

    left, right = call(
        sides_kernel, [((2 * SIDE, width), BF16)] * 2, [jnp.asarray(SIDES, BF16), k, v]
    )
    from_right = shifted(left, "wa", -1)
    from_left = shifted(right, "wa", 1)
    part, own = call(
        own_kernel,
        [((OWN, width), F32), ((2 * OWN, width), F32)],
        [live, stats, q, g, k, v, text_keys, text_values],
        us=3,
        smem=1,
    )
    top, bottom = call(
        ends_kernel,
        [((2 * ENDS, width), BF16)] * 2,
        [jnp.asarray(BANDS, BF16), k, v, from_left, from_right],
    )
    from_below = shifted(top, HA, -1)
    from_above = shifted(bottom, HA, 1)
    top_grad, bottom_grad, part = call(
        band_kernel,
        [((2 * ENDS + 8, width), I16)] * 2 + [((OWN, width), F32)],
        [live, stats, q, g, from_above, from_below, part],
        us=2,
        smem=1,
    )
    above = shifted(bottom_grad, HA, 1)
    below = shifted(top_grad, HA, -1)
    left_grad, right_grad, query_grad = call(
        side_kernel,
        [((2 * SIDE, width), F32)] * 2 + [((OWN, width), BF16)],
        [live, stats, q, g, from_left, from_right, part],
        us=2,
        smem=1,
    )
    back = np.concatenate([BANDS[0].T, BANDS[1].T], axis=1)
    left_grad, right_grad = call(
        corners_kernel,
        [((2 * SIDE + 8, width), I16)] * 2,
        [jnp.asarray(back[OWN:], F32), left_grad, right_grad, above, below],
    )
    after = shifted(left_grad, "wa", -1)
    before = shifted(right_grad, "wa", 1)
    back = np.concatenate([SIDES[0].T, SIDES[1].T], axis=1)
    key_grad, value_grad = call(
        sum_kernel,
        [((OWN, width), BF16)] * 2,
        [jnp.asarray(back, F32), own, before, after, above, below],
    )
    return (
        query_grad.reshape(shape),
        key_grad.reshape(shape),
        value_grad.reshape(shape),
        text_key_grad,
        text_value_grad,
    )


def solution(mesh):
    split = Mesh(
        mesh.devices.reshape(mesh.shape["group"], 8, 2, mesh.shape["wa"]),
        ("group", "ha_0", "ha_1", "wa"),
    )
    return jax.shard_map(
        local,
        mesh=split,
        in_specs=(
            P("group", HA, "wa", None),
            P("group", HA, "wa", None),
            P("group", HA, "wa", None),
            P("group", HA, "wa", None),
            P(None, "group", HA, "wa"),
            P(None, "group", HA, "wa"),
            P("group", None),
            P("group", None),
            P(),
        ),
        out_specs=(
            P("group", HA, "wa", None),
            P("group", HA, "wa", None),
            P("group", HA, "wa", None),
            P("group", None),
            P("group", None),
        ),
        check_vma=False,
    )
```

```python
import math

import jax
import jax.numpy as jnp
import numpy as np
from jax import lax
from jax.experimental import pallas as pl
from jax.experimental.pallas import tpu as pltpu
from jax.sharding import Mesh
from jax.sharding import PartitionSpec as P


HEADS = 12
HDIM = 128
TILE = 8
HALO = 2
HA = ("ha_0", "ha_1")
F32 = jnp.float32
BF16 = jnp.bfloat16
SCALE = 1.0 / math.sqrt(HDIM)

FRAMES = 2
OWN = FRAMES * TILE * TILE
SIDE = FRAMES * TILE * HALO
CORNER = HALO * HALO
BAND = HALO * TILE + 2 * CORNER
ENDS = FRAMES * BAND


def nt(a, b):
    return lax.dot_general(a, b, (((1,), (1,)), ((), ())), preferred_element_type=F32)


def nn(a, b):
    return lax.dot_general(a, b, (((1,), (0,)), ((), ())), preferred_element_type=F32)


def tn(a, b):
    return lax.dot_general(a, b, (((0,), (0,)), ((), ())), preferred_element_type=F32)


def picked(select, rows):
    high = rows.astype(BF16)
    low = (rows - high.astype(F32)).astype(BF16)
    return nn(select, high) + nn(select, low)


STEPS = 128.0
MOST = 32000.0
I16 = jnp.int16


def scaled(x, level):
    half = jnp.exp2(level * (0.5 / STEPS))
    return (x * half) * half


def coded(x):
    most = jnp.maximum(jnp.max(jnp.abs(x), axis=0, keepdims=True), 2.0**-120)
    level = jnp.ceil(jnp.log2(most) * STEPS)
    code = jnp.floor(scaled(x, -level) * MOST + 0.5)
    return code.astype(jnp.int32).astype(I16), level


def levels_of(rows):
    blank = jnp.zeros((8 - len(rows), rows[0].shape[1]), F32)
    return jnp.concatenate([*rows, blank], axis=0).astype(jnp.int32).astype(I16)


def wide(code):
    return code.astype(jnp.int32).astype(F32)


def decoded(code, level):
    return scaled(wide(code) * (1.0 / MOST), level)


def own_row(frame, row, col):
    return frame * TILE * TILE + row * TILE + col


def side_row(frame, row, col):
    return (frame * TILE + row) * HALO + col


def select_sides():
    out = np.zeros((2, SIDE, OWN), np.float32)
    for side, first in enumerate((0, TILE - HALO)):
        for frame in range(FRAMES):
            for row in range(TILE):
                for col in range(HALO):
                    out[side, side_row(frame, row, col), own_row(frame, row, first + col)] = 1
    return out


def select_ends():
    out = np.zeros((2, ENDS, OWN + 2 * SIDE), np.float32)
    for end, first in enumerate((0, TILE - HALO)):
        for frame in range(FRAMES):
            at = frame * BAND
            for row in range(HALO):
                for col in range(TILE):
                    out[end, at, own_row(frame, first + row, col)] = 1
                    at += 1
            for side in range(2):
                for row in range(HALO):
                    for col in range(HALO):
                        out[end, at, OWN + side * SIDE + side_row(frame, first + row, col)] = 1
                        at += 1
    return out


SIDES = select_sides()
BANDS = select_ends()


GROUP = 2


def ends_kernel(select_ref, keys_ref, values_ref, left_ref, right_ref, top_ref, bottom_ref):
    for part, ref in enumerate((keys_ref, values_ref)):
        at = slice(part * SIDE, (part + 1) * SIDE)
        rows = jnp.concatenate([ref[...], left_ref[at, :], right_ref[at, :]], axis=0)
        to = slice(part * ENDS, (part + 1) * ENDS)
        top_ref[to, :] = nn(select_ref[0], rows).astype(BF16)
        bottom_ref[to, :] = nn(select_ref[1], rows).astype(BF16)


def sides_kernel(select_ref, keys_ref, values_ref, left_ref, right_ref):
    for part, ref in enumerate((keys_ref, values_ref)):
        rows = ref[...]
        at = slice(part * SIDE, (part + 1) * SIDE)
        left_ref[at, :] = nn(select_ref[0], rows).astype(BF16)
        right_ref[at, :] = nn(select_ref[1], rows).astype(BF16)


def text_kernel(
    ready,
    norm_ref,
    delta_ref,
    query_ref,
    out_grad_ref,
    key_ref,
    value_ref,
    grad_ref,
    stats_ref,
    levels_ref,
):
    levels_ref[...] = jnp.zeros(levels_ref.shape, F32)
    heads = lax.broadcasted_iota(jnp.int32, (16, HEADS), 1)
    identity = (heads == lax.broadcasted_iota(jnp.int32, (16, HEADS), 0)).astype(F32)
    stats = []
    for which, ref in enumerate((norm_ref, delta_ref)):
        rows = lax.dot_general(
            identity,
            ref[...],
            (((1,), (1,)), ((), ())),
            precision=lax.Precision.HIGHEST,
            preferred_element_type=F32,
        )
        stats_ref[which * 16 : (which + 1) * 16, :] = rows
        stats.append(rows)
    norm, delta = stats
    text = key_ref.shape[0]
    pieces = levels_ref.shape[0] // 8
    sent = grad_ref.shape[0] // pieces
    piece = sent - 8

    def load(h):
        ready(h)
        cols = columns(h)
        q, g, k, v = (r[:, cols] for r in (query_ref, out_grad_ref, key_ref, value_ref))
        return q, g, k, v, norm[h : h + 1], delta[h : h + 1]

    def store(h, q, g, k, probs, score_grad):
        for part, grad in enumerate((nn(score_grad, q) * SCALE, nn(probs, g))):
            for at in range(0, text, 16):
                chip, within = divmod(h * text + at, piece)
                to = 2 * chip + part
                code, level = coded(grad[at : at + 16])
                grad_ref[to * sent + within : to * sent + within + 16, :] = code
                levels_ref[to * 8 + within // 16 : to * 8 + within // 16 + 1, :] = level

    backward(load, store, None)
    for to in range(pieces):
        levels = levels_ref[to * 8 : (to + 1) * 8, :].astype(jnp.int32).astype(I16)
        grad_ref[(to + 1) * sent - 8 : (to + 1) * sent, :] = levels


def over_chips_kernel(parts_ref, out_ref):
    count, sent, _ = parts_ref.shape
    total = 0.0
    for n in range(count):
        levels = wide(parts_ref[n, sent - 8 :, :])
        blocks = [
            decoded(parts_ref[n, 16 * b : 16 * b + 16, :], levels[b : b + 1])
            for b in range((sent - 8) // 16)
        ]
        total = total + jnp.concatenate(blocks, axis=0)
    code, level = coded(total)
    levels = levels_of([level])
    for n in range(out_ref.shape[0]):
        out_ref[n, : sent - 8, :] = code
        out_ref[n, sent - 8 :, :] = levels


def over_tiles_kernel(parts_ref, out_ref):
    count, sent, _ = parts_ref.shape
    total = 0.0
    for n in range(count):
        level = wide(parts_ref[n, sent - 8 :, :])[:1]
        total = total + decoded(parts_ref[n, : sent - 8, :], level)
    total = total.astype(BF16)
    for n in range(out_ref.shape[0]):
        out_ref[n] = total


BLOCK = 12


def backward(load, store, live):
    for first in range(0, HEADS, BLOCK):
        heads = range(first, first + BLOCK)
        given = [load(h) for h in heads]
        scores = [nt(k, q) for q, _, k, _, _, _ in given]
        prob_grads = [nt(v, g) for _, g, _, v, _, _ in given]
        made = []
        for (_, _, _, _, norm, delta), score, prob_grad in zip(given, scores, prob_grads):
            probs = jnp.exp(score * SCALE - norm)
            if live is not None:
                probs = probs * live
            made.append((probs.astype(BF16), (probs * (prob_grad - delta)).astype(BF16)))
        for h, (q, g, k, _, _, _), (probs, score_grad) in zip(heads, given, made):
            store(h, q, g, k, probs, score_grad)


def columns(h):
    return slice(h * HDIM, (h + 1) * HDIM)


def own_kernel(
    live_ref,
    stats_ref,
    query_ref,
    out_grad_ref,
    keys_ref,
    values_ref,
    text_key_ref,
    text_value_ref,
    part_ref,
    query_grad_ref,
    own_ref,
):
    text = text_key_ref.shape[0]
    rows = lax.broadcasted_iota(jnp.int32, (OWN + text, HDIM), 0)
    live = jnp.where(rows < OWN, live_ref[4].astype(F32), 1.0)

    def load(h):
        cols = columns(h)
        k = jnp.concatenate([keys_ref[:, cols], text_key_ref[:, cols]], axis=0)
        v = jnp.concatenate([values_ref[:, cols], text_value_ref[:, cols]], axis=0)
        norm, delta = stats_ref[h : h + 1, :], stats_ref[16 + h : 17 + h, :]
        return query_ref[:, cols], out_grad_ref[:, cols], k, v, norm, delta

    def store(h, q, g, k, probs, score_grad):
        cols = columns(h)
        query_grad = part_ref[:, cols] + tn(score_grad, k)
        query_grad_ref[:, cols] = (query_grad * SCALE).astype(BF16)
        own_ref[:OWN, cols] = nn(score_grad[:OWN], q) * SCALE
        own_ref[OWN:, cols] = nn(probs[:OWN], g)

    backward(load, store, live)


def band_kernel(
    live_ref,
    stats_ref,
    query_ref,
    out_grad_ref,
    top_ref,
    bottom_ref,
    part_ref,
    top_grad_ref,
    bottom_grad_ref,
    query_grad_ref,
):
    def live(block):
        return live_ref[block].astype(F32)

    band = lax.rem(lax.broadcasted_iota(jnp.int32, (ENDS, HDIM), 0), BAND)
    lives = [
        jnp.where(
            band < HALO * TILE,
            live(first + 1),
            jnp.where(band < HALO * TILE + CORNER, live(first), live(first + 2)),
        )
        for first in (0, 6)
    ]
    two_halves(
        (stats_ref, query_ref, out_grad_ref, top_ref, bottom_ref, part_ref),
        (top_grad_ref, bottom_grad_ref, query_grad_ref),
        jnp.concatenate(lives, axis=0),
        True,
    )


def side_kernel(
    live_ref,
    stats_ref,
    query_ref,
    out_grad_ref,
    left_ref,
    right_ref,
    side_grad_ref,
    query_grad_ref,
):
    rows = lax.broadcasted_iota(jnp.int32, (2 * SIDE, HDIM), 0)
    lives = jnp.where(rows < SIDE, live_ref[3].astype(F32), live_ref[5].astype(F32))
    two_halves(
        (stats_ref, query_ref, out_grad_ref, left_ref, right_ref, None),
        (side_grad_ref.at[: 2 * SIDE], side_grad_ref.at[2 * SIDE :], query_grad_ref),
        lives,
        False,
    )


def two_halves(given, made, live, code):
    stats_ref, query_ref, out_grad_ref, first_ref, second_ref, part_ref = given
    first_grad_ref, second_grad_ref, query_grad_ref = made
    rows = first_ref.shape[0] // 2

    def load(h):
        cols = columns(h)
        k, v = (
            jnp.concatenate([first_ref[at, cols], second_ref[at, cols]], axis=0)
            for at in (slice(0, rows), slice(rows, 2 * rows))
        )
        norm, delta = stats_ref[h : h + 1, :], stats_ref[16 + h : 17 + h, :]
        return query_ref[:, cols], out_grad_ref[:, cols], k, v, norm, delta

    def store(h, q, g, k, probs, score_grad):
        cols = columns(h)
        query_grad = tn(score_grad, k)
        query_grad_ref[:, cols] = query_grad if part_ref is None else part_ref[:, cols] + query_grad
        grads = (nn(score_grad, q) * SCALE, nn(probs, g))
        for n, ref in enumerate((first_grad_ref, second_grad_ref)):
            levels = []
            for at, grad in ((slice(0, rows), grads[0]), (slice(rows, 2 * rows), grads[1])):
                block = grad[n * rows : (n + 1) * rows]
                if code:
                    block, level = coded(block)
                    levels.append(level)
                ref[at, cols] = block
            if code:
                ref[2 * rows :, cols] = levels_of(levels)

    backward(load, store, live)


def received(ref, part, rows):
    level = wide(ref[2 * rows :, :])[part : part + 1]
    return decoded(ref[part * rows : (part + 1) * rows, :], level)


def corners_kernel(
    select_ref, sides_ref, above_ref, below_ref, left_out_ref, right_out_ref
):
    levels = ([], [])
    for part in range(2):
        side = slice(part * SIDE, (part + 1) * SIDE)
        bands = [received(ref, part, ENDS) for ref in (above_ref, below_ref)]
        more = picked(select_ref[...], jnp.concatenate(bands, axis=0))
        for n, out in enumerate((left_out_ref, right_out_ref)):
            here = sides_ref[(2 * n + part) * SIDE : (2 * n + part + 1) * SIDE, :]
            code, level = coded(here + more[n * SIDE : (n + 1) * SIDE])
            out[side, :] = code
            levels[n].append(level)
    left_out_ref[2 * SIDE :, :] = levels_of(levels[0])
    right_out_ref[2 * SIDE :, :] = levels_of(levels[1])


def sum_kernel(
    select_ref, own_ref, left_ref, right_ref, above_ref, below_ref, key_ref, value_ref
):
    edge = HALO * TILE
    for part, out in enumerate((key_ref, value_ref)):
        above, below = received(above_ref, part, ENDS), received(below_ref, part, ENDS)
        sides = [received(ref, part, SIDE) for ref in (left_ref, right_ref)]
        rows = jnp.concatenate(sides, axis=0)
        total = own_ref[part * OWN : (part + 1) * OWN, :] + picked(select_ref[...], rows)
        for frame in range(FRAMES):
            at = frame * BAND
            top = frame * TILE * TILE
            bottom = top + TILE * TILE - edge
            end = top + TILE * TILE
            out[top : top + edge, :] = (
                total[top : top + edge] + above[at : at + edge]
            ).astype(BF16)
            out[top + edge : bottom, :] = total[top + edge : bottom].astype(BF16)
            out[bottom:end, :] = (total[bottom:end] + below[at : at + edge]).astype(BF16)


def words_kernel(parts_ref, key_ref, value_ref):
    text = key_ref.shape[0]
    rows = parts_ref.shape[1]
    for part, out in enumerate((key_ref, value_ref)):
        for h in range(HEADS):
            for at in range(0, text, 16):
                chip, within = divmod(h * text + at, rows)
                piece = parts_ref[2 * chip + part, within : within + 16, :]
                out[at : at + 16, h * HDIM : (h + 1) * HDIM] = piece


def call(kernel, outs, ins, us=1.0, smem=0, fetch=False, scratch=()):
    groups = HEADS // GROUP
    step = GROUP * HDIM

    def body(*refs):
        n = len(ins)
        outputs = refs[n : n + len(outs)]
        buffers = refs[n + len(outs) : 2 * n + len(outs)]
        semaphores, *rest = refs[2 * n + len(outs) :]
        small, wide = [], [[] for _ in range(groups)]
        for i, (far, near) in enumerate(zip(refs[:n], buffers)):
            if ins[i].ndim == 2 and ins[i].shape[1] == groups * step:
                for m in range(groups):
                    at = (slice(None), slice(m * step, (m + 1) * step))
                    copy = pltpu.make_async_copy(far.at[at], near.at[at], semaphores.at[i, m])
                    wide[m].append(copy)
            else:
                small.append(pltpu.make_async_copy(far, near, semaphores.at[i, 0]))
        for copies in (small, *wide):
            for copy in copies:
                copy.start()
        for copy in small:
            copy.wait()

        def ready(h):
            if h % GROUP == 0:
                for copy in wide[h // GROUP]:
                    copy.wait()

        kernel(ready, *buffers, *outputs, *rest)

    here = pl.BlockSpec(memory_space=pltpu.VMEM)
    scalars = pl.BlockSpec(memory_space=pltpu.SMEM)
    if not fetch:
        function, specs, scratch, limit = kernel, [scalars] * smem + [here] * (len(ins) - smem), [*scratch], 16
    else:
        function, specs, limit = body, [pl.BlockSpec(memory_space=pltpu.HBM)] * len(ins), 56
        buffers = [pltpu.VMEM(a.shape, a.dtype) for a in ins]
        scratch = [*buffers, pltpu.SemaphoreType.DMA((len(ins), groups)), *scratch]
    return pl.pallas_call(
        function,
        out_shape=[jax.ShapeDtypeStruct(shape, dtype) for shape, dtype in outs],
        in_specs=specs,
        out_specs=[here] * len(outs),
        scratch_shapes=scratch,
        compiler_params=pltpu.CompilerParams(vmem_limit_bytes=limit * 2**20),
        cost_estimate=pl.CostEstimate(
            flops=int(us * 50000000), bytes_accessed=1000000, transcendentals=0
        ),
    )(*ins)


def shifted(value, axis, steps):
    count = lax.axis_size(axis)
    return lax.ppermute(value, axis, [(i, (i + steps) % count) for i in range(count)])


def by_query(rows):
    return rows.transpose(1, 2, 3, 0).reshape(OWN, HEADS)


def exchanged(pieces, axis):
    return lax.all_to_all(pieces, axis, 0, 0, tiled=True)


def local(
    queries, keys, values, out_grad, log_norm, delta_rows, text_keys, text_values, window_table
):
    shape = queries.shape
    width = shape[-1]
    text = text_keys.shape[0]
    q = queries.reshape(OWN, width)
    g = out_grad.reshape(OWN, width)
    k = keys.reshape(OWN, width)
    v = values.reshape(OWN, width)
    anchor = jnp.zeros((), jnp.int32)
    live = lax.dynamic_slice(
        window_table, (lax.axis_index(HA), lax.axis_index("wa"), anchor), (1, 1, 9)
    ).reshape(9)

    count = lax.axis_size(HA)
    piece = 2 * HEADS * text // count
    sent = piece + 8
    words, stats = call(
        text_kernel,
        [((count * sent, HDIM), I16), ((32, HDIM), F32)],
        [by_query(log_norm), by_query(delta_rows), q, g, text_keys, text_values],
        us=3,
        fetch=True,
        scratch=[pltpu.VMEM((count * 8, HDIM), F32)],
    )
    words = exchanged(words.reshape(count, sent, HDIM), HA)
    tiles = lax.axis_size("wa")
    (words,) = call(over_chips_kernel, [((tiles, sent, HDIM), I16)], [words])
    words = exchanged(words, "wa")
    (words,) = call(over_tiles_kernel, [((count, piece, HDIM), BF16)], [words])
    words = exchanged(words, HA)
    text_key_grad, text_value_grad = call(
        words_kernel, [((text, width), BF16)] * 2, [words]
    )

    left, right = call(
        sides_kernel, [((2 * SIDE, width), BF16)] * 2, [jnp.asarray(SIDES, BF16), k, v]
    )
    from_right = shifted(left, "wa", -1)
    from_left = shifted(right, "wa", 1)
    top, bottom = call(
        ends_kernel,
        [((2 * ENDS, width), BF16)] * 2,
        [jnp.asarray(BANDS, BF16), k, v, from_left, from_right],
    )
    from_below = shifted(top, HA, -1)
    from_above = shifted(bottom, HA, 1)
    side_grad, part = call(
        side_kernel,
        [((4 * SIDE, width), F32), ((OWN, width), F32)],
        [live, stats, q, g, from_left, from_right],
        us=2,
        smem=1,
    )
    top_grad, bottom_grad, part = call(
        band_kernel,
        [((2 * ENDS + 8, width), I16)] * 2 + [((OWN, width), F32)],
        [live, stats, q, g, from_above, from_below, part],
        us=2,
        smem=1,
    )
    above = shifted(bottom_grad, HA, 1)
    below = shifted(top_grad, HA, -1)
    back = np.concatenate([BANDS[0].T, BANDS[1].T], axis=1)
    left_grad, right_grad = call(
        corners_kernel,
        [((2 * SIDE + 8, width), I16)] * 2,
        [jnp.asarray(back[OWN:], BF16), side_grad, above, below],
    )
    after = shifted(left_grad, "wa", -1)
    before = shifted(right_grad, "wa", 1)
    query_grad, own = call(
        own_kernel,
        [((OWN, width), BF16), ((2 * OWN, width), F32)],
        [live, stats, q, g, k, v, text_keys, text_values, part],
        us=3,
        smem=1,
    )
    back = np.concatenate([SIDES[0].T, SIDES[1].T], axis=1)
    key_grad, value_grad = call(
        sum_kernel,
        [((OWN, width), BF16)] * 2,
        [jnp.asarray(back, BF16), own, before, after, above, below],
    )
    return (
        query_grad.reshape(shape),
        key_grad.reshape(shape),
        value_grad.reshape(shape),
        text_key_grad,
        text_value_grad,
    )


def solution(mesh):
    split = Mesh(
        mesh.devices.reshape(mesh.shape["group"], 8, 2, mesh.shape["wa"]),
        ("group", "ha_0", "ha_1", "wa"),
    )
    return jax.shard_map(
        local,
        mesh=split,
        in_specs=(
            P("group", HA, "wa", None),
            P("group", HA, "wa", None),
            P("group", HA, "wa", None),
            P("group", HA, "wa", None),
            P(None, "group", HA, "wa"),
            P(None, "group", HA, "wa"),
            P("group", None),
            P("group", None),
            P(),
        ),
        out_specs=(
            P("group", HA, "wa", None),
            P("group", HA, "wa", None),
            P("group", HA, "wa", None),
            P("group", None),
            P("group", None),
        ),
        check_vma=False,
    )
```

```python
import math

import jax
import jax.numpy as jnp
import numpy as np
from jax import lax
from jax.experimental import pallas as pl
from jax.experimental.pallas import tpu as pltpu
from jax.sharding import Mesh
from jax.sharding import PartitionSpec as P


HEADS = 12
HDIM = 128
TILE = 8
HALO = 2
HA = ("ha_0", "ha_1")
WA = ("wa_0", "wa_1")
NEAR = (*HA, "wa_1")
F32 = jnp.float32
BF16 = jnp.bfloat16
SCALE = 1.0 / math.sqrt(HDIM)

FRAMES = 2
OWN = FRAMES * TILE * TILE
SIDE = FRAMES * TILE * HALO
CORNER = HALO * HALO
BAND = HALO * TILE + 2 * CORNER
ENDS = FRAMES * BAND


def nt(a, b):
    return lax.dot_general(a, b, (((1,), (1,)), ((), ())), preferred_element_type=F32)


def nn(a, b):
    return lax.dot_general(a, b, (((1,), (0,)), ((), ())), preferred_element_type=F32)


def tn(a, b):
    return lax.dot_general(a, b, (((0,), (0,)), ((), ())), preferred_element_type=F32)


def picked(select, rows):
    high = rows.astype(BF16)
    low = (rows - high.astype(F32)).astype(BF16)
    return nn(select, high) + nn(select, low)


STEPS = 128.0
MOST = 32000.0
I16 = jnp.int16


def scaled(x, level):
    half = jnp.exp2(level * (0.5 / STEPS))
    return (x * half) * half


def coded(x):
    most = jnp.maximum(jnp.max(jnp.abs(x), axis=0, keepdims=True), 2.0**-120)
    level = jnp.ceil(jnp.log2(most) * STEPS)
    code = jnp.floor(scaled(x, -level) * MOST + 0.5)
    return code.astype(jnp.int32).astype(I16), level


def levels_of(rows):
    blank = jnp.zeros((8 - len(rows), rows[0].shape[1]), F32)
    return jnp.concatenate([*rows, blank], axis=0).astype(jnp.int32).astype(I16)


def wide(code):
    return code.astype(jnp.int32).astype(F32)


def decoded(code, level):
    return scaled(wide(code) * (1.0 / MOST), level)


def own_row(frame, row, col):
    return frame * TILE * TILE + row * TILE + col


def side_row(frame, row, col):
    return (frame * TILE + row) * HALO + col


def select_sides():
    out = np.zeros((2, SIDE, OWN), np.float32)
    for side, first in enumerate((0, TILE - HALO)):
        for frame in range(FRAMES):
            for row in range(TILE):
                for col in range(HALO):
                    out[side, side_row(frame, row, col), own_row(frame, row, first + col)] = 1
    return out


def select_ends():
    out = np.zeros((2, ENDS, OWN + 2 * SIDE), np.float32)
    for end, first in enumerate((0, TILE - HALO)):
        for frame in range(FRAMES):
            at = frame * BAND
            for row in range(HALO):
                for col in range(TILE):
                    out[end, at, own_row(frame, first + row, col)] = 1
                    at += 1
            for side in range(2):
                for row in range(HALO):
                    for col in range(HALO):
                        out[end, at, OWN + side * SIDE + side_row(frame, first + row, col)] = 1
                        at += 1
    return out


SIDES = select_sides()
BANDS = select_ends()


GROUP = 2


def ends_kernel(select_ref, keys_ref, values_ref, left_ref, right_ref, top_ref, bottom_ref):
    for part, ref in enumerate((keys_ref, values_ref)):
        at = slice(part * SIDE, (part + 1) * SIDE)
        rows = jnp.concatenate([ref[...], left_ref[at, :], right_ref[at, :]], axis=0)
        to = slice(part * ENDS, (part + 1) * ENDS)
        top_ref[to, :] = nn(select_ref[0], rows).astype(BF16)
        bottom_ref[to, :] = nn(select_ref[1], rows).astype(BF16)


def sides_kernel(select_ref, keys_ref, values_ref, left_ref, right_ref):
    for part, ref in enumerate((keys_ref, values_ref)):
        rows = ref[...]
        at = slice(part * SIDE, (part + 1) * SIDE)
        left_ref[at, :] = nn(select_ref[0], rows).astype(BF16)
        right_ref[at, :] = nn(select_ref[1], rows).astype(BF16)


def place(part, row, rows):
    piece, within = divmod(row, rows)
    return 4 * (piece // 2) + 2 * part + piece % 2, within


def text_kernel(
    ready,
    norm_ref,
    delta_ref,
    query_ref,
    out_grad_ref,
    key_ref,
    value_ref,
    grad_ref,
    stats_ref,
    levels_ref,
):
    levels_ref[...] = jnp.zeros(levels_ref.shape, F32)
    heads = lax.broadcasted_iota(jnp.int32, (16, HEADS), 1)
    identity = (heads == lax.broadcasted_iota(jnp.int32, (16, HEADS), 0)).astype(F32)
    stats = []
    for which, ref in enumerate((norm_ref, delta_ref)):
        rows = lax.dot_general(
            identity,
            ref[...],
            (((1,), (1,)), ((), ())),
            precision=lax.Precision.HIGHEST,
            preferred_element_type=F32,
        )
        stats_ref[which * 16 : (which + 1) * 16, :] = rows
        stats.append(rows)
    norm, delta = stats
    text = key_ref.shape[0]
    pieces = levels_ref.shape[0] // 8
    sent = grad_ref.shape[0] // pieces
    piece = sent - 8

    def load(h):
        ready(h)
        cols = columns(h)
        q, g, k, v = (r[:, cols] for r in (query_ref, out_grad_ref, key_ref, value_ref))
        return q, g, k, v, norm[h : h + 1], delta[h : h + 1]

    def store(h, q, g, k, probs, score_grad):
        for part, grad in enumerate((nn(score_grad, q) * SCALE, nn(probs, g))):
            code, level = coded(grad)
            for at in range(0, text, 8):
                to, within = place(part, h * text + at, piece)
                grad_ref[to * sent + within : to * sent + within + 8, :] = code[at : at + 8]
                row = to * 8 + within // 8
                levels_ref[row : row + 1, :] = level

    backward(load, store, None)
    for to in range(pieces):
        levels = levels_ref[to * 8 : (to + 1) * 8, :].astype(jnp.int32).astype(I16)
        grad_ref[(to + 1) * sent - 8 : (to + 1) * sent, :] = levels


def over_chips_kernel(parts_ref, out_ref):
    count, sent, _ = parts_ref.shape
    total = 0.0
    for n in range(count):
        levels = wide(parts_ref[n, sent - 8 :, :])
        blocks = [
            decoded(parts_ref[n, 8 * b : 8 * b + 8, :], levels[b : b + 1])
            for b in range((sent - 8) // 8)
        ]
        total = total + jnp.concatenate(blocks, axis=0)
    code, level = coded(total)
    levels = levels_of([level])
    for n in range(out_ref.shape[0]):
        out_ref[n, : sent - 8, :] = code
        out_ref[n, sent - 8 :, :] = levels


def over_tiles_kernel(parts_ref, out_ref):
    count, sent, _ = parts_ref.shape
    total = 0.0
    for n in range(count):
        level = wide(parts_ref[n, sent - 8 :, :])[:1]
        total = total + decoded(parts_ref[n, : sent - 8, :], level)
    total = total.astype(BF16)
    for n in range(out_ref.shape[0]):
        out_ref[n] = total


BLOCK = 12


def backward(load, store, live):
    for first in range(0, HEADS, BLOCK):
        heads = range(first, first + BLOCK)
        given = [load(h) for h in heads]
        scores = [nt(k, q) for q, _, k, _, _, _ in given]
        prob_grads = [nt(v, g) for _, g, _, v, _, _ in given]
        made = []
        for (_, _, _, _, norm, delta), score, prob_grad in zip(given, scores, prob_grads):
            probs = jnp.exp(score * SCALE - norm)
            if live is not None:
                probs = probs * live
            made.append((probs.astype(BF16), (probs * (prob_grad - delta)).astype(BF16)))
        for h, (q, g, k, _, _, _), (probs, score_grad) in zip(heads, given, made):
            store(h, q, g, k, probs, score_grad)


def columns(h):
    return slice(h * HDIM, (h + 1) * HDIM)


def own_kernel(
    ready,
    live_ref,
    query_ref,
    out_grad_ref,
    keys_ref,
    values_ref,
    text_key_ref,
    text_value_ref,
    stats_ref,
    part_ref,
    query_grad_ref,
    own_ref,
):
    text = text_key_ref.shape[0]
    rows = lax.broadcasted_iota(jnp.int32, (OWN + text, HDIM), 0)
    live = jnp.where(rows < OWN, live_ref[4].astype(F32), 1.0)

    def load(h):
        ready(h)
        cols = columns(h)
        k = jnp.concatenate([keys_ref[:, cols], text_key_ref[:, cols]], axis=0)
        v = jnp.concatenate([values_ref[:, cols], text_value_ref[:, cols]], axis=0)
        norm, delta = stats_ref[h : h + 1, :], stats_ref[16 + h : 17 + h, :]
        return query_ref[:, cols], out_grad_ref[:, cols], k, v, norm, delta

    def store(h, q, g, k, probs, score_grad):
        cols = columns(h)
        query_grad = part_ref[:, cols] + tn(score_grad, k)
        query_grad_ref[:, cols] = (query_grad * SCALE).astype(BF16)
        own_ref[:OWN, cols] = nn(score_grad[:OWN], q) * SCALE
        own_ref[OWN:, cols] = nn(probs[:OWN], g)

    backward(load, store, live)


def band_kernel(
    live_ref,
    stats_ref,
    query_ref,
    out_grad_ref,
    top_ref,
    bottom_ref,
    part_ref,
    top_grad_ref,
    bottom_grad_ref,
    query_grad_ref,
):
    def live(block):
        return live_ref[block].astype(F32)

    band = lax.rem(lax.broadcasted_iota(jnp.int32, (ENDS, HDIM), 0), BAND)
    lives = [
        jnp.where(
            band < HALO * TILE,
            live(first + 1),
            jnp.where(band < HALO * TILE + CORNER, live(first), live(first + 2)),
        )
        for first in (0, 6)
    ]
    two_halves(
        (stats_ref, query_ref, out_grad_ref, top_ref, bottom_ref, part_ref),
        (top_grad_ref, bottom_grad_ref, query_grad_ref),
        jnp.concatenate(lives, axis=0),
        True,
    )


def side_kernel(
    live_ref,
    stats_ref,
    query_ref,
    out_grad_ref,
    left_ref,
    right_ref,
    side_grad_ref,
    query_grad_ref,
):
    rows = lax.broadcasted_iota(jnp.int32, (2 * SIDE, HDIM), 0)
    lives = jnp.where(rows < SIDE, live_ref[3].astype(F32), live_ref[5].astype(F32))
    two_halves(
        (stats_ref, query_ref, out_grad_ref, left_ref, right_ref, None),
        (side_grad_ref.at[: 2 * SIDE], side_grad_ref.at[2 * SIDE :], query_grad_ref),
        lives,
        False,
    )


def two_halves(given, made, live, code):
    stats_ref, query_ref, out_grad_ref, first_ref, second_ref, part_ref = given
    first_grad_ref, second_grad_ref, query_grad_ref = made
    rows = first_ref.shape[0] // 2

    def load(h):
        cols = columns(h)
        k, v = (
            jnp.concatenate([first_ref[at, cols], second_ref[at, cols]], axis=0)
            for at in (slice(0, rows), slice(rows, 2 * rows))
        )
        norm, delta = stats_ref[h : h + 1, :], stats_ref[16 + h : 17 + h, :]
        return query_ref[:, cols], out_grad_ref[:, cols], k, v, norm, delta

    def store(h, q, g, k, probs, score_grad):
        cols = columns(h)
        query_grad = tn(score_grad, k)
        query_grad_ref[:, cols] = query_grad if part_ref is None else part_ref[:, cols] + query_grad
        grads = (nn(score_grad, q) * SCALE, nn(probs, g))
        for n, ref in enumerate((first_grad_ref, second_grad_ref)):
            levels = []
            for at, grad in ((slice(0, rows), grads[0]), (slice(rows, 2 * rows), grads[1])):
                block = grad[n * rows : (n + 1) * rows]
                if code:
                    block, level = coded(block)
                    levels.append(level)
                ref[at, cols] = block
            if code:
                ref[2 * rows :, cols] = levels_of(levels)

    backward(load, store, live)


def received(ref, part, rows):
    level = wide(ref[2 * rows :, :])[part : part + 1]
    return decoded(ref[part * rows : (part + 1) * rows, :], level)


def corners_kernel(
    select_ref, sides_ref, above_ref, below_ref, left_out_ref, right_out_ref
):
    levels = ([], [])
    for part in range(2):
        side = slice(part * SIDE, (part + 1) * SIDE)
        bands = [received(ref, part, ENDS) for ref in (above_ref, below_ref)]
        more = picked(select_ref[...], jnp.concatenate(bands, axis=0))
        for n, out in enumerate((left_out_ref, right_out_ref)):
            here = sides_ref[(2 * n + part) * SIDE : (2 * n + part + 1) * SIDE, :]
            code, level = coded(here + more[n * SIDE : (n + 1) * SIDE])
            out[side, :] = code
            levels[n].append(level)
    left_out_ref[2 * SIDE :, :] = levels_of(levels[0])
    right_out_ref[2 * SIDE :, :] = levels_of(levels[1])


def sum_kernel(
    select_ref, own_ref, left_ref, right_ref, above_ref, below_ref, key_ref, value_ref
):
    edge = HALO * TILE
    for part, out in enumerate((key_ref, value_ref)):
        above, below = received(above_ref, part, ENDS), received(below_ref, part, ENDS)
        sides = [received(ref, part, SIDE) for ref in (left_ref, right_ref)]
        rows = jnp.concatenate(sides, axis=0)
        total = own_ref[part * OWN : (part + 1) * OWN, :] + picked(select_ref[...], rows)
        for frame in range(FRAMES):
            at = frame * BAND
            top = frame * TILE * TILE
            bottom = top + TILE * TILE - edge
            end = top + TILE * TILE
            out[top : top + edge, :] = (
                total[top : top + edge] + above[at : at + edge]
            ).astype(BF16)
            out[top + edge : bottom, :] = total[top + edge : bottom].astype(BF16)
            out[bottom:end, :] = (total[bottom:end] + below[at : at + edge]).astype(BF16)


def words_kernel(parts_ref, key_ref, value_ref):
    text = key_ref.shape[0]
    rows = parts_ref.shape[1]
    for part, out in enumerate((key_ref, value_ref)):
        for h in range(HEADS):
            for at in range(0, text, 8):
                to, within = place(part, h * text + at, rows)
                piece = parts_ref[to, within : within + 8, :]
                out[at : at + 8, h * HDIM : (h + 1) * HDIM] = piece


def call(kernel, outs, ins, us=1.0, smem=0, fetch=0, scratch=()):
    groups = HEADS // GROUP
    step = GROUP * HDIM

    def body(*refs):
        n = len(ins)
        outputs = refs[n : n + len(outs)]
        near_refs = refs[n + len(outs) : n + len(outs) + fetch]
        semaphores, *rest = refs[n + len(outs) + fetch :]
        small, wide = [], [[] for _ in range(groups)]
        for i, (far, near) in enumerate(zip(refs[smem : smem + fetch], near_refs)):
            if near.ndim == 2 and near.shape[1] == groups * step:
                for m in range(groups):
                    at = (slice(None), slice(m * step, (m + 1) * step))
                    copy = pltpu.make_async_copy(far.at[at], near.at[at], semaphores.at[i, m])
                    wide[m].append(copy)
            else:
                small.append(pltpu.make_async_copy(far, near, semaphores.at[i, 0]))
        for copies in (small, *wide):
            for copy in copies:
                copy.start()
        for copy in small:
            copy.wait()

        def ready(h):
            if h % GROUP == 0:
                for copy in wide[h // GROUP]:
                    copy.wait()

        kernel(ready, *refs[:smem], *near_refs, *refs[smem + fetch : n], *outputs, *rest)

    here = pl.BlockSpec(memory_space=pltpu.VMEM)
    scalars = pl.BlockSpec(memory_space=pltpu.SMEM)
    if not fetch:
        function, specs, scratch, limit = kernel, [scalars] * smem + [here] * (len(ins) - smem), [*scratch], 16
    else:
        function, limit = body, 56
        far = pl.BlockSpec(memory_space=pltpu.HBM)
        specs = [scalars] * smem + [far] * fetch + [here] * (len(ins) - smem - fetch)
        buffers = [pltpu.VMEM(a.shape, a.dtype) for a in ins[smem : smem + fetch]]
        scratch = [*buffers, pltpu.SemaphoreType.DMA((fetch, groups)), *scratch]
    return pl.pallas_call(
        function,
        out_shape=[jax.ShapeDtypeStruct(shape, dtype) for shape, dtype in outs],
        in_specs=specs,
        out_specs=[here] * len(outs),
        scratch_shapes=scratch,
        compiler_params=pltpu.CompilerParams(vmem_limit_bytes=limit * 2**20),
        cost_estimate=pl.CostEstimate(
            flops=int(us * 50000000), bytes_accessed=1000000, transcendentals=0
        ),
    )(*ins)


def shifted(value, axis, steps):
    count = lax.axis_size(axis)
    return lax.ppermute(value, axis, [(i, (i + steps) % count) for i in range(count)])


def by_query(rows):
    return rows.transpose(1, 2, 3, 0).reshape(OWN, HEADS)


def exchanged(pieces, axis):
    return lax.all_to_all(pieces, axis, 0, 0, tiled=True)


def local(
    queries, keys, values, out_grad, log_norm, delta_rows, text_keys, text_values, window_table
):
    shape = queries.shape
    width = shape[-1]
    text = text_keys.shape[0]
    q = queries.reshape(OWN, width)
    g = out_grad.reshape(OWN, width)
    k = keys.reshape(OWN, width)
    v = values.reshape(OWN, width)
    anchor = jnp.zeros((), jnp.int32)
    live = lax.dynamic_slice(
        window_table, (lax.axis_index(HA), lax.axis_index(WA), anchor), (1, 1, 9)
    ).reshape(9)

    count = lax.axis_size(NEAR)
    piece = 2 * HEADS * text // count
    sent = piece + 8
    words, stats = call(
        text_kernel,
        [((count * sent, HDIM), I16), ((32, HDIM), F32)],
        [by_query(log_norm), by_query(delta_rows), q, g, text_keys, text_values],
        us=3,
        fetch=6,
        scratch=[pltpu.VMEM((count * 8, HDIM), F32)],
    )
    words = exchanged(words.reshape(count, sent, HDIM), NEAR)
    tiles = lax.axis_size("wa_0")
    (words,) = call(over_chips_kernel, [((tiles, sent, HDIM), I16)], [words])
    words = exchanged(words, "wa_0")
    (words,) = call(over_tiles_kernel, [((count, piece, HDIM), BF16)], [words])
    words = exchanged(words, NEAR)
    text_key_grad, text_value_grad = call(
        words_kernel, [((text, width), BF16)] * 2, [words]
    )

    left, right = call(
        sides_kernel, [((2 * SIDE, width), BF16)] * 2, [jnp.asarray(SIDES, BF16), k, v]
    )
    from_right = shifted(left, WA, -1)
    from_left = shifted(right, WA, 1)
    top, bottom = call(
        ends_kernel,
        [((2 * ENDS, width), BF16)] * 2,
        [jnp.asarray(BANDS, BF16), k, v, from_left, from_right],
    )
    from_below = shifted(top, HA, -1)
    from_above = shifted(bottom, HA, 1)
    side_grad, part = call(
        side_kernel,
        [((4 * SIDE, width), F32), ((OWN, width), F32)],
        [live, stats, q, g, from_left, from_right],
        us=2,
        smem=1,
    )
    top_grad, bottom_grad, part = call(
        band_kernel,
        [((2 * ENDS + 8, width), I16)] * 2 + [((OWN, width), F32)],
        [live, stats, q, g, from_above, from_below, part],
        us=2,
        smem=1,
    )
    above = shifted(bottom_grad, HA, 1)
    below = shifted(top_grad, HA, -1)
    back = np.concatenate([BANDS[0].T, BANDS[1].T], axis=1)
    left_grad, right_grad = call(
        corners_kernel,
        [((2 * SIDE + 8, width), I16)] * 2,
        [jnp.asarray(back[OWN:], BF16), side_grad, above, below],
    )
    after = shifted(left_grad, WA, -1)
    before = shifted(right_grad, WA, 1)
    query_grad, own = call(
        own_kernel,
        [((OWN, width), BF16), ((2 * OWN, width), F32)],
        [live, q, g, k, v, text_keys, text_values, stats, part],
        us=3,
        smem=1,
        fetch=6,
    )
    back = np.concatenate([SIDES[0].T, SIDES[1].T], axis=1)
    key_grad, value_grad = call(
        sum_kernel,
        [((OWN, width), BF16)] * 2,
        [jnp.asarray(back, BF16), own, before, after, above, below],
    )
    return (
        query_grad.reshape(shape),
        key_grad.reshape(shape),
        value_grad.reshape(shape),
        text_key_grad,
        text_value_grad,
    )


def solution(mesh):
    split = Mesh(
        mesh.devices.reshape(mesh.shape["group"], 8, 2, mesh.shape["wa"] // 2, 2),
        ("group", "ha_0", "ha_1", "wa_0", "wa_1"),
    )
    return jax.shard_map(
        local,
        mesh=split,
        in_specs=(
            P("group", HA, WA, None),
            P("group", HA, WA, None),
            P("group", HA, WA, None),
            P("group", HA, WA, None),
            P(None, "group", HA, WA),
            P(None, "group", HA, WA),
            P("group", None),
            P("group", None),
            P(),
        ),
        out_specs=(
            P("group", HA, WA, None),
            P("group", HA, WA, None),
            P("group", HA, WA, None),
            P("group", None),
            P("group", None),
        ),
        check_vma=False,
    )
```

```python
import math

import jax
import jax.numpy as jnp
import numpy as np
from jax import lax
from jax.experimental import pallas as pl
from jax.experimental.pallas import tpu as pltpu
from jax.sharding import Mesh
from jax.sharding import PartitionSpec as P


HEADS = 12
HDIM = 128
TILE = 8
HALO = 2
HA = ("ha_0", "ha_1")
WA = ("wa_0", "wa_1")
NEAR = (*HA, "wa_1")
F32 = jnp.float32
BF16 = jnp.bfloat16
SCALE = 1.0 / math.sqrt(HDIM)

FRAMES = 2
OWN = FRAMES * TILE * TILE
SIDE = FRAMES * TILE * HALO
CORNER = HALO * HALO
BAND = HALO * TILE + 2 * CORNER
ENDS = FRAMES * BAND


def nt(a, b):
    return lax.dot_general(a, b, (((1,), (1,)), ((), ())), preferred_element_type=F32)


def nn(a, b):
    return lax.dot_general(a, b, (((1,), (0,)), ((), ())), preferred_element_type=F32)


def tn(a, b):
    return lax.dot_general(a, b, (((0,), (0,)), ((), ())), preferred_element_type=F32)


def picked(select, rows):
    high = rows.astype(BF16)
    low = (rows - high.astype(F32)).astype(BF16)
    return nn(select, high) + nn(select, low)


STEPS = 128.0
MOST = 32000.0
I16 = jnp.int16


def scaled(x, level):
    half = jnp.exp2(level * (0.5 / STEPS))
    return (x * half) * half


def coded(x):
    most = jnp.maximum(jnp.max(jnp.abs(x), axis=0, keepdims=True), 2.0**-120)
    level = jnp.ceil(jnp.log2(most) * STEPS)
    code = jnp.floor(scaled(x, -level) * MOST + 0.5)
    return code.astype(jnp.int32).astype(I16), level


def levels_of(rows):
    blank = jnp.zeros((8 - len(rows), rows[0].shape[1]), F32)
    return jnp.concatenate([*rows, blank], axis=0).astype(jnp.int32).astype(I16)


def wide(code):
    return code.astype(jnp.int32).astype(F32)


def decoded(code, level):
    return scaled(wide(code) * (1.0 / MOST), level)


def own_row(frame, row, col):
    return frame * TILE * TILE + row * TILE + col


def side_row(frame, row, col):
    return (frame * TILE + row) * HALO + col


def select_sides():
    out = np.zeros((2, SIDE, OWN), np.float32)
    for side, first in enumerate((0, TILE - HALO)):
        for frame in range(FRAMES):
            for row in range(TILE):
                for col in range(HALO):
                    out[side, side_row(frame, row, col), own_row(frame, row, first + col)] = 1
    return out


def select_ends():
    out = np.zeros((2, ENDS, OWN + 2 * SIDE), np.float32)
    for end, first in enumerate((0, TILE - HALO)):
        for frame in range(FRAMES):
            at = frame * BAND
            for row in range(HALO):
                for col in range(TILE):
                    out[end, at, own_row(frame, first + row, col)] = 1
                    at += 1
            for side in range(2):
                for row in range(HALO):
                    for col in range(HALO):
                        out[end, at, OWN + side * SIDE + side_row(frame, first + row, col)] = 1
                        at += 1
    return out


SIDES = select_sides()
BANDS = select_ends()


GROUP = 2


def ends_kernel(select_ref, keys_ref, values_ref, left_ref, right_ref, top_ref, bottom_ref):
    for part, ref in enumerate((keys_ref, values_ref)):
        at = slice(part * SIDE, (part + 1) * SIDE)
        rows = jnp.concatenate([ref[...], left_ref[at, :], right_ref[at, :]], axis=0)
        to = slice(part * ENDS, (part + 1) * ENDS)
        top_ref[to, :] = nn(select_ref[0], rows).astype(BF16)
        bottom_ref[to, :] = nn(select_ref[1], rows).astype(BF16)


def sides_kernel(select_ref, keys_ref, values_ref, left_ref, right_ref):
    for part, ref in enumerate((keys_ref, values_ref)):
        rows = ref[...]
        at = slice(part * SIDE, (part + 1) * SIDE)
        left_ref[at, :] = nn(select_ref[0], rows).astype(BF16)
        right_ref[at, :] = nn(select_ref[1], rows).astype(BF16)


def place(part, row, rows):
    piece, within = divmod(row, rows)
    return 4 * (piece // 2) + 2 * part + piece % 2, within


def text_kernel(
    ready,
    norm_ref,
    delta_ref,
    query_ref,
    out_grad_ref,
    key_ref,
    value_ref,
    grad_ref,
    stats_ref,
    levels_ref,
):
    levels_ref[...] = jnp.zeros(levels_ref.shape, F32)
    heads = lax.broadcasted_iota(jnp.int32, (16, HEADS), 1)
    identity = (heads == lax.broadcasted_iota(jnp.int32, (16, HEADS), 0)).astype(F32)
    stats = []
    for which, ref in enumerate((norm_ref, delta_ref)):
        rows = lax.dot_general(
            identity,
            ref[...],
            (((1,), (1,)), ((), ())),
            precision=lax.Precision.HIGHEST,
            preferred_element_type=F32,
        )
        stats_ref[which * 16 : (which + 1) * 16, :] = rows
        stats.append(rows)
    norm, delta = stats
    text = key_ref.shape[0]
    pieces = levels_ref.shape[0] // 8
    sent = grad_ref.shape[0] // pieces
    piece = sent - 8

    def load(h):
        ready(h)
        cols = columns(h)
        q, g, k, v = (r[:, cols] for r in (query_ref, out_grad_ref, key_ref, value_ref))
        return q, g, k, v, norm[h : h + 1], delta[h : h + 1]

    def store(h, q, g, k, probs, score_grad):
        for part, grad in enumerate((nn(score_grad, q) * SCALE, nn(probs, g))):
            code, level = coded(grad)
            for at in range(0, text, 8):
                to, within = place(part, h * text + at, piece)
                grad_ref[to * sent + within : to * sent + within + 8, :] = code[at : at + 8]
                row = to * 8 + within // 8
                levels_ref[row : row + 1, :] = level

    backward(load, store, None)
    for to in range(pieces):
        levels = levels_ref[to * 8 : (to + 1) * 8, :].astype(jnp.int32).astype(I16)
        grad_ref[(to + 1) * sent - 8 : (to + 1) * sent, :] = levels


def over_chips_kernel(parts_ref, out_ref):
    count, sent, _ = parts_ref.shape
    total = 0.0
    for n in range(count):
        levels = wide(parts_ref[n, sent - 8 :, :])
        blocks = [
            decoded(parts_ref[n, 8 * b : 8 * b + 8, :], levels[b : b + 1])
            for b in range((sent - 8) // 8)
        ]
        total = total + jnp.concatenate(blocks, axis=0)
    code, level = coded(total)
    levels = levels_of([level])
    for n in range(out_ref.shape[0]):
        out_ref[n, : sent - 8, :] = code
        out_ref[n, sent - 8 :, :] = levels


def over_tiles_kernel(parts_ref, out_ref):
    count, sent, _ = parts_ref.shape
    total = 0.0
    for n in range(count):
        level = wide(parts_ref[n, sent - 8 :, :])[:1]
        total = total + decoded(parts_ref[n, : sent - 8, :], level)
    total = total.astype(BF16)
    for n in range(out_ref.shape[0]):
        out_ref[n] = total


BLOCK = 12


def backward(load, store, live):
    for first in range(0, HEADS, BLOCK):
        heads = range(first, first + BLOCK)
        given = [load(h) for h in heads]
        scores = [nt(k, q) for q, _, k, _, _, _ in given]
        prob_grads = [nt(v, g) for _, g, _, v, _, _ in given]
        made = []
        for (_, _, _, _, norm, delta), score, prob_grad in zip(given, scores, prob_grads):
            probs = jnp.exp(score * SCALE - norm)
            if live is not None:
                probs = probs * live
            made.append((probs.astype(BF16), (probs * (prob_grad - delta)).astype(BF16)))
        for h, (q, g, k, _, _, _), (probs, score_grad) in zip(heads, given, made):
            store(h, q, g, k, probs, score_grad)


def columns(h):
    return slice(h * HDIM, (h + 1) * HDIM)


def own_kernel(
    live_ref,
    query_ref,
    out_grad_ref,
    keys_ref,
    values_ref,
    text_key_ref,
    text_value_ref,
    stats_ref,
    part_ref,
    query_grad_ref,
    own_ref,
):
    text = text_key_ref.shape[0]
    rows = lax.broadcasted_iota(jnp.int32, (OWN + text, HDIM), 0)
    live = jnp.where(rows < OWN, live_ref[4].astype(F32), 1.0)

    def load(h):
        cols = columns(h)
        k = jnp.concatenate([keys_ref[:, cols], text_key_ref[:, cols]], axis=0)
        v = jnp.concatenate([values_ref[:, cols], text_value_ref[:, cols]], axis=0)
        norm, delta = stats_ref[h : h + 1, :], stats_ref[16 + h : 17 + h, :]
        return query_ref[:, cols], out_grad_ref[:, cols], k, v, norm, delta

    def store(h, q, g, k, probs, score_grad):
        cols = columns(h)
        query_grad_ref[:, cols] = part_ref[:, cols] + tn(score_grad, k)
        own_ref[:OWN, cols] = nn(score_grad[:OWN], q) * SCALE
        own_ref[OWN:, cols] = nn(probs[:OWN], g)

    backward(load, store, live)


def band_kernel(
    live_ref,
    stats_ref,
    query_ref,
    out_grad_ref,
    top_ref,
    bottom_ref,
    part_ref,
    top_grad_ref,
    bottom_grad_ref,
    query_grad_ref,
):
    def live(block):
        return live_ref[block].astype(F32)

    band = lax.rem(lax.broadcasted_iota(jnp.int32, (ENDS, HDIM), 0), BAND)
    lives = [
        jnp.where(
            band < HALO * TILE,
            live(first + 1),
            jnp.where(band < HALO * TILE + CORNER, live(first), live(first + 2)),
        )
        for first in (0, 6)
    ]
    two_halves(
        (stats_ref, query_ref, out_grad_ref, top_ref, bottom_ref, part_ref),
        (top_grad_ref, bottom_grad_ref, query_grad_ref),
        jnp.concatenate(lives, axis=0),
    )


def side_kernel(
    live_ref,
    stats_ref,
    query_ref,
    out_grad_ref,
    left_ref,
    right_ref,
    side_grad_ref,
    query_grad_ref,
):
    rows = lax.broadcasted_iota(jnp.int32, (2 * SIDE, HDIM), 0)
    lives = jnp.where(rows < SIDE, live_ref[3].astype(F32), live_ref[5].astype(F32))
    two_halves(
        (stats_ref, query_ref, out_grad_ref, left_ref, right_ref, None),
        (side_grad_ref.at[: 2 * SIDE + 8], side_grad_ref.at[2 * SIDE + 8 :], query_grad_ref),
        lives,
    )


def two_halves(given, made, live):
    stats_ref, query_ref, out_grad_ref, first_ref, second_ref, part_ref = given
    first_grad_ref, second_grad_ref, query_grad_ref = made
    rows = first_ref.shape[0] // 2

    def load(h):
        cols = columns(h)
        k, v = (
            jnp.concatenate([first_ref[at, cols], second_ref[at, cols]], axis=0)
            for at in (slice(0, rows), slice(rows, 2 * rows))
        )
        norm, delta = stats_ref[h : h + 1, :], stats_ref[16 + h : 17 + h, :]
        return query_ref[:, cols], out_grad_ref[:, cols], k, v, norm, delta

    def store(h, q, g, k, probs, score_grad):
        cols = columns(h)
        query_grad = tn(score_grad, k)
        if part_ref is not None:
            query_grad = ((part_ref[:, cols] + query_grad) * SCALE).astype(BF16)
        query_grad_ref[:, cols] = query_grad
        grads = (nn(score_grad, q) * SCALE, nn(probs, g))
        for n, ref in enumerate((first_grad_ref, second_grad_ref)):
            levels = []
            for at, grad in ((slice(0, rows), grads[0]), (slice(rows, 2 * rows), grads[1])):
                code, level = coded(grad[n * rows : (n + 1) * rows])
                ref[at, cols] = code
                levels.append(level)
            ref[2 * rows :, cols] = levels_of(levels)

    backward(load, store, live)


def received(ref, part, rows):
    level = wide(ref[2 * rows :, :])[part : part + 1]
    return decoded(ref[part * rows : (part + 1) * rows, :], level)


def corners_kernel(
    select_ref, sides_ref, above_ref, below_ref, left_out_ref, right_out_ref
):
    levels = ([], [])
    for part in range(2):
        side = slice(part * SIDE, (part + 1) * SIDE)
        bands = [received(ref, part, ENDS) for ref in (above_ref, below_ref)]
        more = picked(select_ref[...], jnp.concatenate(bands, axis=0))
        for n, out in enumerate((left_out_ref, right_out_ref)):
            rows = 2 * SIDE + 8
            here = received(sides_ref.at[n * rows : (n + 1) * rows], part, SIDE)
            code, level = coded(here + more[n * SIDE : (n + 1) * SIDE])
            out[side, :] = code
            levels[n].append(level)
    left_out_ref[2 * SIDE :, :] = levels_of(levels[0])
    right_out_ref[2 * SIDE :, :] = levels_of(levels[1])


def sum_kernel(
    select_ref, own_ref, left_ref, right_ref, above_ref, below_ref, key_ref, value_ref
):
    edge = HALO * TILE
    for part, out in enumerate((key_ref, value_ref)):
        above, below = received(above_ref, part, ENDS), received(below_ref, part, ENDS)
        sides = [received(ref, part, SIDE) for ref in (left_ref, right_ref)]
        rows = jnp.concatenate(sides, axis=0)
        total = own_ref[part * OWN : (part + 1) * OWN, :] + picked(select_ref[...], rows)
        for frame in range(FRAMES):
            at = frame * BAND
            top = frame * TILE * TILE
            bottom = top + TILE * TILE - edge
            end = top + TILE * TILE
            out[top : top + edge, :] = (
                total[top : top + edge] + above[at : at + edge]
            ).astype(BF16)
            out[top + edge : bottom, :] = total[top + edge : bottom].astype(BF16)
            out[bottom:end, :] = (total[bottom:end] + below[at : at + edge]).astype(BF16)


def words_kernel(parts_ref, key_ref, value_ref):
    text = key_ref.shape[0]
    rows = parts_ref.shape[1]
    for part, out in enumerate((key_ref, value_ref)):
        for h in range(HEADS):
            for at in range(0, text, 8):
                to, within = place(part, h * text + at, rows)
                piece = parts_ref[to, within : within + 8, :]
                out[at : at + 8, h * HDIM : (h + 1) * HDIM] = piece


def call(kernel, outs, ins, us=1.0, smem=0, fetch=0, scratch=()):
    groups = HEADS // GROUP
    step = GROUP * HDIM

    def body(*refs):
        n = len(ins)
        outputs = refs[n : n + len(outs)]
        near_refs = refs[n + len(outs) : n + len(outs) + fetch]
        semaphores, *rest = refs[n + len(outs) + fetch :]
        small, wide = [], [[] for _ in range(groups)]
        for i, (far, near) in enumerate(zip(refs[smem : smem + fetch], near_refs)):
            if near.ndim == 2 and near.shape[1] == groups * step:
                for m in range(groups):
                    at = (slice(None), slice(m * step, (m + 1) * step))
                    copy = pltpu.make_async_copy(far.at[at], near.at[at], semaphores.at[i, m])
                    wide[m].append(copy)
            else:
                small.append(pltpu.make_async_copy(far, near, semaphores.at[i, 0]))
        for copies in (small, *wide):
            for copy in copies:
                copy.start()
        for copy in small:
            copy.wait()

        def ready(h):
            if h % GROUP == 0:
                for copy in wide[h // GROUP]:
                    copy.wait()

        kernel(ready, *refs[:smem], *near_refs, *refs[smem + fetch : n], *outputs, *rest)

    here = pl.BlockSpec(memory_space=pltpu.VMEM)
    scalars = pl.BlockSpec(memory_space=pltpu.SMEM)
    if not fetch:
        function, specs, scratch, limit = kernel, [scalars] * smem + [here] * (len(ins) - smem), [*scratch], 16
    else:
        function, limit = body, 56
        far = pl.BlockSpec(memory_space=pltpu.HBM)
        specs = [scalars] * smem + [far] * fetch + [here] * (len(ins) - smem - fetch)
        buffers = [pltpu.VMEM(a.shape, a.dtype) for a in ins[smem : smem + fetch]]
        scratch = [*buffers, pltpu.SemaphoreType.DMA((fetch, groups)), *scratch]
    return pl.pallas_call(
        function,
        out_shape=[jax.ShapeDtypeStruct(shape, dtype) for shape, dtype in outs],
        in_specs=specs,
        out_specs=[here] * len(outs),
        scratch_shapes=scratch,
        compiler_params=pltpu.CompilerParams(vmem_limit_bytes=limit * 2**20),
        cost_estimate=pl.CostEstimate(
            flops=int(us * 50000000), bytes_accessed=1000000, transcendentals=0
        ),
    )(*ins)


def shifted(value, axis, steps):
    count = lax.axis_size(axis)
    return lax.ppermute(value, axis, [(i, (i + steps) % count) for i in range(count)])


def by_query(rows):
    return rows.transpose(1, 2, 3, 0).reshape(OWN, HEADS)


def exchanged(pieces, axis):
    return lax.all_to_all(pieces, axis, 0, 0, tiled=True)


def local(
    queries, keys, values, out_grad, log_norm, delta_rows, text_keys, text_values, window_table
):
    shape = queries.shape
    width = shape[-1]
    text = text_keys.shape[0]
    q = queries.reshape(OWN, width)
    g = out_grad.reshape(OWN, width)
    k = keys.reshape(OWN, width)
    v = values.reshape(OWN, width)
    anchor = jnp.zeros((), jnp.int32)
    live = lax.dynamic_slice(
        window_table, (lax.axis_index(HA), lax.axis_index(WA), anchor), (1, 1, 9)
    ).reshape(9)

    count = lax.axis_size(NEAR)
    piece = 2 * HEADS * text // count
    sent = piece + 8
    words, stats = call(
        text_kernel,
        [((count * sent, HDIM), I16), ((32, HDIM), F32)],
        [by_query(log_norm), by_query(delta_rows), q, g, text_keys, text_values],
        us=3,
        fetch=6,
        scratch=[pltpu.VMEM((count * 8, HDIM), F32)],
    )
    words = exchanged(words.reshape(count, sent, HDIM), NEAR)
    tiles = lax.axis_size("wa_0")
    (words,) = call(over_chips_kernel, [((tiles, sent, HDIM), I16)], [words])
    words = exchanged(words, "wa_0")
    (words,) = call(over_tiles_kernel, [((count, piece, HDIM), BF16)], [words])
    words = exchanged(words, NEAR)
    text_key_grad, text_value_grad = call(
        words_kernel, [((text, width), BF16)] * 2, [words]
    )

    left, right = call(
        sides_kernel, [((2 * SIDE, width), BF16)] * 2, [jnp.asarray(SIDES, BF16), k, v]
    )
    from_right = shifted(left, WA, -1)
    from_left = shifted(right, WA, 1)
    top, bottom = call(
        ends_kernel,
        [((2 * ENDS, width), BF16)] * 2,
        [jnp.asarray(BANDS, BF16), k, v, from_left, from_right],
    )
    from_below = shifted(top, HA, -1)
    from_above = shifted(bottom, HA, 1)
    side_grad, part = call(
        side_kernel,
        [((4 * SIDE + 16, width), I16), ((OWN, width), F32)],
        [live, stats, q, g, from_left, from_right],
        us=2,
        smem=1,
    )
    part, own = call(
        own_kernel,
        [((OWN, width), F32), ((2 * OWN, width), F32)],
        [live, q, g, k, v, text_keys, text_values, stats, part],
        us=3,
        smem=1,
    )
    top_grad, bottom_grad, query_grad = call(
        band_kernel,
        [((2 * ENDS + 8, width), I16)] * 2 + [((OWN, width), BF16)],
        [live, stats, q, g, from_above, from_below, part],
        us=2,
        smem=1,
    )
    above = shifted(bottom_grad, HA, 1)
    below = shifted(top_grad, HA, -1)
    back = np.concatenate([BANDS[0].T, BANDS[1].T], axis=1)
    left_grad, right_grad = call(
        corners_kernel,
        [((2 * SIDE + 8, width), I16)] * 2,
        [jnp.asarray(back[OWN:], BF16), side_grad, above, below],
    )
    after = shifted(left_grad, WA, -1)
    before = shifted(right_grad, WA, 1)
    back = np.concatenate([SIDES[0].T, SIDES[1].T], axis=1)
    key_grad, value_grad = call(
        sum_kernel,
        [((OWN, width), BF16)] * 2,
        [jnp.asarray(back, BF16), own, before, after, above, below],
    )
    return (
        query_grad.reshape(shape),
        key_grad.reshape(shape),
        value_grad.reshape(shape),
        text_key_grad,
        text_value_grad,
    )


def solution(mesh):
    split = Mesh(
        mesh.devices.reshape(mesh.shape["group"], 8, 2, mesh.shape["wa"] // 2, 2),
        ("group", "ha_0", "ha_1", "wa_0", "wa_1"),
    )
    return jax.shard_map(
        local,
        mesh=split,
        in_specs=(
            P("group", HA, WA, None),
            P("group", HA, WA, None),
            P("group", HA, WA, None),
            P("group", HA, WA, None),
            P(None, "group", HA, WA),
            P(None, "group", HA, WA),
            P("group", None),
            P("group", None),
            P(),
        ),
        out_specs=(
            P("group", HA, WA, None),
            P("group", HA, WA, None),
            P("group", HA, WA, None),
            P("group", None),
            P("group", None),
        ),
        check_vma=False,
    )
```

```python
import math

import jax
import jax.numpy as jnp
import numpy as np
from jax import lax
from jax.experimental import pallas as pl
from jax.experimental.pallas import tpu as pltpu
from jax.sharding import Mesh
from jax.sharding import PartitionSpec as P


HEADS = 12
HDIM = 128
TILE = 8
HALO = 2
HA = ("ha_0", "ha_1")
WA = ("wa_0", "wa_1")
NEAR = (*HA, "wa_1")
F32 = jnp.float32
BF16 = jnp.bfloat16
SCALE = 1.0 / math.sqrt(HDIM)

FRAMES = 2
OWN = FRAMES * TILE * TILE
SIDE = FRAMES * TILE * HALO
CORNER = HALO * HALO
BAND = HALO * TILE + 2 * CORNER
ENDS = FRAMES * BAND


def nt(a, b):
    return lax.dot_general(a, b, (((1,), (1,)), ((), ())), preferred_element_type=F32)


def nn(a, b):
    return lax.dot_general(a, b, (((1,), (0,)), ((), ())), preferred_element_type=F32)


def tn(a, b):
    return lax.dot_general(a, b, (((0,), (0,)), ((), ())), preferred_element_type=F32)


def picked(select, rows):
    high = rows.astype(BF16)
    low = (rows - high.astype(F32)).astype(BF16)
    return nn(select, high) + nn(select, low)


STEPS = 128.0
MOST = 32000.0
I16 = jnp.int16


def scaled(x, level):
    half = jnp.exp2(level * (0.5 / STEPS))
    return (x * half) * half


def coded(x):
    most = jnp.maximum(jnp.max(jnp.abs(x), axis=0, keepdims=True), 2.0**-120)
    level = jnp.ceil(jnp.log2(most) * STEPS)
    code = jnp.floor(scaled(x, -level) * MOST + 0.5)
    return code.astype(jnp.int32).astype(I16), level


def levels_of(rows):
    blank = jnp.zeros((8 - len(rows), rows[0].shape[1]), F32)
    return jnp.concatenate([*rows, blank], axis=0).astype(jnp.int32).astype(I16)


def wide(code):
    return code.astype(jnp.int32).astype(F32)


def decoded(code, level):
    return scaled(wide(code) * (1.0 / MOST), level)


def own_row(frame, row, col):
    return frame * TILE * TILE + row * TILE + col


def side_row(frame, row, col):
    return (frame * TILE + row) * HALO + col


def select_sides():
    out = np.zeros((2, SIDE, OWN), np.float32)
    for side, first in enumerate((0, TILE - HALO)):
        for frame in range(FRAMES):
            for row in range(TILE):
                for col in range(HALO):
                    out[side, side_row(frame, row, col), own_row(frame, row, first + col)] = 1
    return out


def select_ends():
    out = np.zeros((2, ENDS, OWN + 2 * SIDE), np.float32)
    for end, first in enumerate((0, TILE - HALO)):
        for frame in range(FRAMES):
            at = frame * BAND
            for row in range(HALO):
                for col in range(TILE):
                    out[end, at, own_row(frame, first + row, col)] = 1
                    at += 1
            for side in range(2):
                for row in range(HALO):
                    for col in range(HALO):
                        out[end, at, OWN + side * SIDE + side_row(frame, first + row, col)] = 1
                        at += 1
    return out


SIDES = select_sides()
BANDS = select_ends()


GROUP = 2


def ends_kernel(select_ref, keys_ref, values_ref, left_ref, right_ref, top_ref, bottom_ref):
    for part, ref in enumerate((keys_ref, values_ref)):
        at = slice(part * SIDE, (part + 1) * SIDE)
        rows = jnp.concatenate([ref[...], left_ref[at, :], right_ref[at, :]], axis=0)
        to = slice(part * ENDS, (part + 1) * ENDS)
        top_ref[to, :] = nn(select_ref[0], rows).astype(BF16)
        bottom_ref[to, :] = nn(select_ref[1], rows).astype(BF16)


def sides_kernel(select_ref, keys_ref, values_ref, left_ref, right_ref):
    for part, ref in enumerate((keys_ref, values_ref)):
        rows = ref[...]
        at = slice(part * SIDE, (part + 1) * SIDE)
        left_ref[at, :] = nn(select_ref[0], rows).astype(BF16)
        right_ref[at, :] = nn(select_ref[1], rows).astype(BF16)


def place(part, row, rows):
    piece, within = divmod(row, rows)
    return 4 * (piece // 2) + 2 * part + piece % 2, within


def text_kernel(
    ready,
    norm_ref,
    delta_ref,
    query_ref,
    out_grad_ref,
    key_ref,
    value_ref,
    grad_ref,
    stats_ref,
    levels_ref,
):
    levels_ref[...] = jnp.zeros(levels_ref.shape, F32)
    heads = lax.broadcasted_iota(jnp.int32, (16, HEADS), 1)
    identity = (heads == lax.broadcasted_iota(jnp.int32, (16, HEADS), 0)).astype(F32)
    stats = []
    for which, ref in enumerate((norm_ref, delta_ref)):
        rows = lax.dot_general(
            identity,
            ref[...],
            (((1,), (1,)), ((), ())),
            precision=lax.Precision.HIGHEST,
            preferred_element_type=F32,
        )
        stats_ref[which * 16 : (which + 1) * 16, :] = rows
        stats.append(rows)
    norm, delta = stats
    text = key_ref.shape[0]
    pieces = levels_ref.shape[0] // 8
    sent = grad_ref.shape[0] // pieces
    piece = sent - 8

    def load(h):
        ready(h)
        cols = columns(h)
        q, g, k, v = (r[:, cols] for r in (query_ref, out_grad_ref, key_ref, value_ref))
        return q, g, k, v, norm[h : h + 1], delta[h : h + 1]

    def store(h, q, g, k, probs, score_grad):
        for part, grad in enumerate((nn(score_grad, q) * SCALE, nn(probs, g))):
            code, level = coded(grad)
            for at in range(0, text, 8):
                to, within = place(part, h * text + at, piece)
                grad_ref[to * sent + within : to * sent + within + 8, :] = code[at : at + 8]
                row = to * 8 + within // 8
                levels_ref[row : row + 1, :] = level

    backward(load, store, None)
    for to in range(pieces):
        levels = levels_ref[to * 8 : (to + 1) * 8, :].astype(jnp.int32).astype(I16)
        grad_ref[(to + 1) * sent - 8 : (to + 1) * sent, :] = levels


def over_chips_kernel(parts_ref, out_ref):
    count, sent, _ = parts_ref.shape
    total = 0.0
    for n in range(count):
        levels = wide(parts_ref[n, sent - 8 :, :])
        blocks = [
            decoded(parts_ref[n, 8 * b : 8 * b + 8, :], levels[b : b + 1])
            for b in range((sent - 8) // 8)
        ]
        total = total + jnp.concatenate(blocks, axis=0)
    code, level = coded(total)
    levels = levels_of([level])
    for n in range(out_ref.shape[0]):
        out_ref[n, : sent - 8, :] = code
        out_ref[n, sent - 8 :, :] = levels


def over_tiles_kernel(parts_ref, out_ref):
    count, sent, _ = parts_ref.shape
    total = 0.0
    for n in range(count):
        level = wide(parts_ref[n, sent - 8 :, :])[:1]
        total = total + decoded(parts_ref[n, : sent - 8, :], level)
    total = total.astype(BF16)
    for n in range(out_ref.shape[0]):
        out_ref[n] = total


BLOCK = 12


def backward(load, store, live):
    for first in range(0, HEADS, BLOCK):
        heads = range(first, first + BLOCK)
        given = [load(h) for h in heads]
        scores = [nt(k, q) for q, _, k, _, _, _ in given]
        prob_grads = [nt(v, g) for _, g, _, v, _, _ in given]
        made = []
        for (_, _, _, _, norm, delta), score, prob_grad in zip(given, scores, prob_grads):
            probs = jnp.exp(score * SCALE - norm)
            if live is not None:
                probs = probs * live
            made.append((probs.astype(BF16), (probs * (prob_grad - delta)).astype(BF16)))
        for h, (q, g, k, _, _, _), (probs, score_grad) in zip(heads, given, made):
            store(h, q, g, k, probs, score_grad)


def columns(h):
    return slice(h * HDIM, (h + 1) * HDIM)


def own_kernel(
    live_ref,
    query_ref,
    out_grad_ref,
    keys_ref,
    values_ref,
    text_key_ref,
    text_value_ref,
    stats_ref,
    part_ref,
    query_grad_ref,
    own_key_ref,
    own_value_ref,
):
    text = text_key_ref.shape[0]
    rows = lax.broadcasted_iota(jnp.int32, (OWN + text, HDIM), 0)
    live = jnp.where(rows < OWN, live_ref[4].astype(F32), 1.0)

    def load(h):
        cols = columns(h)
        k = jnp.concatenate([keys_ref[:, cols], text_key_ref[:, cols]], axis=0)
        v = jnp.concatenate([values_ref[:, cols], text_value_ref[:, cols]], axis=0)
        norm, delta = stats_ref[h : h + 1, :], stats_ref[16 + h : 17 + h, :]
        return query_ref[:, cols], out_grad_ref[:, cols], k, v, norm, delta

    def store(h, q, g, k, probs, score_grad):
        cols = columns(h)
        query_grad_ref[:, cols] = part_ref[:, cols] + tn(score_grad, k)
        own_key_ref[:, cols] = nn(score_grad[:OWN], q) * SCALE
        own_value_ref[:, cols] = nn(probs[:OWN], g)

    backward(load, store, live)


def band_kernel(
    live_ref,
    stats_ref,
    query_ref,
    out_grad_ref,
    top_ref,
    bottom_ref,
    part_ref,
    top_grad_ref,
    bottom_grad_ref,
    query_grad_ref,
):
    def live(block):
        return live_ref[block].astype(F32)

    band = lax.rem(lax.broadcasted_iota(jnp.int32, (ENDS, HDIM), 0), BAND)
    lives = [
        jnp.where(
            band < HALO * TILE,
            live(first + 1),
            jnp.where(band < HALO * TILE + CORNER, live(first), live(first + 2)),
        )
        for first in (0, 6)
    ]
    two_halves(
        (stats_ref, query_ref, out_grad_ref, top_ref, bottom_ref, part_ref),
        (top_grad_ref, bottom_grad_ref, query_grad_ref),
        jnp.concatenate(lives, axis=0),
    )


def side_kernel(
    live_ref,
    stats_ref,
    query_ref,
    out_grad_ref,
    left_ref,
    right_ref,
    side_grad_ref,
    query_grad_ref,
):
    rows = lax.broadcasted_iota(jnp.int32, (2 * SIDE, HDIM), 0)
    lives = jnp.where(rows < SIDE, live_ref[3].astype(F32), live_ref[5].astype(F32))
    two_halves(
        (stats_ref, query_ref, out_grad_ref, left_ref, right_ref, None),
        (side_grad_ref.at[: 2 * SIDE + 8], side_grad_ref.at[2 * SIDE + 8 :], query_grad_ref),
        lives,
    )


def two_halves(given, made, live):
    stats_ref, query_ref, out_grad_ref, first_ref, second_ref, part_ref = given
    first_grad_ref, second_grad_ref, query_grad_ref = made
    rows = first_ref.shape[0] // 2

    def load(h):
        cols = columns(h)
        k, v = (
            jnp.concatenate([first_ref[at, cols], second_ref[at, cols]], axis=0)
            for at in (slice(0, rows), slice(rows, 2 * rows))
        )
        norm, delta = stats_ref[h : h + 1, :], stats_ref[16 + h : 17 + h, :]
        return query_ref[:, cols], out_grad_ref[:, cols], k, v, norm, delta

    def store(h, q, g, k, probs, score_grad):
        cols = columns(h)
        query_grad = tn(score_grad, k)
        if part_ref is not None:
            query_grad = ((part_ref[:, cols] + query_grad) * SCALE).astype(BF16)
        query_grad_ref[:, cols] = query_grad
        grads = (nn(score_grad, q) * SCALE, nn(probs, g))
        for n, ref in enumerate((first_grad_ref, second_grad_ref)):
            levels = []
            for at, grad in ((slice(0, rows), grads[0]), (slice(rows, 2 * rows), grads[1])):
                code, level = coded(grad[n * rows : (n + 1) * rows])
                ref[at, cols] = code
                levels.append(level)
            ref[2 * rows :, cols] = levels_of(levels)

    backward(load, store, live)


def received(ref, part, rows):
    level = wide(ref[2 * rows :, :])[part : part + 1]
    return decoded(ref[part * rows : (part + 1) * rows, :], level)


def corners_kernel(
    select_ref, sides_ref, above_ref, below_ref, left_out_ref, right_out_ref
):
    levels = ([], [])
    for part in range(2):
        side = slice(part * SIDE, (part + 1) * SIDE)
        bands = [received(ref, part, ENDS) for ref in (above_ref, below_ref)]
        more = picked(select_ref[...], jnp.concatenate(bands, axis=0))
        for n, out in enumerate((left_out_ref, right_out_ref)):
            rows = 2 * SIDE + 8
            here = received(sides_ref.at[n * rows : (n + 1) * rows], part, SIDE)
            code, level = coded(here + more[n * SIDE : (n + 1) * SIDE])
            out[side, :] = code
            levels[n].append(level)
    left_out_ref[2 * SIDE :, :] = levels_of(levels[0])
    right_out_ref[2 * SIDE :, :] = levels_of(levels[1])


def bands_kernel(above_ref, below_ref, own_key_ref, own_value_ref, key_ref, value_ref):
    edge = HALO * TILE
    refs = ((own_key_ref, key_ref), (own_value_ref, value_ref))
    for part, (own_ref, out_ref) in enumerate(refs):
        above, below = received(above_ref, part, ENDS), received(below_ref, part, ENDS)
        for frame in range(FRAMES):
            at = frame * BAND
            top, end = frame * TILE * TILE, (frame + 1) * TILE * TILE
            bottom = end - edge
            out_ref[top : top + edge, :] = own_ref[top : top + edge, :] + above[at : at + edge]
            out_ref[top + edge : bottom, :] = own_ref[top + edge : bottom, :]
            out_ref[bottom:end, :] = own_ref[bottom:end, :] + below[at : at + edge]


def sum_kernel(select_ref, own_key_ref, own_value_ref, left_ref, right_ref, key_ref, value_ref):
    refs = ((own_key_ref, key_ref), (own_value_ref, value_ref))
    for part, (own_ref, out_ref) in enumerate(refs):
        sides = [received(ref, part, SIDE) for ref in (left_ref, right_ref)]
        total = own_ref[...] + picked(select_ref[...], jnp.concatenate(sides, axis=0))
        out_ref[...] = total.astype(BF16)


def words_kernel(parts_ref, key_ref, value_ref):
    text = key_ref.shape[0]
    rows = parts_ref.shape[1]
    for part, out in enumerate((key_ref, value_ref)):
        for h in range(HEADS):
            for at in range(0, text, 8):
                to, within = place(part, h * text + at, rows)
                piece = parts_ref[to, within : within + 8, :]
                out[at : at + 8, h * HDIM : (h + 1) * HDIM] = piece


def call(kernel, outs, ins, us=1.0, smem=0, fetch=0, scratch=()):
    groups = HEADS // GROUP
    step = GROUP * HDIM

    def body(*refs):
        n = len(ins)
        outputs = refs[n : n + len(outs)]
        near_refs = refs[n + len(outs) : n + len(outs) + fetch]
        semaphores, *rest = refs[n + len(outs) + fetch :]
        small, wide = [], [[] for _ in range(groups)]
        for i, (far, near) in enumerate(zip(refs[smem : smem + fetch], near_refs)):
            if near.ndim == 2 and near.shape[1] == groups * step:
                for m in range(groups):
                    at = (slice(None), slice(m * step, (m + 1) * step))
                    copy = pltpu.make_async_copy(far.at[at], near.at[at], semaphores.at[i, m])
                    wide[m].append(copy)
            else:
                small.append(pltpu.make_async_copy(far, near, semaphores.at[i, 0]))
        for copies in (small, *wide):
            for copy in copies:
                copy.start()
        for copy in small:
            copy.wait()

        def ready(h):
            if h % GROUP == 0:
                for copy in wide[h // GROUP]:
                    copy.wait()

        kernel(ready, *refs[:smem], *near_refs, *refs[smem + fetch : n], *outputs, *rest)

    here = pl.BlockSpec(memory_space=pltpu.VMEM)
    scalars = pl.BlockSpec(memory_space=pltpu.SMEM)
    if not fetch:
        function, specs, scratch, limit = kernel, [scalars] * smem + [here] * (len(ins) - smem), [*scratch], 16
    else:
        function, limit = body, 56
        far = pl.BlockSpec(memory_space=pltpu.HBM)
        specs = [scalars] * smem + [far] * fetch + [here] * (len(ins) - smem - fetch)
        buffers = [pltpu.VMEM(a.shape, a.dtype) for a in ins[smem : smem + fetch]]
        scratch = [*buffers, pltpu.SemaphoreType.DMA((fetch, groups)), *scratch]
    return pl.pallas_call(
        function,
        out_shape=[jax.ShapeDtypeStruct(shape, dtype) for shape, dtype in outs],
        in_specs=specs,
        out_specs=[here] * len(outs),
        scratch_shapes=scratch,
        compiler_params=pltpu.CompilerParams(vmem_limit_bytes=limit * 2**20),
        cost_estimate=pl.CostEstimate(
            flops=int(us * 50000000), bytes_accessed=1000000, transcendentals=0
        ),
    )(*ins)


def shifted(value, axis, steps):
    count = lax.axis_size(axis)
    return lax.ppermute(value, axis, [(i, (i + steps) % count) for i in range(count)])


def by_query(rows):
    return rows.transpose(1, 2, 3, 0).reshape(OWN, HEADS)


def exchanged(pieces, axis):
    return lax.all_to_all(pieces, axis, 0, 0, tiled=True)


def local(
    queries, keys, values, out_grad, log_norm, delta_rows, text_keys, text_values, window_table
):
    shape = queries.shape
    width = shape[-1]
    text = text_keys.shape[0]
    q = queries.reshape(OWN, width)
    g = out_grad.reshape(OWN, width)
    k = keys.reshape(OWN, width)
    v = values.reshape(OWN, width)
    anchor = jnp.zeros((), jnp.int32)
    live = lax.dynamic_slice(
        window_table, (lax.axis_index(HA), lax.axis_index(WA), anchor), (1, 1, 9)
    ).reshape(9)

    count = lax.axis_size(NEAR)
    piece = 2 * HEADS * text // count
    sent = piece + 8
    words, stats = call(
        text_kernel,
        [((count * sent, HDIM), I16), ((32, HDIM), F32)],
        [by_query(log_norm), by_query(delta_rows), q, g, text_keys, text_values],
        us=3,
        fetch=6,
        scratch=[pltpu.VMEM((count * 8, HDIM), F32)],
    )
    words = exchanged(words.reshape(count, sent, HDIM), NEAR)
    tiles = lax.axis_size("wa_0")
    (words,) = call(over_chips_kernel, [((tiles, sent, HDIM), I16)], [words])
    words = exchanged(words, "wa_0")
    (words,) = call(over_tiles_kernel, [((count, piece, HDIM), BF16)], [words])
    words = exchanged(words, NEAR)
    text_key_grad, text_value_grad = call(
        words_kernel, [((text, width), BF16)] * 2, [words]
    )

    left, right = call(
        sides_kernel, [((2 * SIDE, width), BF16)] * 2, [jnp.asarray(SIDES, BF16), k, v]
    )
    from_right = shifted(left, WA, -1)
    from_left = shifted(right, WA, 1)
    top, bottom = call(
        ends_kernel,
        [((2 * ENDS, width), BF16)] * 2,
        [jnp.asarray(BANDS, BF16), k, v, from_left, from_right],
    )
    from_below = shifted(top, HA, -1)
    from_above = shifted(bottom, HA, 1)
    side_grad, part = call(
        side_kernel,
        [((4 * SIDE + 16, width), I16), ((OWN, width), F32)],
        [live, stats, q, g, from_left, from_right],
        us=2,
        smem=1,
    )
    part, own_key, own_value = call(
        own_kernel,
        [((OWN, width), F32)] * 3,
        [live, q, g, k, v, text_keys, text_values, stats, part],
        us=3,
        smem=1,
    )
    top_grad, bottom_grad, query_grad = call(
        band_kernel,
        [((2 * ENDS + 8, width), I16)] * 2 + [((OWN, width), BF16)],
        [live, stats, q, g, from_above, from_below, part],
        us=2,
        smem=1,
    )
    above = shifted(bottom_grad, HA, 1)
    below = shifted(top_grad, HA, -1)
    back = np.concatenate([BANDS[0].T, BANDS[1].T], axis=1)
    left_grad, right_grad = call(
        corners_kernel,
        [((2 * SIDE + 8, width), I16)] * 2,
        [jnp.asarray(back[OWN:], BF16), side_grad, above, below],
    )
    after = shifted(left_grad, WA, -1)
    before = shifted(right_grad, WA, 1)
    own_key, own_value = call(
        bands_kernel, [((OWN, width), F32)] * 2, [above, below, own_key, own_value]
    )
    back = np.concatenate([SIDES[0].T, SIDES[1].T], axis=1)
    key_grad, value_grad = call(
        sum_kernel,
        [((OWN, width), BF16)] * 2,
        [jnp.asarray(back, BF16), own_key, own_value, before, after],
    )
    return (
        query_grad.reshape(shape),
        key_grad.reshape(shape),
        value_grad.reshape(shape),
        text_key_grad,
        text_value_grad,
    )


def solution(mesh):
    split = Mesh(
        mesh.devices.reshape(mesh.shape["group"], 8, 2, mesh.shape["wa"] // 2, 2),
        ("group", "ha_0", "ha_1", "wa_0", "wa_1"),
    )
    return jax.shard_map(
        local,
        mesh=split,
        in_specs=(
            P("group", HA, WA, None),
            P("group", HA, WA, None),
            P("group", HA, WA, None),
            P("group", HA, WA, None),
            P(None, "group", HA, WA),
            P(None, "group", HA, WA),
            P("group", None),
            P("group", None),
            P(),
        ),
        out_specs=(
            P("group", HA, WA, None),
            P("group", HA, WA, None),
            P("group", HA, WA, None),
            P("group", None),
            P("group", None),
        ),
        check_vma=False,
    )
```

```python
import math

import jax
import jax.numpy as jnp
import numpy as np
from jax import lax
from jax.experimental import pallas as pl
from jax.experimental.pallas import tpu as pltpu
from jax.sharding import Mesh
from jax.sharding import PartitionSpec as P


HEADS = 12
HDIM = 128
TILE = 8
HALO = 2
HA = ("ha_0", "ha_1")
WA = ("wa_0", "wa_1")
NEAR = (*HA, "wa_1")
F32 = jnp.float32
BF16 = jnp.bfloat16
SCALE = 1.0 / math.sqrt(HDIM)

FRAMES = 2
OWN = FRAMES * TILE * TILE
SIDE = FRAMES * TILE * HALO
CORNER = HALO * HALO
BAND = HALO * TILE + 2 * CORNER
ENDS = FRAMES * BAND


def nt(a, b):
    return lax.dot_general(a, b, (((1,), (1,)), ((), ())), preferred_element_type=F32)


def nn(a, b):
    return lax.dot_general(a, b, (((1,), (0,)), ((), ())), preferred_element_type=F32)


def tn(a, b):
    return lax.dot_general(a, b, (((0,), (0,)), ((), ())), preferred_element_type=F32)


def picked(select, rows):
    high = rows.astype(BF16)
    low = (rows - high.astype(F32)).astype(BF16)
    return nn(select, high) + nn(select, low)


STEPS = 128.0
MOST = 32000.0
I16 = jnp.int16


def scaled(x, level):
    half = jnp.exp2(level * (0.5 / STEPS))
    return (x * half) * half


def coded(x):
    most = jnp.maximum(jnp.max(jnp.abs(x), axis=0, keepdims=True), 2.0**-120)
    level = jnp.ceil(jnp.log2(most) * STEPS)
    code = jnp.floor(scaled(x, -level) * MOST + 0.5)
    return code.astype(jnp.int32).astype(I16), level


def levels_of(rows):
    blank = jnp.zeros((8 - len(rows), rows[0].shape[1]), F32)
    return jnp.concatenate([*rows, blank], axis=0).astype(jnp.int32).astype(I16)


def wide(code):
    return code.astype(jnp.int32).astype(F32)


def decoded(code, level):
    return scaled(wide(code) * (1.0 / MOST), level)


def own_row(frame, row, col):
    return frame * TILE * TILE + row * TILE + col


def side_row(frame, row, col):
    return (frame * TILE + row) * HALO + col


def select_sides():
    out = np.zeros((2, SIDE, OWN), np.float32)
    for side, first in enumerate((0, TILE - HALO)):
        for frame in range(FRAMES):
            for row in range(TILE):
                for col in range(HALO):
                    out[side, side_row(frame, row, col), own_row(frame, row, first + col)] = 1
    return out


def select_ends():
    out = np.zeros((2, ENDS, OWN + 2 * SIDE), np.float32)
    for end, first in enumerate((0, TILE - HALO)):
        for frame in range(FRAMES):
            at = frame * BAND
            for row in range(HALO):
                for col in range(TILE):
                    out[end, at, own_row(frame, first + row, col)] = 1
                    at += 1
            for side in range(2):
                for row in range(HALO):
                    for col in range(HALO):
                        out[end, at, OWN + side * SIDE + side_row(frame, first + row, col)] = 1
                        at += 1
    return out


SIDES = select_sides()
BANDS = select_ends()


GROUP = 2


def ends_kernel(select_ref, keys_ref, values_ref, left_ref, right_ref, top_ref, bottom_ref):
    for part, ref in enumerate((keys_ref, values_ref)):
        at = slice(part * SIDE, (part + 1) * SIDE)
        rows = jnp.concatenate([ref[...], left_ref[at, :], right_ref[at, :]], axis=0)
        to = slice(part * ENDS, (part + 1) * ENDS)
        top_ref[to, :] = nn(select_ref[0], rows).astype(BF16)
        bottom_ref[to, :] = nn(select_ref[1], rows).astype(BF16)


def sides_kernel(select_ref, keys_ref, values_ref, left_ref, right_ref):
    for part, ref in enumerate((keys_ref, values_ref)):
        rows = ref[...]
        at = slice(part * SIDE, (part + 1) * SIDE)
        left_ref[at, :] = nn(select_ref[0], rows).astype(BF16)
        right_ref[at, :] = nn(select_ref[1], rows).astype(BF16)


def place(part, row, rows):
    piece, within = divmod(row, rows)
    return 4 * (piece // 2) + 2 * part + piece % 2, within


def text_kernel(
    ready,
    norm_ref,
    delta_ref,
    query_ref,
    out_grad_ref,
    key_ref,
    value_ref,
    grad_ref,
    stats_ref,
    levels_ref,
):
    levels_ref[...] = jnp.zeros(levels_ref.shape, F32)
    heads = lax.broadcasted_iota(jnp.int32, (16, HEADS), 1)
    identity = (heads == lax.broadcasted_iota(jnp.int32, (16, HEADS), 0)).astype(F32)
    stats = []
    for which, ref in enumerate((norm_ref, delta_ref)):
        rows = lax.dot_general(
            identity,
            ref[...],
            (((1,), (1,)), ((), ())),
            precision=lax.Precision.HIGHEST,
            preferred_element_type=F32,
        )
        stats_ref[which * 16 : (which + 1) * 16, :] = rows
        stats.append(rows)
    norm, delta = stats
    text = key_ref.shape[0]
    pieces = levels_ref.shape[0] // 8
    sent = grad_ref.shape[0] // pieces
    piece = sent - 8

    def load(h):
        ready(h)
        cols = columns(h)
        q, g, k, v = (r[:, cols] for r in (query_ref, out_grad_ref, key_ref, value_ref))
        return q, g, k, v, norm[h : h + 1], delta[h : h + 1]

    def store(h, q, g, k, probs, score_grad):
        for part, grad in enumerate((nn(score_grad, q) * SCALE, nn(probs, g))):
            code, level = coded(grad)
            for at in range(0, text, 8):
                to, within = place(part, h * text + at, piece)
                grad_ref[to * sent + within : to * sent + within + 8, :] = code[at : at + 8]
                row = to * 8 + within // 8
                levels_ref[row : row + 1, :] = level

    backward(load, store, None)
    for to in range(pieces):
        levels = levels_ref[to * 8 : (to + 1) * 8, :].astype(jnp.int32).astype(I16)
        grad_ref[(to + 1) * sent - 8 : (to + 1) * sent, :] = levels


def over_chips_kernel(parts_ref, out_ref):
    count, sent, _ = parts_ref.shape
    total = 0.0
    for n in range(count):
        levels = wide(parts_ref[n, sent - 8 :, :])
        blocks = [
            decoded(parts_ref[n, 8 * b : 8 * b + 8, :], levels[b : b + 1])
            for b in range((sent - 8) // 8)
        ]
        total = total + jnp.concatenate(blocks, axis=0)
    code, level = coded(total)
    levels = levels_of([level])
    for n in range(out_ref.shape[0]):
        out_ref[n, : sent - 8, :] = code
        out_ref[n, sent - 8 :, :] = levels


def over_tiles_kernel(parts_ref, out_ref):
    count, sent, _ = parts_ref.shape
    total = 0.0
    for n in range(count):
        level = wide(parts_ref[n, sent - 8 :, :])[:1]
        total = total + decoded(parts_ref[n, : sent - 8, :], level)
    total = total.astype(BF16)
    for n in range(out_ref.shape[0]):
        out_ref[n] = total


BLOCK = 12


def backward(load, store, live):
    for first in range(0, HEADS, BLOCK):
        heads = range(first, first + BLOCK)
        given = [load(h) for h in heads]
        scores = [nt(k, q) for q, _, k, _, _, _ in given]
        prob_grads = [nt(v, g) for _, g, _, v, _, _ in given]
        made = []
        for (_, _, _, _, norm, delta), score, prob_grad in zip(given, scores, prob_grads):
            probs = jnp.exp(score * SCALE - norm)
            if live is not None:
                probs = probs * live
            made.append((probs.astype(BF16), (probs * (prob_grad - delta)).astype(BF16)))
        for h, (q, g, k, _, _, _), (probs, score_grad) in zip(heads, given, made):
            store(h, q, g, k, probs, score_grad)


def columns(h):
    return slice(h * HDIM, (h + 1) * HDIM)


def own_kernel(
    live_ref,
    query_ref,
    out_grad_ref,
    keys_ref,
    values_ref,
    text_key_ref,
    text_value_ref,
    stats_ref,
    part_ref,
    query_grad_ref,
    own_key_ref,
    own_value_ref,
):
    text = text_key_ref.shape[0]
    rows = lax.broadcasted_iota(jnp.int32, (OWN + text, HDIM), 0)
    live = jnp.where(rows < OWN, live_ref[4].astype(F32), 1.0)

    def load(h):
        cols = columns(h)
        k = jnp.concatenate([keys_ref[:, cols], text_key_ref[:, cols]], axis=0)
        v = jnp.concatenate([values_ref[:, cols], text_value_ref[:, cols]], axis=0)
        norm, delta = stats_ref[h : h + 1, :], stats_ref[16 + h : 17 + h, :]
        return query_ref[:, cols], out_grad_ref[:, cols], k, v, norm, delta

    def store(h, q, g, k, probs, score_grad):
        cols = columns(h)
        query_grad_ref[:, cols] = part_ref[:, cols] + tn(score_grad, k)
        own_key_ref[:, cols] = nn(score_grad[:OWN], q) * SCALE
        own_value_ref[:, cols] = nn(probs[:OWN], g)

    backward(load, store, live)


def band_kernel(
    live_ref,
    stats_ref,
    query_ref,
    out_grad_ref,
    top_ref,
    bottom_ref,
    part_ref,
    top_grad_ref,
    bottom_grad_ref,
    query_grad_ref,
):
    def live(block):
        return live_ref[block].astype(F32)

    band = lax.rem(lax.broadcasted_iota(jnp.int32, (ENDS, HDIM), 0), BAND)
    lives = [
        jnp.where(
            band < HALO * TILE,
            live(first + 1),
            jnp.where(band < HALO * TILE + CORNER, live(first), live(first + 2)),
        )
        for first in (0, 6)
    ]
    two_halves(
        (stats_ref, query_ref, out_grad_ref, top_ref, bottom_ref, part_ref),
        (top_grad_ref, bottom_grad_ref, query_grad_ref),
        jnp.concatenate(lives, axis=0),
    )


def side_kernel(
    live_ref,
    stats_ref,
    query_ref,
    out_grad_ref,
    left_ref,
    right_ref,
    side_grad_ref,
    query_grad_ref,
):
    rows = lax.broadcasted_iota(jnp.int32, (2 * SIDE, HDIM), 0)
    lives = jnp.where(rows < SIDE, live_ref[3].astype(F32), live_ref[5].astype(F32))
    two_halves(
        (stats_ref, query_ref, out_grad_ref, left_ref, right_ref, None),
        (side_grad_ref.at[: 2 * SIDE + 8], side_grad_ref.at[2 * SIDE + 8 :], query_grad_ref),
        lives,
    )


def two_halves(given, made, live):
    stats_ref, query_ref, out_grad_ref, first_ref, second_ref, part_ref = given
    first_grad_ref, second_grad_ref, query_grad_ref = made
    rows = first_ref.shape[0] // 2

    def load(h):
        cols = columns(h)
        k, v = (
            jnp.concatenate([first_ref[at, cols], second_ref[at, cols]], axis=0)
            for at in (slice(0, rows), slice(rows, 2 * rows))
        )
        norm, delta = stats_ref[h : h + 1, :], stats_ref[16 + h : 17 + h, :]
        return query_ref[:, cols], out_grad_ref[:, cols], k, v, norm, delta

    def store(h, q, g, k, probs, score_grad):
        cols = columns(h)
        query_grad = tn(score_grad, k)
        if part_ref is not None:
            query_grad = ((part_ref[:, cols] + query_grad) * SCALE).astype(BF16)
        query_grad_ref[:, cols] = query_grad
        grads = (nn(score_grad, q) * SCALE, nn(probs, g))
        for n, ref in enumerate((first_grad_ref, second_grad_ref)):
            levels = []
            for at, grad in ((slice(0, rows), grads[0]), (slice(rows, 2 * rows), grads[1])):
                code, level = coded(grad[n * rows : (n + 1) * rows])
                ref[at, cols] = code
                levels.append(level)
            ref[2 * rows :, cols] = levels_of(levels)

    backward(load, store, live)


def received(ref, part, rows):
    level = wide(ref[2 * rows :, :])[part : part + 1]
    return decoded(ref[part * rows : (part + 1) * rows, :], level)


def corners_kernel(
    select_ref, sides_ref, above_ref, below_ref, left_out_ref, right_out_ref
):
    levels = ([], [])
    for part in range(2):
        side = slice(part * SIDE, (part + 1) * SIDE)
        bands = [received(ref, part, ENDS) for ref in (above_ref, below_ref)]
        more = picked(select_ref[...], jnp.concatenate(bands, axis=0))
        for n, out in enumerate((left_out_ref, right_out_ref)):
            rows = 2 * SIDE + 8
            here = received(sides_ref.at[n * rows : (n + 1) * rows], part, SIDE)
            code, level = coded(here + more[n * SIDE : (n + 1) * SIDE])
            out[side, :] = code
            levels[n].append(level)
    left_out_ref[2 * SIDE :, :] = levels_of(levels[0])
    right_out_ref[2 * SIDE :, :] = levels_of(levels[1])


def sum_kernel(
    select_ref,
    own_key_ref,
    own_value_ref,
    left_ref,
    right_ref,
    above_ref,
    below_ref,
    key_ref,
    value_ref,
):
    own_refs = (own_key_ref, own_value_ref)
    edge = HALO * TILE
    for part, out in enumerate((key_ref, value_ref)):
        above, below = received(above_ref, part, ENDS), received(below_ref, part, ENDS)
        sides = [received(ref, part, SIDE) for ref in (left_ref, right_ref)]
        rows = jnp.concatenate(sides, axis=0)
        total = own_refs[part][...] + picked(select_ref[...], rows)
        for frame in range(FRAMES):
            at = frame * BAND
            top = frame * TILE * TILE
            bottom = top + TILE * TILE - edge
            end = top + TILE * TILE
            out[top : top + edge, :] = (
                total[top : top + edge] + above[at : at + edge]
            ).astype(BF16)
            out[top + edge : bottom, :] = total[top + edge : bottom].astype(BF16)
            out[bottom:end, :] = (total[bottom:end] + below[at : at + edge]).astype(BF16)


def words_kernel(parts_ref, key_ref, value_ref):
    text = key_ref.shape[0]
    rows = parts_ref.shape[1]
    for part, out in enumerate((key_ref, value_ref)):
        for h in range(HEADS):
            for at in range(0, text, 8):
                to, within = place(part, h * text + at, rows)
                piece = parts_ref[to, within : within + 8, :]
                out[at : at + 8, h * HDIM : (h + 1) * HDIM] = piece


def call(kernel, outs, ins, us=1.0, smem=0, fetch=0, scratch=()):
    groups = HEADS // GROUP
    step = GROUP * HDIM

    def body(*refs):
        n = len(ins)
        outputs = refs[n : n + len(outs)]
        near_refs = refs[n + len(outs) : n + len(outs) + fetch]
        semaphores, *rest = refs[n + len(outs) + fetch :]
        small, wide = [], [[] for _ in range(groups)]
        for i, (far, near) in enumerate(zip(refs[smem : smem + fetch], near_refs)):
            if near.ndim == 2 and near.shape[1] == groups * step:
                for m in range(groups):
                    at = (slice(None), slice(m * step, (m + 1) * step))
                    copy = pltpu.make_async_copy(far.at[at], near.at[at], semaphores.at[i, m])
                    wide[m].append(copy)
            else:
                small.append(pltpu.make_async_copy(far, near, semaphores.at[i, 0]))
        for copies in (small, *wide):
            for copy in copies:
                copy.start()
        for copy in small:
            copy.wait()

        def ready(h):
            if h % GROUP == 0:
                for copy in wide[h // GROUP]:
                    copy.wait()

        kernel(ready, *refs[:smem], *near_refs, *refs[smem + fetch : n], *outputs, *rest)

    here = pl.BlockSpec(memory_space=pltpu.VMEM)
    scalars = pl.BlockSpec(memory_space=pltpu.SMEM)
    if not fetch:
        function, specs, scratch, limit = kernel, [scalars] * smem + [here] * (len(ins) - smem), [*scratch], 16
    else:
        function, limit = body, 56
        far = pl.BlockSpec(memory_space=pltpu.HBM)
        specs = [scalars] * smem + [far] * fetch + [here] * (len(ins) - smem - fetch)
        buffers = [pltpu.VMEM(a.shape, a.dtype) for a in ins[smem : smem + fetch]]
        scratch = [*buffers, pltpu.SemaphoreType.DMA((fetch, groups)), *scratch]
    return pl.pallas_call(
        function,
        out_shape=[jax.ShapeDtypeStruct(shape, dtype) for shape, dtype in outs],
        in_specs=specs,
        out_specs=[here] * len(outs),
        scratch_shapes=scratch,
        compiler_params=pltpu.CompilerParams(vmem_limit_bytes=limit * 2**20),
        cost_estimate=pl.CostEstimate(
            flops=int(us * 50000000), bytes_accessed=1000000, transcendentals=0
        ),
    )(*ins)


def shifted(value, axis, steps):
    count = lax.axis_size(axis)
    return lax.ppermute(value, axis, [(i, (i + steps) % count) for i in range(count)])


def by_query(rows):
    return rows.transpose(1, 2, 3, 0).reshape(OWN, HEADS)


def exchanged(pieces, axis):
    return lax.all_to_all(pieces, axis, 0, 0, tiled=True)


def local(
    queries, keys, values, out_grad, log_norm, delta_rows, text_keys, text_values, window_table
):
    shape = queries.shape
    width = shape[-1]
    text = text_keys.shape[0]
    q = queries.reshape(OWN, width)
    g = out_grad.reshape(OWN, width)
    k = keys.reshape(OWN, width)
    v = values.reshape(OWN, width)
    anchor = jnp.zeros((), jnp.int32)
    live = lax.dynamic_slice(
        window_table, (lax.axis_index(HA), lax.axis_index(WA), anchor), (1, 1, 9)
    ).reshape(9)

    count = lax.axis_size(NEAR)
    piece = 2 * HEADS * text // count
    sent = piece + 8
    words, stats = call(
        text_kernel,
        [((count * sent, HDIM), I16), ((32, HDIM), F32)],
        [by_query(log_norm), by_query(delta_rows), q, g, text_keys, text_values],
        us=3,
        fetch=6,
        scratch=[pltpu.VMEM((count * 8, HDIM), F32)],
    )
    words = exchanged(words.reshape(count, sent, HDIM), NEAR)
    tiles = lax.axis_size("wa_0")
    (words,) = call(over_chips_kernel, [((tiles, sent, HDIM), I16)], [words])
    words = exchanged(words, "wa_0")
    (words,) = call(over_tiles_kernel, [((count, piece, HDIM), BF16)], [words])
    words = exchanged(words, NEAR)
    text_key_grad, text_value_grad = call(
        words_kernel, [((text, width), BF16)] * 2, [words]
    )

    left, right = call(
        sides_kernel, [((2 * SIDE, width), BF16)] * 2, [jnp.asarray(SIDES, BF16), k, v]
    )
    from_right = shifted(left, WA, -1)
    from_left = shifted(right, WA, 1)
    top, bottom = call(
        ends_kernel,
        [((2 * ENDS, width), BF16)] * 2,
        [jnp.asarray(BANDS, BF16), k, v, from_left, from_right],
    )
    from_below = shifted(top, HA, -1)
    from_above = shifted(bottom, HA, 1)
    side_grad, part = call(
        side_kernel,
        [((4 * SIDE + 16, width), I16), ((OWN, width), F32)],
        [live, stats, q, g, from_left, from_right],
        us=2,
        smem=1,
    )
    part, own_key, own_value = call(
        own_kernel,
        [((OWN, width), F32)] * 3,
        [live, q, g, k, v, text_keys, text_values, stats, part],
        us=3,
        smem=1,
    )
    top_grad, bottom_grad, query_grad = call(
        band_kernel,
        [((2 * ENDS + 8, width), I16)] * 2 + [((OWN, width), BF16)],
        [live, stats, q, g, from_above, from_below, part],
        us=2,
        smem=1,
    )
    above = shifted(bottom_grad, HA, 1)
    below = shifted(top_grad, HA, -1)
    back = np.concatenate([BANDS[0].T, BANDS[1].T], axis=1)
    left_grad, right_grad = call(
        corners_kernel,
        [((2 * SIDE + 8, width), I16)] * 2,
        [jnp.asarray(back[OWN:], BF16), side_grad, above, below],
    )
    after = shifted(left_grad, WA, -1)
    before = shifted(right_grad, WA, 1)
    back = np.concatenate([SIDES[0].T, SIDES[1].T], axis=1)
    key_grad, value_grad = call(
        sum_kernel,
        [((OWN, width), BF16)] * 2,
        [jnp.asarray(back, BF16), own_key, own_value, before, after, above, below],
    )
    return (
        query_grad.reshape(shape),
        key_grad.reshape(shape),
        value_grad.reshape(shape),
        text_key_grad,
        text_value_grad,
    )


def solution(mesh):
    split = Mesh(
        mesh.devices.reshape(mesh.shape["group"], 8, 2, mesh.shape["wa"] // 2, 2),
        ("group", "ha_0", "ha_1", "wa_0", "wa_1"),
    )
    return jax.shard_map(
        local,
        mesh=split,
        in_specs=(
            P("group", HA, WA, None),
            P("group", HA, WA, None),
            P("group", HA, WA, None),
            P("group", HA, WA, None),
            P(None, "group", HA, WA),
            P(None, "group", HA, WA),
            P("group", None),
            P("group", None),
            P(),
        ),
        out_specs=(
            P("group", HA, WA, None),
            P("group", HA, WA, None),
            P("group", HA, WA, None),
            P("group", None),
            P("group", None),
        ),
        check_vma=False,
    )
```
